32 devices in a mesh: vel: 8 (over z, y), gx: 4 (over x, core).
Axes of the slice: x: 2, y: 2, z: 4, core: 2. Of those that a mesh axis runs over, the one named last changes fastest.
Arguments:
- distribution: float32 [4096, 32, 128], P('vel', 'gx'), may hold values from 0.1 to 10
- velocity: float32 [3, 4096], P(None, 'vel'), may hold values from -3 to 3
- weights: float32 [4096], P('vel'), may hold values from 0.00012207031 to 0.00048828125
- collision: float32 [32, 128], P('gx'), may hold values from 0.2 to 2
- solid: int32 [32, 128], P('gx'), may hold values 0 or 1
- inflow: float32 [2, 4096, 128], P(None, 'vel'), may hold values from 0.1 to 10
Outputs:
- evolved: float32 [4096, 32, 128], P('vel', 'gx')
- macroscopic: float32 [5, 32, 128], P(None, 'gx')
The draws below stay inside these ranges and needn't reach their ends.
All inputs are finite; a program needn't handle non-finite values. No bound on the sum of `solid` on one device may be relied on, other than what follows from the above.
Results may differ from the reference program's by a relative error of at most 0.0001.
Values sent between devices are 32-bit elements; how exact they have to be, the bound alone decides.
No kernel may reach another device: no remote copies, remote signals or barrier semaphores. Data moves between devices by JAX's collectives and lax.ppermute only.
A program may use at most 128 MiB of HBM per device.

```python
import math
import jax
import jax.numpy as jnp
from jax import lax

NV = 4096
NY = 16
NZ = 8
ITERS = 2
JACOBI = 2
NX = 32
N_VEL = 8


def place_ends(drawn, own_key, smallest, high):
    longest = drawn.shape.index(max(drawn.shape))
    spots = []
    for shift in (0, 1):
        where = [jax.random.randint(jax.random.fold_in(own_key, axis), (), 0, length) for axis, length in enumerate(drawn.shape)]
        where[longest] = (where[longest] + shift) % drawn.shape[longest]
        spots.append(tuple(where))
    return drawn.at[spots[0]].set(smallest).at[spots[1]].set(high)


def block_levels(key, shape, cuts, smallest, top_value):
    loudness = 1.0
    for position, parts in cuts:
        heights = jax.random.uniform(jax.random.fold_in(jax.random.fold_in(key, 6), position), (parts,), jnp.float32, smallest / len(cuts), top_value / len(cuts))
        loudness = loudness * jnp.repeat(jnp.exp(heights), shape[position] // parts).reshape((-1,) + (1,) * (len(shape) - 1 - position))
    return loudness


def setup_inputs(seed: int = 0) -> dict:
    arg_keys = jax.random.split(jax.random.key(seed), 7)
    distribution = jnp.clip(jnp.exp(math.log(10.0) - 4.6051702 * jax.random.uniform(arg_keys[0], (NV, NX, NY * NZ), jnp.float32) ** block_levels(arg_keys[0], (NV, NX, NY * NZ), ((0, 8), (1, 4)), -0.2, 0.2)), 0.1, 10.0)
    velocity = jnp.clip(jax.random.uniform(arg_keys[1], (3, NV), jnp.float32, -3.0, 3.0) * block_levels(arg_keys[1], (3, NV), ((1, 8),), -0.4, 0.0), -3.0, 3.0)
    weights = jnp.clip(jnp.exp(math.log(0.00048828125) - 1.3862944 * jax.random.uniform(arg_keys[2], (NV,), jnp.float32) ** block_levels(arg_keys[2], (NV,), ((0, 8),), -0.2, 0.2)), 0.00012207031, 0.00048828125)
    collision = jnp.clip(jnp.exp(math.log(2.0) - 2.3025851 * jax.random.uniform(arg_keys[3], (NX, NY * NZ), jnp.float32) ** block_levels(arg_keys[3], (NX, NY * NZ), ((0, 4),), -0.2, 0.2)), 0.2, 2.0)
    solid = place_ends((jax.random.randint(arg_keys[4], (NX, NY * NZ), 0, 8) < 1).astype(jnp.int32), jax.random.fold_in(arg_keys[4], 1), 0, 1)
    inflow = jnp.clip(jnp.exp(math.log(10.0) - 4.6051702 * jax.random.uniform(arg_keys[5], (2, NV, NY * NZ), jnp.float32) ** block_levels(arg_keys[5], (2, NV, NY * NZ), ((1, 8),), -0.2, 0.2)), 0.1, 10.0)
    return dict(distribution=distribution, velocity=velocity, weights=weights, collision=collision, solid=solid, inflow=inflow)


pseudo_rate = 0.5
cross_spacing = 2.0
source_gain = 0.5
diffusion = (0.6, 0.8, 0.8, 0.8, 1.0)
viscous_conduction_ratio = 2.0 / 3.0
wall_rate = 4.0
box_volume = 216.0
highest_moment = lax.Precision.HIGHEST


def basis_rows(speed, thermal_scale):
    stream, spanwise, normal = speed[0], speed[1], speed[2]
    relative_motion_energy = stream * stream + spanwise * spanwise + normal * normal
    rows = jnp.stack([jnp.ones_like(stream), stream, spanwise, normal, relative_motion_energy,
                      stream * stream, spanwise * spanwise, stream * spanwise, stream * normal, spanwise * normal,
                      stream * relative_motion_energy, spanwise * relative_motion_energy, normal * relative_motion_energy])
    return rows * thermal_scale[None, :]


def macro_fields(weighted_integrals):
    particle_concentration = weighted_integrals[0]
    mean_flow_vector = [weighted_integrals[1] / particle_concentration, weighted_integrals[2] / particle_concentration, weighted_integrals[3] / particle_concentration]
    magnitude_power_two = mean_flow_vector[0] * mean_flow_vector[0] + mean_flow_vector[1] * mean_flow_vector[1] + mean_flow_vector[2] * mean_flow_vector[2]
    kinetic_warmth = (weighted_integrals[4] / particle_concentration - magnitude_power_two) / 3.0
    isotropic_normal_force = particle_concentration * kinetic_warmth
    second = [[weighted_integrals[5], weighted_integrals[7], weighted_integrals[8]],
              [weighted_integrals[7], weighted_integrals[6], weighted_integrals[9]],
              [weighted_integrals[8], weighted_integrals[9], weighted_integrals[4] - weighted_integrals[5] - weighted_integrals[6]]]
    deviatoric_tensor = [second[0][0] - particle_concentration * mean_flow_vector[0] * mean_flow_vector[0] - isotropic_normal_force,
              second[1][1] - particle_concentration * mean_flow_vector[1] * mean_flow_vector[1] - isotropic_normal_force,
              second[0][1] - particle_concentration * mean_flow_vector[0] * mean_flow_vector[1],
              second[0][2] - particle_concentration * mean_flow_vector[0] * mean_flow_vector[2],
              second[1][2] - particle_concentration * mean_flow_vector[1] * mean_flow_vector[2]]
    energy_transport_vector = []
    for column in range(3):
        inner = mean_flow_vector[0] * second[column][0] + mean_flow_vector[1] * second[column][1] + mean_flow_vector[2] * second[column][2]
        energy_transport_vector.append(0.5 * (weighted_integrals[10 + column] - 2.0 * inner - mean_flow_vector[column] * weighted_integrals[4]
                           + 2.0 * particle_concentration * mean_flow_vector[column] * magnitude_power_two))
    return jnp.stack([particle_concentration] + mean_flow_vector + [kinetic_warmth] + deviatoric_tensor + energy_transport_vector)


def roll_cells(field, offset, along):
    grid = field.reshape(field.shape[:-1] + (NY, NZ))
    return jnp.roll(grid, offset, axis=grid.ndim - 2 + along).reshape(field.shape)


def centred(field, along):
    return 0.5 * (roll_cells(field, -1, along) - roll_cells(field, 1, along))


def flux_pack(layered_arrays):
    return jnp.stack([layered_arrays[0] * layered_arrays[1], layered_arrays[5], layered_arrays[7], layered_arrays[8], layered_arrays[10]])


def sources(layered_arrays, padded):
    across = 0.5 * (padded[:, 2:] - padded[:, :-2])
    particle_concentration, kinetic_warmth = layered_arrays[0], layered_arrays[4]
    zz_stress = -(layered_arrays[5] + layered_arrays[6])
    div_mass = across[0] + centred(particle_concentration * layered_arrays[2], 0) + centred(particle_concentration * layered_arrays[3], 1)
    div_first = across[1] + centred(layered_arrays[7], 0) + centred(layered_arrays[8], 1)
    div_second = across[2] + centred(layered_arrays[6], 0) + centred(layered_arrays[9], 1)
    cubic_integral_spread = across[3] + centred(layered_arrays[9], 0) + centred(zz_stress, 1)
    energy_transport_spread = across[4] + centred(layered_arrays[11], 0) + centred(layered_arrays[12], 1)
    return -source_gain * jnp.stack([div_mass / particle_concentration, div_first / particle_concentration, div_second / particle_concentration,
                                     cubic_integral_spread / particle_concentration, (2.0 / 3.0) * energy_transport_spread / (particle_concentration * kinetic_warmth)])


def relax(source, delta, padded):
    weight = jnp.array(diffusion, jnp.float32)[:, None, None]
    beside_all = padded[:, 2:] + padded[:, :-2]
    beside_all = beside_all + roll_cells(delta, 1, 0) + roll_cells(delta, -1, 0)
    beside_all = beside_all + roll_cells(delta, 1, 1) + roll_cells(delta, -1, 1)
    return (source + weight * beside_all) / (1.0 + 6.0 * weight)


def corrected(layered_arrays, delta):
    return jnp.stack([layered_arrays[0] * jnp.exp(delta[0]), layered_arrays[1] + delta[1], layered_arrays[2] + delta[2],
                      layered_arrays[3] + delta[3], layered_arrays[4] * jnp.exp(delta[4])])


def peculiar_terms(speed, hydrodynamic_description):
    peculiar = [speed[component][:, None, None] - hydrodynamic_description[1 + component][None] for component in range(3)]
    relative_motion_energy = peculiar[0] * peculiar[0] + peculiar[1] * peculiar[1] + peculiar[2] * peculiar[2]
    exponent_factor = jnp.exp(-relative_motion_energy / (2.0 * hydrodynamic_description[4][None]))
    return peculiar, relative_motion_energy, exponent_factor


def kinetic_terms(speed, state, hydrodynamic_description, energy_transport_vector, total, wall, rate, extent, peculiar, relative_motion_energy, exponent_factor):
    particle_concentration = hydrodynamic_description[0][None]
    kinetic_warmth = hydrodynamic_description[4][None]
    gaussian_local_distribution = particle_concentration * exponent_factor / total[None]
    dyadic_matrix = peculiar[0] * energy_transport_vector[0][None] + peculiar[1] * energy_transport_vector[1][None] + peculiar[2] * energy_transport_vector[2][None]
    corrected_relaxation_goal = gaussian_local_distribution * (1.0 + (1.0 - viscous_conduction_ratio) * dyadic_matrix * (relative_motion_energy / kinetic_warmth - 5.0)
                         / (5.0 * particle_concentration * kinetic_warmth * kinetic_warmth))
    resting = box_volume * (2.0 * math.pi) ** -1.5 * jnp.exp(-0.5 * jnp.sum(speed * speed, axis=0))
    target = (1.0 - wall[None]) * corrected_relaxation_goal + wall[None] * particle_concentration * resting[:, None, None]
    stream = speed[0][:, None, None]
    spanwise = speed[1][:, None, None]
    normal = speed[2][:, None, None]
    driving = pseudo_rate * state
    driving = driving + jnp.maximum(spanwise, 0.0) / cross_spacing * roll_cells(state, 1, 0)
    driving = driving + jnp.maximum(-spanwise, 0.0) / cross_spacing * roll_cells(state, -1, 0)
    driving = driving + jnp.maximum(normal, 0.0) / cross_spacing * roll_cells(state, 1, 1)
    driving = driving + jnp.maximum(-normal, 0.0) / cross_spacing * roll_cells(state, -1, 1)
    driving = driving + rate[None] * target
    denominator = pseudo_rate + (jnp.abs(spanwise) + jnp.abs(normal)) / cross_spacing + rate[None] + jnp.abs(stream) * extent
    forward = jnp.maximum(stream, 0.0) * extent / denominator
    backward = jnp.maximum(-stream, 0.0) * extent / denominator
    return forward, backward, driving / denominator


def chain(earlier, later):
    return (earlier[0] * later[0], later[0] * earlier[1] + later[1])


def global_sweep(forward, backward, offset, entering):
    gain, carry = lax.associative_scan(chain, (forward, offset), axis=1)
    upwind = gain * entering[0][:, None, :] + carry
    gain, carry = lax.associative_scan(chain, (backward, upwind), reverse=True, axis=1)
    return gain * entering[1][:, None, :] + carry


def x_pad(field):
    return jnp.pad(field, ((0, 0), (1, 1), (0, 0)))


def reference(distribution, velocity, weights, collision, solid, inflow):
    block = NV // N_VEL
    cells = NY * NZ
    wall = solid.astype(jnp.float32)
    rate = collision + wall_rate * wall
    speeds = velocity.reshape(3, N_VEL, block).transpose(1, 0, 2)
    scales = weights.reshape(N_VEL, block)
    entering = inflow.reshape(2, N_VEL, block, cells).transpose(1, 0, 2, 3)
    state = distribution.reshape(N_VEL, block, NX, cells)
    for repeat in range(ITERS):
        def moment_block(pieces):
            speed, thermal_scale, piece = pieces
            return jnp.dot(basis_rows(speed, thermal_scale), piece.reshape(block, NX * cells), precision=highest_moment)

        weighted_integrals = jnp.sum(lax.map(moment_block, (speeds, scales, state)), axis=0).reshape(13, NX, cells)
        layered_arrays = macro_fields(weighted_integrals)
        source = sources(layered_arrays, x_pad(flux_pack(layered_arrays)))
        delta = source
        for sweep in range(JACOBI):
            delta = relax(source, delta, x_pad(delta))
        hydrodynamic_description = corrected(layered_arrays, delta)
        energy_transport_vector = layered_arrays[10:13]

        def mass_block(pieces):
            speed, thermal_scale = pieces
            exponent_factor = peculiar_terms(speed, hydrodynamic_description)[2]
            return jnp.einsum("h,hob->ob", thermal_scale, exponent_factor, precision=highest_moment)

        total = jnp.sum(lax.map(mass_block, (speeds, scales)), axis=0)

        def advance(pieces):
            speed, piece, enter = pieces
            peculiar, relative_motion_energy, exponent_factor = peculiar_terms(speed, hydrodynamic_description)
            forward, backward, offset = kinetic_terms(speed, piece, hydrodynamic_description, energy_transport_vector, total, wall, rate, NX,
                                                      peculiar, relative_motion_energy, exponent_factor)
            return global_sweep(forward, backward, offset, enter)

        state = lax.map(advance, (speeds, state, entering))
    return state.reshape(NV, NX, cells), hydrodynamic_description
```

```python
import functools
import math

import jax
import jax.numpy as jnp
from jax import lax
from jax.experimental import pallas as pl
from jax.experimental.pallas import tpu as pltpu
from jax.sharding import PartitionSpec as P

NY = 16
NZ = 8
ITERS = 2
JACOBI = 2
HALO = JACOBI + 1
pseudo_rate = 0.5
source_gain = 0.5
diffusion = (0.6, 0.8, 0.8, 0.8, 1.0)
viscous_conduction_ratio = 2.0 / 3.0
wall_rate = 4.0
box_volume = 216.0
LOG2E = math.log2(math.e)
LANES = 128
SUB = 8
PAIRS = ((0, 0), (0, 1), (1, 0), (0, 2), (2, 0), (1, 1))
FEATURES = 32
A, B, E, W, HB, HE, BASE, FA, BA, REST = range(10)
TABLE = 10


def f32(*shape):
    return jax.ShapeDtypeStruct(shape, jnp.float32)


def add_moments(acc, s, t_ref, rows):
    a, b, e = (t_ref[k, rows, :] for k in (A, B, E))
    g = s * t_ref[W, rows, :]
    ga, gb, ge = g * a, g * b, g * e
    gaa, gbb, gee = ga * a, gb * b, ge * e
    gs = gaa + gbb + gee
    terms = (g, ga, gb, ge, gs, gaa, gbb, ga * b, ga * e, gb * e, gs * a, gs * b, gs * e)
    return tuple(old + new for old, new in zip(acc, terms))


def write_moments(m_ref, x, acc):
    for field, value in enumerate(acc):
        m_ref[field, x : x + 1, :] = jnp.sum(value, axis=0, keepdims=True)


def moments_loop(m_ref, t_ref, width, groups, state_at):
    zero = tuple(jnp.zeros((SUB, LANES), jnp.float32) for _ in range(13))
    for x in range(width):

        def step(g, acc):
            rows = pl.ds(pl.multiple_of(g * SUB, SUB), SUB)
            return add_moments(acc, state_at(x, rows), t_ref, rows)

        write_moments(m_ref, x, lax.fori_loop(0, groups, step, zero, unroll=4))


def first_kernel(extent, v_ref, dist_ref, m_ref, t_ref, s_ref):
    count, width = dist_ref.shape[0], dist_ref.shape[1]
    columns = v_ref[...].T

    def wide(k):
        return jnp.broadcast_to(columns[:, k : k + 1], (count, LANES))

    a, b, e = wide(0), wide(1), wide(2)
    t_ref[A], t_ref[B], t_ref[E], t_ref[W] = a, b, e, wide(3)
    hb, he = 0.5 * jnp.abs(b), 0.5 * jnp.abs(e)
    t_ref[HB], t_ref[HE] = hb, he
    t_ref[BASE] = pseudo_rate + (hb + he) + jnp.abs(a) * extent
    t_ref[FA], t_ref[BA] = jnp.maximum(a, 0.0) * extent, jnp.maximum(-a, 0.0) * extent
    t_ref[REST] = (box_volume * (2.0 * math.pi) ** (-1.5)) * jnp.exp(-0.5 * (a * a + b * b + e * e))

    def state_at(x, rows):
        s = dist_ref[rows, x, :]
        s_ref[x, rows, :] = s
        return s

    moments_loop(m_ref, t_ref, width, count // SUB, state_at)


def gains_kernel(peers, me_ref, t_ref, rate_ref, rden_ref, p_ref, g_ref):
    width, count = rden_ref.shape[0], rden_ref.shape[1]
    me = me_ref[0]

    def step(g, carry):
        rows = pl.ds(pl.multiple_of(g * SUB, SUB), SUB)
        base, fa, ba = t_ref[BASE, rows, :], t_ref[FA, rows, :], t_ref[BA, rows, :]
        gain = fa + ba
        ahead = t_ref[A, rows, :] >= 0.0
        power = gain * gain
        power = power * power
        power = power * power if width == 8 else gain**width
        for d in range(peers):
            product = base + rate_ref[d ^ me, 0:1, :]
            for x in range(1, width):
                product = product * (base + rate_ref[d ^ me, x : x + 1, :])
            g_ref[d, rows, :] = power / product
        steps = []
        for x in range(width):
            rden = 1.0 / (base + rate_ref[0, x : x + 1, :])
            rden_ref[x, rows, :] = rden
            steps.append(gain * rden)
        up, down = [steps[0]], [steps[-1]]
        for x in range(1, width):
            up.append(up[-1] * steps[x])
            down.append(down[-1] * steps[width - 1 - x])
        for x in range(width):
            p_ref[x, rows, :] = jnp.where(ahead, up[x], down[width - 1 - x])
        return carry

    lax.fori_loop(0, count // SUB, step, 0)


def features_kernel(v_ref, f_ref):
    blocks = v_ref.shape[0]
    part = v_ref.shape[1] // 4
    for k in range(blocks):
        a, b, e, w = (v_ref[k, i * part : (i + 1) * part, :] for i in range(4))
        sides = [split(value) for value in (a, b, e, a * a + b * b + e * e)]
        one, zero = jnp.ones_like(a), jnp.zeros_like(a)
        rows = [side[i] for side in sides for i, _ in PAIRS] + [one] * 3 + split(jnp.log2(w))
        rows = rows + [zero] * (FEATURES - len(rows))
        for i, row in enumerate(rows):
            f_ref[i, k * part : (k + 1) * part, :] = row


def split(value):
    parts = []
    for _ in range(3):
        part = value.astype(jnp.bfloat16).astype(jnp.float32)
        parts.append(part)
        value = value - part
    return parts


def lane_z():
    return lax.broadcasted_iota(jnp.int32, (1, LANES), 1) % NZ


def y_less(v):
    return pltpu.roll(v, NZ, 1)


def y_more(v):
    return pltpu.roll(v, LANES - NZ, 1)


def z_less(v):
    return jnp.where(lane_z() == 0, pltpu.roll(v, LANES - NZ + 1, 1), pltpu.roll(v, 1, 1))


def z_more(v):
    return jnp.where(lane_z() == NZ - 1, pltpu.roll(v, NZ - 1, 1), pltpu.roll(v, LANES - 1, 1))


def dy(v):
    return 0.5 * (y_more(v) - y_less(v))


def dz(v):
    return 0.5 * (z_more(v) - z_less(v))


def x_less(v):
    return pltpu.roll(v, 1, 0)


def x_more(v):
    return pltpu.roll(v, v.shape[0] - 1, 0)


def fields_of(m):
    rho = m[0]
    inverse = 1.0 / rho
    u = [m[1 + i] * inverse for i in range(3)]
    square = u[0] * u[0] + u[1] * u[1] + u[2] * u[2]
    warm = (m[4] * inverse - square) * (1.0 / 3.0)
    force = rho * warm
    second = [[m[5], m[7], m[8]], [m[7], m[6], m[9]], [m[8], m[9], m[4] - m[5] - m[6]]]
    xx = second[0][0] - rho * u[0] * u[0] - force
    yy = second[1][1] - rho * u[1] * u[1] - force
    xy = second[0][1] - rho * u[0] * u[1]
    xz = second[0][2] - rho * u[0] * u[2]
    yz = second[1][2] - rho * u[1] * u[2]
    heat = []
    for i in range(3):
        inner = u[0] * second[i][0] + u[1] * second[i][1] + u[2] * second[i][2]
        heat.append(0.5 * (m[10 + i] - 2.0 * inner - u[i] * m[4] + 2.0 * rho * u[i] * square))
    return rho, inverse, u, warm, (xx, yy, xy, xz, yz), heat


def correction(rho, inverse, u, warm, stress, heat, inside):
    xx, yy, xy, xz, yz = stress
    zz = -(xx + yy)

    def dx(v):
        v = jnp.where(inside, v, 0.0)
        return 0.5 * (x_more(v) - x_less(v))

    source = [
        dx(rho * u[0]) + dy(rho * u[1]) + dz(rho * u[2]),
        dx(xx) + dy(xy) + dz(xz),
        dx(xy) + dy(yy) + dz(yz),
        dx(xz) + dy(yz) + dz(zz),
        dx(heat[0]) + dy(heat[1]) + dz(heat[2]),
    ]
    scale = [-source_gain * inverse] * 4 + [(-source_gain * 2.0 / 3.0) / (rho * warm)]
    source = [jnp.where(inside, s * c, 0.0) for s, c in zip(source, scale)]
    delta = source
    for _ in range(JACOBI):
        fresh = []
        for mu, s, d in zip(diffusion, source, delta):
            beside = x_less(d) + x_more(d) + y_less(d) + y_more(d) + z_less(d) + z_more(d)
            fresh.append(jnp.where(inside, (s + mu * beside) * (1.0 / (1.0 + 6.0 * mu)), 0.0))
        delta = fresh
    return delta


def kinetic_kernel(
    peers, me_ref, before_ref, m_ref, after_ref, f_ref, t_ref, rate_ref, wall_ref, state_ref, rden_ref,
    s_ref, c_ref, macro_ref, pad_ref, cell_ref, field_ref, total_ref,
):
    width, count = s_ref.shape[0], s_ref.shape[1]
    me = me_ref[0]
    tall = width + 2 * SUB
    own = slice(SUB, SUB + width)
    pad_ref[...] = jnp.ones_like(pad_ref)
    for k in range(13):
        pad_ref[k, SUB - HALO : SUB, :] = before_ref[k]
        pad_ref[k, own, :] = m_ref[k]
        pad_ref[k, SUB + width : SUB + width + HALO, :] = after_ref[k]
    row = lax.broadcasted_iota(jnp.int32, (tall, LANES), 0) + (me * width - SUB)
    inside = (row >= 0) & (row < peers * width)
    rho, inverse, u, warm, stress, heat = fields_of([pad_ref[k] for k in range(13)])
    delta = correction(rho, inverse, u, warm, stress, heat, inside)
    for k, value in enumerate(
        (rho * jnp.exp(delta[0]), u[0] + delta[1], u[1] + delta[2], u[2] + delta[3], warm * jnp.exp(delta[4]))
    ):
        pad_ref[k] = value
        macro_ref[k] = pad_ref[k, own, :]
    for k in range(3):
        pad_ref[5 + k] = heat[k]
    R, U, T = macro_ref[0], [macro_ref[1 + k] for k in range(3)], macro_ref[4]
    q = [pad_ref[5 + k, own, :] for k in range(3)]
    cold = 1.0 / T
    beta = (-0.5 * LOG2E) * cold
    alpha = [(LOG2E * cold) * U[k] for k in range(3)]
    gamma = beta * (U[0] * U[0] + U[1] * U[1] + U[2] * U[2])
    rows = [side[j] for side in (split(v) for v in (*alpha, beta)) for _, j in PAIRS]
    rows = rows + split(gamma) + [jnp.ones_like(T)] * 3
    rows = rows + [jnp.zeros_like(T)] * (FEATURES - len(rows))
    for i, value in enumerate(rows):
        for x in range(width):
            cell_ref[i : i + 1, x * LANES : (x + 1) * LANES] = value[x : x + 1, :]
    cells = cell_ref[...].astype(jnp.bfloat16)

    def mass(r, acc):
        some = f_ref[:, r, :].astype(jnp.bfloat16)
        power = lax.dot_general(some, cells, (((0,), (0,)), ((), ())), preferred_element_type=jnp.float32)
        weight = jnp.exp2(power)
        return acc + jnp.sum(weight.reshape(LANES // SUB, SUB, width * LANES), axis=0)

    acc = lax.fori_loop(0, f_ref.shape[1], mass, jnp.zeros((SUB, width * LANES), jnp.float32))
    acc = jnp.sum(acc, axis=0, keepdims=True)
    for x in range(width):
        total_ref[x : x + 1, :] = acc[:, x * LANES : (x + 1) * LANES]
    wall, rate = wall_ref[...], rate_ref[...]
    third = (1.0 - viscous_conduction_ratio) / (5.0 * R * T * T)
    values = [*U, beta, *(v * third for v in q), cold]
    values += [(1.0 - wall) * R * rate / total_ref[...], wall * R * rate]
    for k, value in enumerate(values):
        field_ref[k] = value

    for x in range(width):
        ux, uy, uz, power, qx, qy, qz, inv, maxwell, rest = (
            jnp.broadcast_to(field_ref[k, x : x + 1, :], (SUB, LANES)) for k in range(10)
        )

        def ahead(g, carry):
            rows = pl.ds(pl.multiple_of(g * SUB, SUB), SUB)
            a, b, e = (t_ref[k, rows, :] for k in (A, B, E))
            s = state_ref[x, rows, :]
            cx, cy, cz = a - ux, b - uy, e - uz
            square = cx * cx + cy * cy + cz * cz
            expo = jnp.exp2(square * power)
            flux = cx * qx + cy * qy + cz * qz
            target = (expo * maxwell) * (1.0 + flux * (square * inv - 5.0)) + rest * t_ref[REST, rows, :]
            driving = pseudo_rate * s + t_ref[HB, rows, :] * jnp.where(b > 0.0, y_less(s), y_more(s))
            driving = driving + t_ref[HE, rows, :] * jnp.where(e > 0.0, z_less(s), z_more(s))
            rden = rden_ref[x, rows, :]
            value = (driving + target) * rden
            if x:
                value = value + (t_ref[FA, rows, :] * rden) * s_ref[x - 1, rows, :]
            s_ref[x, rows, :] = value
            return carry

        lax.fori_loop(0, count // SUB, ahead, 0, unroll=2)

    def back(g, carry):
        rows = pl.ds(pl.multiple_of(g * SUB, SUB), SUB)
        ba = t_ref[BA, rows, :]
        value = s_ref[width - 1, rows, :]
        last = value
        for x in range(width - 2, -1, -1):
            value = s_ref[x, rows, :] + (ba * rden_ref[x, rows, :]) * value
            s_ref[x, rows, :] = value
        c_ref[rows, :] = jnp.where(t_ref[A, rows, :] >= 0.0, last, value)
        return carry

    lax.fori_loop(0, count // SUB, back, 0, unroll=2)


def entering(peers, me, t_ref, c_ref, g_ref, flow_ref, enter_ref):
    count = enter_ref.shape[0]

    def step(g, carry):
        rows = pl.ds(pl.multiple_of(g * SUB, SUB), SUB)
        up, down = flow_ref[0, rows, :], flow_ref[1, rows, :]
        for d in range(peers - 1):
            up = jnp.where(d < me, g_ref[d, rows, :] * up + c_ref[d ^ me, rows, :], up)
        for d in range(peers - 1, 0, -1):
            down = jnp.where(d > me, g_ref[d, rows, :] * down + c_ref[d ^ me, rows, :], down)
        enter_ref[rows, :] = jnp.where(t_ref[A, rows, :] >= 0.0, up, down)
        return carry

    lax.fori_loop(0, count // SUB, step, 0, unroll=2)


def next_kernel(peers, me_ref, t_ref, c_ref, g_ref, flow_ref, s_ref, p_ref, m_ref, state_ref, enter_ref):
    width, count = s_ref.shape[0], s_ref.shape[1]
    entering(peers, me_ref[0], t_ref, c_ref, g_ref, flow_ref, enter_ref)

    def state_at(x, rows):
        s = s_ref[x, rows, :] + p_ref[x, rows, :] * enter_ref[rows, :]
        state_ref[x, rows, :] = s
        return s

    moments_loop(m_ref, t_ref, width, count // SUB, state_at)


def last_kernel(peers, me_ref, t_ref, c_ref, g_ref, flow_ref, s_ref, p_ref, out_ref, enter_ref):
    width, count = s_ref.shape[0], s_ref.shape[1]
    entering(peers, me_ref[0], t_ref, c_ref, g_ref, flow_ref, enter_ref)

    def step(g, carry):
        rows = pl.ds(pl.multiple_of(g * SUB, SUB), SUB)
        enter = enter_ref[rows, :]
        for x in range(width):
            out_ref[rows, x, :] = s_ref[x, rows, :] + p_ref[x, rows, :] * enter
        return carry

    lax.fori_loop(0, count // SUB, step, 0, unroll=2)


def stages(size):
    found, stride = [], 1
    while size > 1:
        factor = next(f for f in range(2, size + 1) if size % f == 0)
        if factor == 2 and size % 4 == 0 and (stride > 1 or size % 8):
            factor = 4
        found.append((factor, stride))
        size, stride = size // factor, stride * factor
    return found


def reduce_over(axis, value, extra=None):
    size = lax.axis_size(axis)
    rows = value.shape[0]
    for factor, stride in stages(size):
        sent = value if extra is None else jnp.concatenate([value, extra.reshape(-1, LANES)])
        got = []
        for turn in range(1, factor):
            pairs = []
            for i in range(size):
                digit = i // stride % factor
                pairs.append((i, i + ((digit + turn) % factor - digit) * stride))
            got.append(lax.ppermute(sent, axis, pairs))
        for piece in got:
            value = value + piece[:rows]
        if extra is not None:
            shape = (-1,) + extra.shape[1:]
            extra = jnp.concatenate([extra] + [piece[rows:].reshape(shape) for piece in got])
    return value, extra


def gather_over(axis, value):
    size = lax.axis_size(axis)
    blocks = value[None]
    order = [0]
    bit = size // 2
    while bit:
        got = lax.ppermute(blocks, axis, [(i, i ^ bit) for i in range(size)])
        blocks = jnp.concatenate([blocks, got])
        order = order + [k ^ bit for k in order]
        bit //= 2
    return jnp.concatenate([blocks[order.index(k)][None] for k in range(size)])


def neighbours(axis, value, width):
    size, me = lax.axis_size(axis), lax.axis_index(axis)
    odd = me % 2 == 1
    first, last = value[:, :width], value[:, value.shape[1] - width :]
    near = [(i, i ^ 1) for i in range(size)]
    far = [(i, i + 1) for i in range(1, size - 1, 2)]
    near = lax.ppermute(jnp.where(odd, first, last), axis, near)
    far = lax.ppermute(jnp.where(odd, last, first), axis, far + [(j, i) for i, j in far])
    return jnp.where(odd, near, far), jnp.where(odd, far, near)


def per_device(distribution, velocity, weights, collision, solid, inflow):
    count, width, cells = distribution.shape
    peers = lax.axis_size("gx")
    me = lax.axis_index("gx").astype(jnp.int32).reshape(1)
    wall = solid.astype(jnp.float32)
    rate = collision + wall_rate * wall
    rates = gather_over("gx", rate)
    vw = jnp.concatenate([velocity, weights[None]])
    smem = pl.BlockSpec(memory_space=pltpu.SMEM)
    vmem = pl.BlockSpec(memory_space=pltpu.VMEM)

    def run(kernel, out_shape, args, scratch=(), scalar=True):
        return pl.pallas_call(
            kernel,
            out_shape=out_shape,
            in_specs=([smem] if scalar else []) + [vmem] * (len(args) - (1 if scalar else 0)),
            out_specs=jax.tree.map(lambda _: vmem, out_shape),
            scratch_shapes=scratch,
            compiler_params=pltpu.CompilerParams(vmem_limit_bytes=32 * 1024 * 1024),
        )(*args)

    padded = jnp.concatenate([vw, jnp.zeros((4, count), jnp.float32)])
    m, table, state = run(
        functools.partial(first_kernel, float(width * peers)),
        (f32(13, width, cells), f32(TABLE, count, cells), f32(width, count, cells)),
        (padded, distribution),
        scalar=False,
    )
    extra = vw.reshape(1, 4 * count // LANES, LANES)
    rden, prefix, gains = run(
        functools.partial(gains_kernel, peers),
        (f32(width, count, cells), f32(width, count, cells), f32(peers, count, cells)),
        (me, table, rates),
    )
    for repeat in range(ITERS):
        m, extra = reduce_over("vel", m.reshape(13 * width, cells), extra)
        m = m.reshape(13, width, cells)
        if repeat == 0:
            everyone = f32(FEATURES, extra.shape[0] * extra.shape[1] // 4, LANES)
            features = run(features_kernel, everyone, (extra,), scalar=False)
            extra = None
        before, after = neighbours("gx", m, HALO)
        local, carry, macro = run(
            functools.partial(kinetic_kernel, peers),
            (f32(width, count, cells), f32(count, cells), f32(5, width, cells)),
            (me, before, m, after, features, table, rate, wall, state, rden),
            scratch=(
                pltpu.VMEM((13, width + 2 * SUB, cells), jnp.float32),
                pltpu.VMEM((FEATURES, width * cells), jnp.float32),
                pltpu.VMEM((10, width, cells), jnp.float32),
                pltpu.VMEM((width, cells), jnp.float32),
            ),
        )
        carries = gather_over("gx", carry)
        args = (me, table, carries, gains, inflow, local, prefix)
        scratch = (pltpu.VMEM((count, cells), jnp.float32),)
        if repeat < ITERS - 1:
            m, state = run(
                functools.partial(next_kernel, peers),
                (f32(13, width, cells), f32(width, count, cells)),
                args,
                scratch,
            )
        else:
            state = run(functools.partial(last_kernel, peers), f32(count, width, cells), args, scratch)
    return state, macro


def solution(mesh):
    return jax.shard_map(
        per_device,
        mesh=mesh,
        in_specs=(
            P("vel", "gx", None),
            P(None, "vel"),
            P("vel"),
            P("gx", None),
            P("gx", None),
            P(None, "vel", None),
        ),
        out_specs=(P("vel", "gx", None), P(None, "gx", None)),
        check_vma=False,
    )
```

```python
import functools
import math

import jax
import jax.numpy as jnp
from jax import lax
from jax.experimental import pallas as pl
from jax.experimental.pallas import tpu as pltpu
from jax.sharding import PartitionSpec as P

NY = 16
NZ = 8
ITERS = 2
JACOBI = 2
HALO = JACOBI + 1
pseudo_rate = 0.5
source_gain = 0.5
diffusion = (0.6, 0.8, 0.8, 0.8, 1.0)
viscous_conduction_ratio = 2.0 / 3.0
wall_rate = 4.0
box_volume = 216.0
LOG2E = math.log2(math.e)
LANES = 128
SUB = 8
PAIRS = ((0, 0), (0, 1), (1, 0), (0, 2), (2, 0), (1, 1))
FEATURES = 32
A, B, E, W, HB, HE, BASE, FA, BA, REST = range(10)
TABLE = 10


def f32(*shape):
    return jax.ShapeDtypeStruct(shape, jnp.float32)


def add_moments(acc, s, t_ref, rows):
    a, b, e = (t_ref[k, rows, :] for k in (A, B, E))
    g = s * t_ref[W, rows, :]
    ga, gb, ge = g * a, g * b, g * e
    gaa, gbb, gee = ga * a, gb * b, ge * e
    gs = gaa + gbb + gee
    terms = (g, ga, gb, ge, gs, gaa, gbb, ga * b, ga * e, gb * e, gs * a, gs * b, gs * e)
    return tuple(old + new for old, new in zip(acc, terms))


def write_moments(m_ref, x, acc):
    for field, value in enumerate(acc):
        m_ref[field, x : x + 1, :] = jnp.sum(value, axis=0, keepdims=True)


def moments_loop(m_ref, t_ref, width, groups, state_at):
    zero = tuple(jnp.zeros((SUB, LANES), jnp.float32) for _ in range(13))
    for x in range(width):

        def step(g, acc):
            rows = pl.ds(pl.multiple_of(g * SUB, SUB), SUB)
            return add_moments(acc, state_at(x, rows), t_ref, rows)

        write_moments(m_ref, x, lax.fori_loop(0, groups, step, zero, unroll=4))


def first_kernel(extent, v_ref, dist_ref, m_ref, t_ref, s_ref):
    count, width = dist_ref.shape[0], dist_ref.shape[1]
    columns = v_ref[...].T

    def wide(k):
        return jnp.broadcast_to(columns[:, k : k + 1], (count, LANES))

    a, b, e = wide(0), wide(1), wide(2)
    t_ref[A], t_ref[B], t_ref[E], t_ref[W] = a, b, e, wide(3)
    hb, he = 0.5 * jnp.abs(b), 0.5 * jnp.abs(e)
    t_ref[HB], t_ref[HE] = hb, he
    t_ref[BASE] = pseudo_rate + (hb + he) + jnp.abs(a) * extent
    t_ref[FA], t_ref[BA] = jnp.maximum(a, 0.0) * extent, jnp.maximum(-a, 0.0) * extent
    t_ref[REST] = (box_volume * (2.0 * math.pi) ** (-1.5)) * jnp.exp(-0.5 * (a * a + b * b + e * e))

    def state_at(x, rows):
        s = dist_ref[rows, x, :]
        s_ref[x, rows, :] = s
        return s

    moments_loop(m_ref, t_ref, width, count // SUB, state_at)


def gains_kernel(peers, me_ref, t_ref, rate_ref, rden_ref, p_ref, g_ref):
    width, count = rden_ref.shape[0], rden_ref.shape[1]
    me = me_ref[0]

    def step(g, carry):
        rows = pl.ds(pl.multiple_of(g * SUB, SUB), SUB)
        base, fa, ba = t_ref[BASE, rows, :], t_ref[FA, rows, :], t_ref[BA, rows, :]
        gain = fa + ba
        ahead = t_ref[A, rows, :] >= 0.0
        power = gain * gain
        power = power * power
        power = power * power if width == 8 else gain**width
        for d in range(peers):
            product = base + rate_ref[d ^ me, 0:1, :]
            for x in range(1, width):
                product = product * (base + rate_ref[d ^ me, x : x + 1, :])
            g_ref[d, rows, :] = power / product
        steps = []
        for x in range(width):
            rden = 1.0 / (base + rate_ref[0, x : x + 1, :])
            rden_ref[x, rows, :] = rden
            steps.append(gain * rden)
        up, down = [steps[0]], [steps[-1]]
        for x in range(1, width):
            up.append(up[-1] * steps[x])
            down.append(down[-1] * steps[width - 1 - x])
        for x in range(width):
            p_ref[x, rows, :] = jnp.where(ahead, up[x], down[width - 1 - x])
        return carry

    lax.fori_loop(0, count // SUB, step, 0)


def features_kernel(v_ref, f_ref, row_ref):
    blocks = v_ref.shape[0]
    part = v_ref.shape[1] // 4
    for k in range(blocks):
        a, b, e, w = (v_ref[k, i * part : (i + 1) * part, :] for i in range(4))
        sides = [split(value) for value in (a, b, e, a * a + b * b + e * e)]
        one, zero = jnp.ones_like(a), jnp.zeros_like(a)
        rows = [side[i] for side in sides for i, _ in PAIRS] + [one] * 3 + split(jnp.log2(w))
        rows = rows + [zero] * (FEATURES - len(rows))
        for i, row in enumerate(rows):
            for j in range(part):
                row_ref[k * part + j, i : i + 1, :] = row[j : j + 1, :]

    def turn(r, carry):
        where = pl.ds(pl.multiple_of(r * LANES, LANES), LANES)
        f_ref[where, :] = row_ref[r].T.astype(jnp.bfloat16)
        return carry

    lax.fori_loop(0, blocks * part, turn, 0, unroll=4)


def split(value):
    parts = []
    for _ in range(3):
        part = value.astype(jnp.bfloat16).astype(jnp.float32)
        parts.append(part)
        value = value - part
    return parts


def lane_z():
    return lax.broadcasted_iota(jnp.int32, (1, LANES), 1) % NZ


def y_less(v):
    return pltpu.roll(v, NZ, 1)


def y_more(v):
    return pltpu.roll(v, LANES - NZ, 1)


def z_less(v):
    return jnp.where(lane_z() == 0, pltpu.roll(v, LANES - NZ + 1, 1), pltpu.roll(v, 1, 1))


def z_more(v):
    return jnp.where(lane_z() == NZ - 1, pltpu.roll(v, NZ - 1, 1), pltpu.roll(v, LANES - 1, 1))


def dy(v):
    return 0.5 * (y_more(v) - y_less(v))


def dz(v):
    return 0.5 * (z_more(v) - z_less(v))


def x_less(v):
    return pltpu.roll(v, 1, 0)


def x_more(v):
    return pltpu.roll(v, v.shape[0] - 1, 0)


def fields_of(m):
    rho = m[0]
    inverse = 1.0 / rho
    u = [m[1 + i] * inverse for i in range(3)]
    square = u[0] * u[0] + u[1] * u[1] + u[2] * u[2]
    warm = (m[4] * inverse - square) * (1.0 / 3.0)
    force = rho * warm
    second = [[m[5], m[7], m[8]], [m[7], m[6], m[9]], [m[8], m[9], m[4] - m[5] - m[6]]]
    xx = second[0][0] - rho * u[0] * u[0] - force
    yy = second[1][1] - rho * u[1] * u[1] - force
    xy = second[0][1] - rho * u[0] * u[1]
    xz = second[0][2] - rho * u[0] * u[2]
    yz = second[1][2] - rho * u[1] * u[2]
    heat = []
    for i in range(3):
        inner = u[0] * second[i][0] + u[1] * second[i][1] + u[2] * second[i][2]
        heat.append(0.5 * (m[10 + i] - 2.0 * inner - u[i] * m[4] + 2.0 * rho * u[i] * square))
    return rho, inverse, u, warm, (xx, yy, xy, xz, yz), heat


def correction(rho, inverse, u, warm, stress, heat, inside):
    xx, yy, xy, xz, yz = stress
    zz = -(xx + yy)

    def dx(v):
        v = jnp.where(inside, v, 0.0)
        return 0.5 * (x_more(v) - x_less(v))

    source = [
        dx(rho * u[0]) + dy(rho * u[1]) + dz(rho * u[2]),
        dx(xx) + dy(xy) + dz(xz),
        dx(xy) + dy(yy) + dz(yz),
        dx(xz) + dy(yz) + dz(zz),
        dx(heat[0]) + dy(heat[1]) + dz(heat[2]),
    ]
    scale = [-source_gain * inverse] * 4 + [(-source_gain * 2.0 / 3.0) / (rho * warm)]
    source = [jnp.where(inside, s * c, 0.0) for s, c in zip(source, scale)]
    delta = source
    for _ in range(JACOBI):
        fresh = []
        for mu, s, d in zip(diffusion, source, delta):
            beside = x_less(d) + x_more(d) + y_less(d) + y_more(d) + z_less(d) + z_more(d)
            fresh.append(jnp.where(inside, (s + mu * beside) * (1.0 / (1.0 + 6.0 * mu)), 0.0))
        delta = fresh
    return delta


def transport_kernel(t_ref, s_ref, drive_ref):
    width, count = s_ref.shape[0], s_ref.shape[1]
    lane = lax.broadcasted_iota(jnp.int32, (SUB, LANES), 1)
    z = lane % NZ
    y_down, y_up = (lane + LANES - NZ) % LANES, (lane + NZ) % LANES
    z_down, z_up = lane - z + (z + NZ - 1) % NZ, lane - z + (z + 1) % NZ

    def step(g, carry):
        rows = pl.ds(pl.multiple_of(g * SUB, SUB), SUB)
        hb, he = t_ref[HB, rows, :], t_ref[HE, rows, :]
        from_y = jnp.where(t_ref[B, rows, :] > 0.0, y_down, y_up)
        from_z = jnp.where(t_ref[E, rows, :] > 0.0, z_down, z_up)
        for x in range(width):
            s = s_ref[x, rows, :]
            sy = jnp.take_along_axis(s, from_y, axis=1, mode="promise_in_bounds")
            sz = jnp.take_along_axis(s, from_z, axis=1, mode="promise_in_bounds")
            drive_ref[x, rows, :] = pseudo_rate * s + hb * sy + he * sz
        return carry

    lax.fori_loop(0, count // SUB, step, 0, unroll=8)


def kinetic_kernel(
    peers, me_ref, before_ref, m_ref, after_ref, f_ref, t_ref, rate_ref, wall_ref, drive_ref, rden_ref,
    s_ref, c_ref, macro_ref, pad_ref, cell_ref, field_ref, total_ref,
):
    width, count = s_ref.shape[0], s_ref.shape[1]
    me = me_ref[0]
    tall = width + 2 * SUB
    own = slice(SUB, SUB + width)
    pad_ref[...] = jnp.ones_like(pad_ref)
    for k in range(13):
        pad_ref[k, SUB - HALO : SUB, :] = before_ref[k]
        pad_ref[k, own, :] = m_ref[k]
        pad_ref[k, SUB + width : SUB + width + HALO, :] = after_ref[k]
    row = lax.broadcasted_iota(jnp.int32, (tall, LANES), 0) + (me * width - SUB)
    inside = (row >= 0) & (row < peers * width)
    rho, inverse, u, warm, stress, heat = fields_of([pad_ref[k] for k in range(13)])
    delta = correction(rho, inverse, u, warm, stress, heat, inside)
    for k, value in enumerate(
        (rho * jnp.exp(delta[0]), u[0] + delta[1], u[1] + delta[2], u[2] + delta[3], warm * jnp.exp(delta[4]))
    ):
        pad_ref[k] = value
        macro_ref[k] = pad_ref[k, own, :]
    for k in range(3):
        pad_ref[5 + k] = heat[k]
    R, U, T = macro_ref[0], [macro_ref[1 + k] for k in range(3)], macro_ref[4]
    q = [pad_ref[5 + k, own, :] for k in range(3)]
    cold = 1.0 / T
    beta = (-0.5 * LOG2E) * cold
    alpha = [(LOG2E * cold) * U[k] for k in range(3)]
    gamma = beta * (U[0] * U[0] + U[1] * U[1] + U[2] * U[2])
    rows = [side[j] for side in (split(v) for v in (*alpha, beta)) for _, j in PAIRS]
    rows = rows + split(gamma) + [jnp.ones_like(T)] * 3
    rows = rows + [jnp.zeros_like(T)] * (FEATURES - len(rows))
    for i, value in enumerate(rows):
        for x in range(width):
            cell_ref[i : i + 1, x * LANES : (x + 1) * LANES] = value[x : x + 1, :]
    cells = cell_ref[...].astype(jnp.bfloat16)

    def mass(r, acc):
        some = f_ref[pl.ds(pl.multiple_of(r * LANES, LANES), LANES), :]
        power = jnp.dot(some, cells, preferred_element_type=jnp.float32)
        weight = jnp.exp2(power)
        return acc + jnp.sum(weight.reshape(LANES // SUB, SUB, width * LANES), axis=0)

    acc = lax.fori_loop(0, f_ref.shape[0] // LANES, mass, jnp.zeros((SUB, width * LANES), jnp.float32), unroll=8)
    acc = jnp.sum(acc, axis=0, keepdims=True)
    for x in range(width):
        total_ref[x : x + 1, :] = acc[:, x * LANES : (x + 1) * LANES]
    wall, rate = wall_ref[...], rate_ref[...]
    third = (1.0 - viscous_conduction_ratio) / (5.0 * R * T * T)
    values = [*U, beta, *(v * third for v in q), cold]
    values += [(1.0 - wall) * R * rate / total_ref[...], wall * R * rate]
    for k, value in enumerate(values):
        field_ref[k] = value

    for x in range(width):
        ux, uy, uz, power, qx, qy, qz, inv, maxwell, rest = (
            jnp.broadcast_to(field_ref[k, x : x + 1, :], (SUB, LANES)) for k in range(10)
        )

        def ahead(g, carry):
            rows = pl.ds(pl.multiple_of(g * SUB, SUB), SUB)
            a, b, e = (t_ref[k, rows, :] for k in (A, B, E))
            cx, cy, cz = a - ux, b - uy, e - uz
            square = cx * cx + cy * cy + cz * cz
            expo = jnp.exp2(square * power)
            flux = cx * qx + cy * qy + cz * qz
            target = (expo * maxwell) * (1.0 + flux * (square * inv - 5.0)) + rest * t_ref[REST, rows, :]
            rden = rden_ref[x, rows, :]
            value = (drive_ref[x, rows, :] + target) * rden
            if x:
                value = value + (t_ref[FA, rows, :] * rden) * s_ref[x - 1, rows, :]
            s_ref[x, rows, :] = value
            return carry

        lax.fori_loop(0, count // SUB, ahead, 0, unroll=16)

    def back(g, carry):
        rows = pl.ds(pl.multiple_of(g * SUB, SUB), SUB)
        ba = t_ref[BA, rows, :]
        value = s_ref[width - 1, rows, :]
        last = value
        for x in range(width - 2, -1, -1):
            value = s_ref[x, rows, :] + (ba * rden_ref[x, rows, :]) * value
            s_ref[x, rows, :] = value
        c_ref[rows, :] = jnp.where(t_ref[A, rows, :] >= 0.0, last, value)
        return carry

    lax.fori_loop(0, count // SUB, back, 0, unroll=4)


def entering(peers, me, t_ref, c_ref, g_ref, flow_ref, enter_ref):
    count = enter_ref.shape[0]

    def step(g, carry):
        rows = pl.ds(pl.multiple_of(g * SUB, SUB), SUB)
        up, down = flow_ref[0, rows, :], flow_ref[1, rows, :]
        for d in range(peers - 1):
            up = jnp.where(d < me, g_ref[d, rows, :] * up + c_ref[d ^ me, rows, :], up)
        for d in range(peers - 1, 0, -1):
            down = jnp.where(d > me, g_ref[d, rows, :] * down + c_ref[d ^ me, rows, :], down)
        enter_ref[rows, :] = jnp.where(t_ref[A, rows, :] >= 0.0, up, down)
        return carry

    lax.fori_loop(0, count // SUB, step, 0, unroll=2)


def next_kernel(peers, me_ref, t_ref, c_ref, g_ref, flow_ref, s_ref, p_ref, m_ref, state_ref, enter_ref):
    width, count = s_ref.shape[0], s_ref.shape[1]
    entering(peers, me_ref[0], t_ref, c_ref, g_ref, flow_ref, enter_ref)

    def state_at(x, rows):
        s = s_ref[x, rows, :] + p_ref[x, rows, :] * enter_ref[rows, :]
        state_ref[x, rows, :] = s
        return s

    moments_loop(m_ref, t_ref, width, count // SUB, state_at)


def last_kernel(peers, me_ref, t_ref, c_ref, g_ref, flow_ref, s_ref, p_ref, out_ref, enter_ref):
    width, count = s_ref.shape[0], s_ref.shape[1]
    entering(peers, me_ref[0], t_ref, c_ref, g_ref, flow_ref, enter_ref)

    def step(g, carry):
        rows = pl.ds(pl.multiple_of(g * SUB, SUB), SUB)
        enter = enter_ref[rows, :]
        for x in range(width):
            out_ref[rows, x, :] = s_ref[x, rows, :] + p_ref[x, rows, :] * enter
        return carry

    lax.fori_loop(0, count // SUB, step, 0, unroll=2)


def stages(size):
    found, stride = [], 1
    while size > 1:
        factor = next(f for f in range(2, size + 1) if size % f == 0)
        if factor == 2 and size % 4 == 0 and (stride > 1 or size % 8):
            factor = 4
        found.append((factor, stride))
        size, stride = size // factor, stride * factor
    return found


def reduce_over(axis, value, extra=None):
    size = lax.axis_size(axis)
    rows = value.shape[0]
    for factor, stride in stages(size):
        sent = value if extra is None else jnp.concatenate([value, extra.reshape(-1, LANES)])
        got = []
        for turn in range(1, factor):
            pairs = []
            for i in range(size):
                digit = i // stride % factor
                pairs.append((i, i + ((digit + turn) % factor - digit) * stride))
            got.append(lax.ppermute(sent, axis, pairs))
        for piece in got:
            value = value + piece[:rows]
        if extra is not None:
            shape = (-1,) + extra.shape[1:]
            extra = jnp.concatenate([extra] + [piece[rows:].reshape(shape) for piece in got])
    return value, extra


def gather_over(axis, value):
    size = lax.axis_size(axis)
    blocks = value[None]
    order = [0]
    bit = size // 2
    while bit:
        got = lax.ppermute(blocks, axis, [(i, i ^ bit) for i in range(size)])
        blocks = jnp.concatenate([blocks, got])
        order = order + [k ^ bit for k in order]
        bit //= 2
    return jnp.concatenate([blocks[order.index(k)][None] for k in range(size)])


def neighbours(axis, value, width):
    size, me = lax.axis_size(axis), lax.axis_index(axis)
    odd = me % 2 == 1
    first, last = value[:, :width], value[:, value.shape[1] - width :]
    near = [(i, i ^ 1) for i in range(size)]
    far = [(i, i + 1) for i in range(1, size - 1, 2)]
    near = lax.ppermute(jnp.where(odd, first, last), axis, near)
    far = lax.ppermute(jnp.where(odd, last, first), axis, far + [(j, i) for i, j in far])
    return jnp.where(odd, near, far), jnp.where(odd, far, near)


def per_device(distribution, velocity, weights, collision, solid, inflow):
    count, width, cells = distribution.shape
    peers = lax.axis_size("gx")
    me = lax.axis_index("gx").astype(jnp.int32).reshape(1)
    wall = solid.astype(jnp.float32)
    rate = collision + wall_rate * wall
    rates = gather_over("gx", rate)
    vw = jnp.concatenate([velocity, weights[None]])
    smem = pl.BlockSpec(memory_space=pltpu.SMEM)
    vmem = pl.BlockSpec(memory_space=pltpu.VMEM)

    def run(kernel, out_shape, args, scratch=(), scalar=True):
        return pl.pallas_call(
            kernel,
            out_shape=out_shape,
            in_specs=([smem] if scalar else []) + [vmem] * (len(args) - (1 if scalar else 0)),
            out_specs=jax.tree.map(lambda _: vmem, out_shape),
            scratch_shapes=scratch,
            compiler_params=pltpu.CompilerParams(vmem_limit_bytes=32 * 1024 * 1024),
        )(*args)

    padded = jnp.concatenate([vw, jnp.zeros((4, count), jnp.float32)])
    m, table, state = run(
        functools.partial(first_kernel, float(width * peers)),
        (f32(13, width, cells), f32(TABLE, count, cells), f32(width, count, cells)),
        (padded, distribution),
        scalar=False,
    )
    extra = vw.reshape(1, 4 * count // LANES, LANES)
    rden, prefix, gains = run(
        functools.partial(gains_kernel, peers),
        (f32(width, count, cells), f32(width, count, cells), f32(peers, count, cells)),
        (me, table, rates),
    )
    for repeat in range(ITERS):
        m, extra = reduce_over("vel", m.reshape(13 * width, cells), extra)
        m = m.reshape(13, width, cells)
        if repeat == 0:
            lines = extra.shape[0] * extra.shape[1] // 4
            features = run(
                features_kernel,
                jax.ShapeDtypeStruct((lines * LANES, FEATURES), jnp.bfloat16),
                (extra,),
                scratch=(pltpu.VMEM((lines, FEATURES, LANES), jnp.float32),),
                scalar=False,
            )
            extra = None
        drive = run(transport_kernel, f32(width, count, cells), (table, state), scalar=False)
        before, after = neighbours("gx", m, HALO)
        local, carry, macro = run(
            functools.partial(kinetic_kernel, peers),
            (f32(width, count, cells), f32(count, cells), f32(5, width, cells)),
            (me, before, m, after, features, table, rate, wall, drive, rden),
            scratch=(
                pltpu.VMEM((13, width + 2 * SUB, cells), jnp.float32),
                pltpu.VMEM((FEATURES, width * cells), jnp.float32),
                pltpu.VMEM((10, width, cells), jnp.float32),
                pltpu.VMEM((width, cells), jnp.float32),
            ),
        )
        carries = gather_over("gx", carry)
        args = (me, table, carries, gains, inflow, local, prefix)
        scratch = (pltpu.VMEM((count, cells), jnp.float32),)
        if repeat < ITERS - 1:
            m, state = run(
                functools.partial(next_kernel, peers),
                (f32(13, width, cells), f32(width, count, cells)),
                args,
                scratch,
            )
        else:
            state = run(functools.partial(last_kernel, peers), f32(count, width, cells), args, scratch)
    return state, macro


def solution(mesh):
    return jax.shard_map(
        per_device,
        mesh=mesh,
        in_specs=(
            P("vel", "gx", None),
            P(None, "vel"),
            P("vel"),
            P("gx", None),
            P("gx", None),
            P(None, "vel", None),
        ),
        out_specs=(P("vel", "gx", None), P(None, "gx", None)),
        check_vma=False,
    )
```

```python
import functools
import math

import jax
import jax.numpy as jnp
from jax import lax
from jax.experimental import pallas as pl
from jax.experimental.pallas import tpu as pltpu
from jax.sharding import PartitionSpec as P


NZ = 8
ITERS = 2
JACOBI = 2
HALO = JACOBI + 1
pseudo_rate = 0.5
source_gain = 0.5
diffusion = (0.6, 0.8, 0.8, 0.8, 1.0)
viscous_conduction_ratio = 2.0 / 3.0
wall_rate = 4.0
box_volume = 216.0
LOG2E = math.log2(math.e)
LANES = 128
SUB = 8
PAIRS = ((0, 0), (0, 1), (1, 0), (0, 2), (2, 0), (1, 1))
FEATURES = 32
A, B, E, W, HB, HE, BASE, FA, BA, REST = range(10)
TABLE = 10
CHUNKS = 2
BLOCKS = 2


SMEM = pl.BlockSpec(memory_space=pltpu.SMEM)
VMEM = pl.BlockSpec(memory_space=pltpu.VMEM)
PARAMS = pltpu.CompilerParams(vmem_limit_bytes=16 * 1024 * 1024)


def run(kernel, out_shape, args, scratch=(), scalar=True):
    return pl.pallas_call(
        kernel,
        out_shape=out_shape,
        in_specs=([SMEM] if scalar else []) + [VMEM] * (len(args) - (1 if scalar else 0)),
        out_specs=jax.tree.map(lambda _: VMEM, out_shape),
        scratch_shapes=scratch,
        compiler_params=PARAMS,
    )(*args)


def f32(*shape):
    return jax.ShapeDtypeStruct(shape, jnp.float32)


def add_moments(acc, s, t_ref, rows):
    a, b, e = (t_ref[k, rows, :] for k in (A, B, E))
    g = s * t_ref[W, rows, :]
    ga, gb, ge = g * a, g * b, g * e
    gaa, gbb, gee = ga * a, gb * b, ge * e
    gs = gaa + gbb + gee
    terms = (g, ga, gb, ge, gs, gaa, gbb, ga * b, ga * e, gb * e, gs * a, gs * b, gs * e)
    return tuple(old + new for old, new in zip(acc, terms))


def write_moments(m_ref, x, acc):
    for field, value in enumerate(acc):
        m_ref[field, x : x + 1, :] = jnp.sum(value, axis=0, keepdims=True)


def moments_loop(acc_ref, t_ref, first, groups, state_at):
    for x in range(acc_ref.shape[1]):

        def step(g, acc):
            rows = pl.ds(pl.multiple_of(g * SUB, SUB), SUB)
            table_rows = pl.ds(pl.multiple_of(first + g * SUB, SUB), SUB)
            return add_moments(acc, state_at(x, rows), t_ref, table_rows)

        acc = tuple(acc_ref[k, x] for k in range(13))
        acc = lax.fori_loop(0, groups, step, acc, unroll=4)
        for k, value in enumerate(acc):
            acc_ref[k, x] = value


def write_moments(m_ref, acc_ref):
    width = acc_ref.shape[1]
    for k in range(13):
        m_ref[k * width : (k + 1) * width, :] = jnp.sum(acc_ref[k], axis=1)


def first_kernel(
    extent, steps, v_ref, w_ref, collision_ref, solid_ref, dist_ref, m_ref, t_ref, rate_ref, wall_ref, vw_ref, acc_ref
):
    block, width = dist_ref.shape[0], dist_ref.shape[1]
    i = pl.program_id(0)
    start = pl.multiple_of(i * block, block)

    @pl.when(i == 0)
    def _():
        wall = solid_ref[...].astype(jnp.float32)
        wall_ref[...] = wall
        rate_ref[...] = collision_ref[...] + wall_rate * wall
        acc_ref[...] = jnp.zeros_like(acc_ref)
        vw_ref[0:3, :] = v_ref[...]
        vw_ref[3:4, :] = w_ref[...]
        vw_ref[4:8, :] = jnp.zeros((4, vw_ref.shape[1]), jnp.float32)
        lines = vw_ref.shape[1] // LANES
        for k in range(4):
            for j in range(lines):
                row = 13 * width + k * lines + j
                m_ref[row : row + 1, :] = vw_ref[k : k + 1, j * LANES : (j + 1) * LANES]

    part = max(block, LANES)

    @pl.when(start % part == 0)
    def _():
        here = pl.ds(pl.multiple_of(start, part), part)
        columns = vw_ref[:, here].T

        def wide(k):
            return jnp.broadcast_to(columns[:, k : k + 1], (part, LANES))

        a, b, e = wide(0), wide(1), wide(2)
        t_ref[A, here], t_ref[B, here], t_ref[E, here], t_ref[W, here] = a, b, e, wide(3)
        hb, he = 0.5 * jnp.abs(b), 0.5 * jnp.abs(e)
        t_ref[HB, here], t_ref[HE, here] = hb, he
        t_ref[BASE, here] = pseudo_rate + (hb + he) + jnp.abs(a) * extent
        t_ref[FA, here] = jnp.maximum(a, 0.0) * extent
        t_ref[BA, here] = jnp.maximum(-a, 0.0) * extent
        t_ref[REST, here] = (box_volume * (2.0 * math.pi) ** (-1.5)) * jnp.exp(-0.5 * (a * a + b * b + e * e))

    moments_loop(acc_ref, t_ref, start, block // SUB, lambda x, rows: dist_ref[rows, x, :])

    @pl.when(i == steps - 1)
    def _():
        write_moments(m_ref, acc_ref)


def gains_kernel(t_ref, rate_ref, rden_ref, p_ref):
    width, count = rden_ref.shape[0], rden_ref.shape[1]

    def step(g, carry):
        rows = pl.ds(pl.multiple_of(g * SUB, SUB), SUB)
        base = t_ref[BASE, rows, :]
        gain = t_ref[FA, rows, :] + t_ref[BA, rows, :]
        ahead = t_ref[A, rows, :] >= 0.0
        steps = []
        for x in range(width):
            rden = 1.0 / (base + rate_ref[x : x + 1, :])
            rden_ref[x, rows, :] = rden
            steps.append(gain * rden)
        up, down = [steps[0]], [steps[-1]]
        for x in range(1, width):
            up.append(up[-1] * steps[x])
            down.append(down[-1] * steps[width - 1 - x])
        for x in range(width):
            p_ref[x, rows, :] = jnp.where(ahead, up[x], down[width - 1 - x])
        return carry

    lax.fori_loop(0, count // SUB, step, 0, unroll=2)


def slabs_kernel(peers, width, me_ref, t_ref, c_ref, g_ref):
    count = g_ref.shape[1]
    below = c_ref.shape[1] - width
    me = me_ref[0]

    def step(g, carry):
        rows = pl.ds(pl.multiple_of(g * SUB, SUB), SUB)
        base = t_ref[BASE, rows, :]
        gain = t_ref[FA, rows, :] + t_ref[BA, rows, :]
        for d in range(peers):
            slab = jnp.ones_like(gain)
            for x in range(0, width, 2):
                product = base + c_ref[d ^ me, below + x : below + x + 1, :]
                power = gain
                if x + 1 < width:
                    product = product * (base + c_ref[d ^ me, below + x + 1 : below + x + 2, :])
                    power = power * gain
                slab = slab * (power / product)
            g_ref[d, rows, :] = slab
        return carry

    lax.fori_loop(0, count // SUB, step, 0, unroll=2)


def features_kernel(v_ref, f_ref, row_ref):
    blocks = v_ref.shape[0]
    part = v_ref.shape[1] // 4
    for k in range(blocks):
        a, b, e, w = (v_ref[k, i * part : (i + 1) * part, :] for i in range(4))
        sides = [split(value) for value in (a, b, e, a * a + b * b + e * e)]
        one, zero = jnp.ones_like(a), jnp.zeros_like(a)
        rows = [side[i] for side in sides for i, _ in PAIRS] + [one] * 3 + split(jnp.log2(w))
        rows = rows + [zero] * (FEATURES - len(rows))
        for i, row in enumerate(rows):
            for j in range(part):
                row_ref[k * part + j, i : i + 1, :] = row[j : j + 1, :]

    def turn(r, carry):
        where = pl.ds(pl.multiple_of(r * LANES, LANES), LANES)
        f_ref[where, :] = row_ref[r].T.astype(jnp.bfloat16)
        return carry

    lax.fori_loop(0, blocks * part, turn, 0, unroll=4)


def split(value):
    parts = []
    for _ in range(3):
        part = value.astype(jnp.bfloat16).astype(jnp.float32)
        parts.append(part)
        value = value - part
    return parts


def lane_z():
    return lax.broadcasted_iota(jnp.int32, (1, LANES), 1) % NZ


def y_less(v):
    return pltpu.roll(v, NZ, 1)


def y_more(v):
    return pltpu.roll(v, LANES - NZ, 1)


def z_less(v):
    return jnp.where(lane_z() == 0, pltpu.roll(v, LANES - NZ + 1, 1), pltpu.roll(v, 1, 1))


def z_more(v):
    return jnp.where(lane_z() == NZ - 1, pltpu.roll(v, NZ - 1, 1), pltpu.roll(v, LANES - 1, 1))


def dy(v):
    return 0.5 * (y_more(v) - y_less(v))


def dz(v):
    return 0.5 * (z_more(v) - z_less(v))


def x_less(v):
    return pltpu.roll(v, 1, 0)


def x_more(v):
    return pltpu.roll(v, v.shape[0] - 1, 0)


def fields_of(m):
    rho = m[0]
    inverse = 1.0 / rho
    u = [m[1 + i] * inverse for i in range(3)]
    square = u[0] * u[0] + u[1] * u[1] + u[2] * u[2]
    warm = (m[4] * inverse - square) * (1.0 / 3.0)
    force = rho * warm
    second = [[m[5], m[7], m[8]], [m[7], m[6], m[9]], [m[8], m[9], m[4] - m[5] - m[6]]]
    xx = second[0][0] - rho * u[0] * u[0] - force
    yy = second[1][1] - rho * u[1] * u[1] - force
    xy = second[0][1] - rho * u[0] * u[1]
    xz = second[0][2] - rho * u[0] * u[2]
    yz = second[1][2] - rho * u[1] * u[2]
    heat = []
    for i in range(3):
        inner = u[0] * second[i][0] + u[1] * second[i][1] + u[2] * second[i][2]
        heat.append(0.5 * (m[10 + i] - 2.0 * inner - u[i] * m[4] + 2.0 * rho * u[i] * square))
    return rho, inverse, u, warm, (xx, yy, xy, xz, yz), heat


def correction(rho, inverse, u, warm, stress, heat, inside):
    xx, yy, xy, xz, yz = stress
    zz = -(xx + yy)

    def dx(v):
        v = jnp.where(inside, v, 0.0)
        return 0.5 * (x_more(v) - x_less(v))

    source = [
        dx(rho * u[0]) + dy(rho * u[1]) + dz(rho * u[2]),
        dx(xx) + dy(xy) + dz(xz),
        dx(xy) + dy(yy) + dz(yz),
        dx(xz) + dy(yz) + dz(zz),
        dx(heat[0]) + dy(heat[1]) + dz(heat[2]),
    ]
    scale = [-source_gain * inverse] * 4 + [(-source_gain * 2.0 / 3.0) / (rho * warm)]
    source = [jnp.where(inside, s * c, 0.0) for s, c in zip(source, scale)]
    delta = source
    for _ in range(JACOBI):
        fresh = []
        for mu, s, d in zip(diffusion, source, delta):
            beside = x_less(d) + x_more(d) + y_less(d) + y_more(d) + z_less(d) + z_more(d)
            fresh.append(jnp.where(inside, (s + mu * beside) * (1.0 / (1.0 + 6.0 * mu)), 0.0))
        delta = fresh
    return delta


def transport_kernel(first, raw, t_ref, s_ref, drive_ref):
    width = drive_ref.shape[0]
    count = s_ref.shape[0] if raw else s_ref.shape[1]
    start = pl.program_id(0) * count
    lane = lax.broadcasted_iota(jnp.int32, (SUB, LANES), 1)
    z = lane % NZ
    y_down, y_up = (lane + LANES - NZ) % LANES, (lane + NZ) % LANES
    z_down, z_up = lane - z + (z + NZ - 1) % NZ, lane - z + (z + 1) % NZ

    def step(g, carry):
        rows = pl.ds(pl.multiple_of(g * SUB, SUB), SUB)
        out = pl.ds(pl.multiple_of(start + g * SUB, SUB), SUB)
        table_rows = pl.ds(pl.multiple_of(first + start + g * SUB, SUB), SUB)
        hb, he = t_ref[HB, table_rows, :], t_ref[HE, table_rows, :]
        from_y = jnp.where(t_ref[B, table_rows, :] > 0.0, y_down, y_up)
        from_z = jnp.where(t_ref[E, table_rows, :] > 0.0, z_down, z_up)
        for x in range(width):
            s = s_ref[rows, x, :] if raw else s_ref[x, rows, :]
            sy = jnp.take_along_axis(s, from_y, axis=1, mode="promise_in_bounds")
            sz = jnp.take_along_axis(s, from_z, axis=1, mode="promise_in_bounds")
            drive_ref[x, out, :] = pseudo_rate * s + hb * sy + he * sz
        return carry

    lax.fori_loop(0, count // SUB, step, 0, unroll=8)


def kinetic_kernel(
    peers, me_ref, before_ref, m_ref, after_ref, f_ref, t_ref, rate_ref, wall_ref, drive_ref, rden_ref,
    s_ref, c_ref, macro_ref, field_ref, pad_ref, cell_ref, total_ref,
):
    width, count = s_ref.shape[0], s_ref.shape[1]
    me = me_ref[0]
    tall = width + 2 * SUB
    own = slice(SUB, SUB + width)
    pad_ref[...] = jnp.ones_like(pad_ref)
    for k in range(13):
        pad_ref[k, SUB - HALO : SUB, :] = before_ref[k]
        pad_ref[k, own, :] = m_ref[k]
        pad_ref[k, SUB + width : SUB + width + HALO, :] = after_ref[k]
    row = lax.broadcasted_iota(jnp.int32, (tall, LANES), 0) + (me * width - SUB)
    inside = (row >= 0) & (row < peers * width)
    rho, inverse, u, warm, stress, heat = fields_of([pad_ref[k] for k in range(13)])
    delta = correction(rho, inverse, u, warm, stress, heat, inside)
    for k, value in enumerate(
        (rho * jnp.exp(delta[0]), u[0] + delta[1], u[1] + delta[2], u[2] + delta[3], warm * jnp.exp(delta[4]))
    ):
        pad_ref[k] = value
        macro_ref[k] = pad_ref[k, own, :]
    for k in range(3):
        pad_ref[5 + k] = heat[k]
    R, U, T = macro_ref[0], [macro_ref[1 + k] for k in range(3)], macro_ref[4]
    q = [pad_ref[5 + k, own, :] for k in range(3)]
    cold = 1.0 / T
    beta = (-0.5 * LOG2E) * cold
    alpha = [(LOG2E * cold) * U[k] for k in range(3)]
    gamma = beta * (U[0] * U[0] + U[1] * U[1] + U[2] * U[2])
    rows = [side[j] for side in (split(v) for v in (*alpha, beta)) for _, j in PAIRS]
    rows = rows + split(gamma) + [jnp.ones_like(T)] * 3
    rows = rows + [jnp.zeros_like(T)] * (FEATURES - len(rows))
    for i, value in enumerate(rows):
        for x in range(width):
            cell_ref[i : i + 1, x * LANES : (x + 1) * LANES] = value[x : x + 1, :]
    cells = cell_ref[...].astype(jnp.bfloat16)

    def mass(r, acc):
        some = f_ref[pl.ds(pl.multiple_of(r * LANES, LANES), LANES), :]
        power = jnp.dot(some, cells, preferred_element_type=jnp.float32)
        weight = jnp.exp2(power)
        return acc + jnp.sum(weight.reshape(LANES // SUB, SUB, width * LANES), axis=0)

    acc = lax.fori_loop(0, f_ref.shape[0] // LANES, mass, jnp.zeros((SUB, width * LANES), jnp.float32), unroll=8)
    acc = jnp.sum(acc, axis=0, keepdims=True)
    for x in range(width):
        total_ref[x : x + 1, :] = acc[:, x * LANES : (x + 1) * LANES]
    wall, rate = wall_ref[...], rate_ref[...]
    third = (1.0 - viscous_conduction_ratio) / (5.0 * R * T * T)
    values = [*U, beta, *(v * third for v in q), cold]
    values += [(1.0 - wall) * R * rate / total_ref[...], wall * R * rate]
    for k, value in enumerate(values):
        field_ref[k] = value

    sweep(0, field_ref, t_ref, drive_ref, rden_ref, s_ref, c_ref)
    c_ref[count : count + width, :] = rate


def sweep_kernel(first, t_ref, field_ref, drive_ref, rden_ref, s_ref, c_ref):
    sweep(first, field_ref, t_ref, drive_ref, rden_ref, s_ref, c_ref)


def sweep(first, field_ref, t_ref, drive_ref, rden_ref, s_ref, c_ref):
    width, count = s_ref.shape[0], s_ref.shape[1]

    def both(g):
        return (
            pl.ds(pl.multiple_of(g * SUB, SUB), SUB),
            pl.ds(pl.multiple_of(first + g * SUB, SUB), SUB),
        )

    for x in range(width):
        ux, uy, uz, power, qx, qy, qz, inv, maxwell, rest = (
            jnp.broadcast_to(field_ref[k, x : x + 1, :], (SUB, LANES)) for k in range(10)
        )

        def ahead(g, carry):
            rows, wide = both(g)
            a, b, e = (t_ref[k, wide, :] for k in (A, B, E))
            cx, cy, cz = a - ux, b - uy, e - uz
            square = cx * cx + cy * cy + cz * cz
            expo = jnp.exp2(square * power)
            flux = cx * qx + cy * qy + cz * qz
            target = (expo * maxwell) * (1.0 + flux * (square * inv - 5.0)) + rest * t_ref[REST, wide, :]
            rden = rden_ref[x, wide, :]
            value = (drive_ref[x, rows, :] + target) * rden
            if x:
                value = value + (t_ref[FA, wide, :] * rden) * s_ref[x - 1, rows, :]
            s_ref[x, rows, :] = value
            return carry

        lax.fori_loop(0, count // SUB, ahead, 0, unroll=16)

    def back(g, carry):
        rows, wide = both(g)
        ba = t_ref[BA, wide, :]
        value = s_ref[width - 1, rows, :]
        last = value
        for x in range(width - 2, -1, -1):
            value = s_ref[x, rows, :] + (ba * rden_ref[x, wide, :]) * value
            s_ref[x, rows, :] = value
        c_ref[rows, :] = jnp.where(t_ref[A, wide, :] >= 0.0, last, value)
        return carry

    lax.fori_loop(0, count // SUB, back, 0, unroll=4)


def entering(peers, me, first, rows, t_ref, c_ref, g_ref, flow_ref):
    wide = pl.ds(pl.multiple_of(first + rows.start, SUB), SUB)
    up, down = flow_ref[0, wide, :], flow_ref[1, wide, :]
    for d in range(peers - 1):
        up = jnp.where(d < me, g_ref[d, wide, :] * up + c_ref[d ^ me, rows, :], up)
    for d in range(peers - 1, 0, -1):
        down = jnp.where(d > me, g_ref[d, wide, :] * down + c_ref[d ^ me, rows, :], down)
    return jnp.where(t_ref[A, wide, :] >= 0.0, up, down)


def next_kernel(peers, first, me_ref, t_ref, c_ref, g_ref, flow_ref, s_ref, p_ref, *refs):
    partial_ref, (m_ref, state_ref, enter_ref, acc_ref) = refs[:-4], refs[-4:]
    count = s_ref.shape[1]
    me = me_ref[0]

    def enter(g, carry):
        rows = pl.ds(pl.multiple_of(g * SUB, SUB), SUB)
        enter_ref[rows, :] = entering(peers, me, first, rows, t_ref, c_ref, g_ref, flow_ref)
        return carry

    lax.fori_loop(0, count // SUB, enter, 0, unroll=2)
    acc_ref[...] = jnp.zeros_like(acc_ref)

    def state_at(x, rows):
        wide = pl.ds(pl.multiple_of(first + rows.start, SUB), SUB)
        s = s_ref[x, rows, :] + p_ref[x, wide, :] * enter_ref[rows, :]
        state_ref[x, rows, :] = s
        return s

    moments_loop(acc_ref, t_ref, first, count // SUB, state_at)
    write_moments(m_ref, acc_ref)
    if partial_ref:
        m_ref[...] += partial_ref[0][...]


def last_kernel(peers, first, me_ref, t_ref, c_ref, g_ref, flow_ref, s_ref, p_ref, *refs):
    out_ref = refs[-1]
    width, block = out_ref.shape[1], out_ref.shape[0]
    me = me_ref[0]
    start = pl.program_id(0) * block

    def step(g, carry):
        rows = pl.ds(pl.multiple_of(start + g * SUB, SUB), SUB)
        wide = pl.ds(pl.multiple_of(first + start + g * SUB, SUB), SUB)
        out = pl.ds(pl.multiple_of(g * SUB, SUB), SUB)
        enter = entering(peers, me, first, rows, t_ref, c_ref, g_ref, flow_ref)
        for x in range(width):
            out_ref[out, x, :] = s_ref[x, rows, :] + p_ref[x, wide, :] * enter
        return carry

    lax.fori_loop(0, block // SUB, step, 0, unroll=2)


def stages(size):
    found, stride = [], 1
    while size > 1:
        factor = next(f for f in range(2, size + 1) if size % f == 0)
        if factor == 2 and size % 4 == 0 and (stride > 1 or size % 8):
            factor = 4
        found.append((factor, stride))
        size, stride = size // factor, stride * factor
    return found


def reduce_over(axis, value, rows):
    size = lax.axis_size(axis)
    value, extra = value[:rows], value[None, rows:]
    done = []
    for factor, stride in stages(size):
        sent = jnp.concatenate([value, extra.reshape(-1, LANES)]) if extra.size else value
        got = []
        for turn in range(1, factor):
            pairs = []
            for i in range(size):
                digit = i // stride % factor
                pairs.append((i, i + ((digit + turn) % factor - digit) * stride))
            got.append(lax.ppermute(sent, axis, pairs))
        done.append(factor)
        for piece in got:
            value = value + piece[:rows]
        if extra.size:
            shape = (-1,) + extra.shape[1:]
            extra = jnp.concatenate([extra] + [piece[rows:].reshape(shape) for piece in got])
    return value, extra


def gather_over(axis, value):
    size = lax.axis_size(axis)
    blocks = value[None]
    order = [0]
    bit = size // 2
    while bit:
        got = lax.ppermute(blocks, axis, [(i, i ^ bit) for i in range(size)])
        blocks = jnp.concatenate([blocks, got])
        order = order + [k ^ bit for k in order]
        bit //= 2
    return jnp.concatenate([blocks[order.index(k)][None] for k in range(size)])


def neighbours(axis, value, width):
    size, me = lax.axis_size(axis), lax.axis_index(axis)
    odd = me % 2 == 1
    first, last = value[:, :width], value[:, value.shape[1] - width :]
    near = [(i, i ^ 1) for i in range(size)]
    far = [(i, i + 1) for i in range(1, size - 1, 2)]
    far = lax.ppermute(jnp.where(odd, last, first), axis, far + [(j, i) for i, j in far])
    near = lax.ppermute(jnp.where(odd, first, last), axis, near)
    return jnp.where(odd, near, far), jnp.where(odd, far, near)


def iteration(repeat, m, states, table, rate, wall, me, inflow, kept):
    width, cells = rate.shape
    count, peers = table.shape[1], lax.axis_size("gx")
    chunk = count // len(states)
    block = chunk // BLOCKS
    if repeat == 0:
        kept["gains"] = run(gains_kernel, (f32(width, count, cells),) * 2, (table, rate), scalar=False)
    rden, prefix = kept["gains"]
    drives = []
    for k, state in enumerate(states):
        kernel = functools.partial(transport_kernel, k * chunk, repeat == 0)
        at = (lambda i, k=k: (k * BLOCKS + i, 0, 0)) if repeat == 0 else None
        source = pl.BlockSpec((block, width, cells), at) if repeat == 0 else VMEM
        drives.append(
            pl.pallas_call(
                kernel,
                grid=(BLOCKS if repeat == 0 else 1,),
                out_shape=f32(width, chunk, cells),
                in_specs=[VMEM, source],
                out_specs=VMEM,
                compiler_params=PARAMS,
            )(table, state)
        )
    m, extra = reduce_over("vel", m, 13 * width)
    m = m.reshape(13, width, cells)
    before, after = neighbours("gx", m, HALO)
    if repeat == 0:
        total = extra.shape[0] * extra.shape[1] // 4
        kept["features"] = run(
            features_kernel,
            jax.ShapeDtypeStruct((total * LANES, FEATURES), jnp.bfloat16),
            (extra,),
            scratch=(pltpu.VMEM((total, FEATURES, LANES), jnp.float32),),
            scalar=False,
        )
    local, carry, macro, fields = run(
        functools.partial(kinetic_kernel, peers),
        (f32(width, chunk, cells), f32(chunk + width, cells), f32(5, width, cells), f32(10, width, cells)),
        (me, before, m, after, kept["features"], table, rate, wall, drives[0], rden),
        scratch=(
            pltpu.VMEM((13, width + 2 * SUB, cells), jnp.float32),
            pltpu.VMEM((FEATURES, width * cells), jnp.float32),
            pltpu.VMEM((width, cells), jnp.float32),
        ),
    )
    locals_, carries = [local], [gather_over("gx", carry)]
    for k in range(1, len(states)):
        local, carry = run(
            functools.partial(sweep_kernel, k * chunk),
            (f32(width, chunk, cells), f32(chunk, cells)),
            (table, fields, drives[k], rden),
            scalar=False,
        )
        locals_.append(local)
        carries.append(gather_over("gx", carry))
    if repeat == 0:
        kernel = functools.partial(slabs_kernel, peers, width)
        kept["slabs"] = run(kernel, f32(peers, count, cells), (me, table, carries[0]))
    states, m, state = [], None, None
    for k in range(len(locals_)):
        args = (me, table, carries[k], kept["slabs"], inflow, locals_[k], prefix)
        if repeat < ITERS - 1:
            m, state = run(
                functools.partial(next_kernel, peers, k * chunk),
                (f32(13 * width, cells), f32(width, chunk, cells)),
                args if m is None else args + (m,),
                (pltpu.VMEM((chunk, cells), jnp.float32), pltpu.VMEM((13, width, SUB, cells), jnp.float32)),
            )
            states.append(state)
        else:
            rest = [] if k == 0 else [states]
            states = pl.pallas_call(
                functools.partial(last_kernel, peers, k * chunk),
                grid=(BLOCKS,),
                out_shape=f32(count, width, cells),
                in_specs=[SMEM] + [VMEM] * 6 + [pl.BlockSpec(memory_space=pl.ANY)] * len(rest),
                out_specs=pl.BlockSpec((block, width, cells), lambda i, k=k: (k * BLOCKS + i, 0, 0)),
                input_output_aliases={len(args): 0} if rest else {},
                compiler_params=PARAMS,
            )(*args, *rest)
    return m, states, macro


def per_device(distribution, velocity, weights, collision, solid, inflow):
    count, width, cells = distribution.shape
    peers = lax.axis_size("gx")
    me = lax.axis_index("gx").astype(jnp.int32).reshape(1)
    chunk = count // CHUNKS
    block = chunk // BLOCKS
    distribution = pltpu.with_memory_space_constraint(distribution, pltpu.HBM)
    lines = 4 * count // LANES
    outs = (f32(13 * width + lines, cells), f32(TABLE, count, cells))
    outs += (f32(width, cells), f32(width, cells))
    m, table, rate, wall = pl.pallas_call(
        functools.partial(first_kernel, float(width * peers), count // block),
        grid=(count // block,),
        out_shape=outs,
        in_specs=[VMEM] * 4 + [pl.BlockSpec((block, width, cells), lambda i: (i, 0, 0))],
        out_specs=(VMEM,) * len(outs),
        scratch_shapes=(pltpu.VMEM((8, count), jnp.float32), pltpu.VMEM((13, width, SUB, cells), jnp.float32)),
        compiler_params=PARAMS,
    )(velocity, weights.reshape(1, count), collision, solid, distribution)
    kept, states = {}, (distribution,) * CHUNKS
    for repeat in range(ITERS):
        m, states, macro = iteration(repeat, m, states, table, rate, wall, me, inflow, kept)
    return states, macro


def solution(mesh):
    return jax.shard_map(
        per_device,
        mesh=mesh,
        in_specs=(
            P("vel", "gx", None),
            P(None, "vel"),
            P("vel"),
            P("gx", None),
            P("gx", None),
            P(None, "vel", None),
        ),
        out_specs=(P("vel", "gx", None), P(None, "gx", None)),
        check_vma=False,
    )
```

```python
import functools
import math

import jax
import jax.numpy as jnp
from jax import lax
from jax.experimental import pallas as pl
from jax.experimental.pallas import tpu as pltpu
from jax.sharding import PartitionSpec as P


NZ = 8
ITERS = 2
JACOBI = 2
HALO = JACOBI + 1
pseudo_rate = 0.5
source_gain = 0.5
diffusion = (0.6, 0.8, 0.8, 0.8, 1.0)
viscous_conduction_ratio = 2.0 / 3.0
wall_rate = 4.0
box_volume = 216.0
LOG2E = math.log2(math.e)
LANES = 128
SUB = 8
PAIRS = ((0, 0), (0, 1), (1, 0), (0, 2), (2, 0), (1, 1))
FEATURES = 32
A, B, E, W, HB, HE, BASE, FA, BA, REST = range(10)
TABLE = 10
CHUNKS = 2
BLOCKS = 4
PAD = 8


SMEM = pl.BlockSpec(memory_space=pltpu.SMEM)
VMEM = pl.BlockSpec(memory_space=pltpu.VMEM)
HBM = pl.BlockSpec(memory_space=pltpu.HBM)
PARAMS = pltpu.CompilerParams(vmem_limit_bytes=16 * 1024 * 1024)


def run(kernel, out_shape, args, scratch=(), scalar=True):
    return pl.pallas_call(
        kernel,
        out_shape=out_shape,
        in_specs=([SMEM] if scalar else []) + [VMEM] * (len(args) - (1 if scalar else 0)),
        out_specs=jax.tree.map(lambda _: VMEM, out_shape),
        scratch_shapes=scratch,
        compiler_params=PARAMS,
    )(*args)


def f32(*shape):
    return jax.ShapeDtypeStruct(shape, jnp.float32)


def add_moments(acc, s, t_ref, rows):
    a, b, e = (t_ref[k, rows, :] for k in (A, B, E))
    g = s * t_ref[W, rows, :]
    ga, gb, ge = g * a, g * b, g * e
    gaa, gbb, gee = ga * a, gb * b, ge * e
    gs = gaa + gbb + gee
    terms = (g, ga, gb, ge, gs, gaa, gbb, ga * b, ga * e, gb * e, gs * a, gs * b, gs * e)
    return tuple(old + new for old, new in zip(acc, terms))


def write_moments(m_ref, x, acc):
    for field, value in enumerate(acc):
        m_ref[field, x : x + 1, :] = jnp.sum(value, axis=0, keepdims=True)


def moments_loop(acc_ref, t_ref, first, groups, state_at):
    for x in range(acc_ref.shape[1]):

        def step(g, acc):
            rows = pl.ds(pl.multiple_of(g * SUB, SUB), SUB)
            table_rows = pl.ds(pl.multiple_of(first + g * SUB, SUB), SUB)
            return add_moments(acc, state_at(x, rows), t_ref, table_rows)

        acc = tuple(acc_ref[k, x] for k in range(13))
        acc = lax.fori_loop(0, groups, step, acc, unroll=min(16, groups))
        for k, value in enumerate(acc):
            acc_ref[k, x] = value


def write_moments(m_ref, acc_ref):
    width = acc_ref.shape[1]
    for k in range(13):
        m_ref[k * width : (k + 1) * width, :] = jnp.sum(acc_ref[k], axis=1)


def first_kernel(extent, *refs):
    sources, (m_ref, t_ref, rate_ref, wall_ref), rest = refs[:5], refs[5:9], refs[9:]
    v_ref, w_ref, collision_ref, solid_ref, dist_ref, vw_ref, acc_ref, sem = rest
    count, width = dist_ref.shape[0], dist_ref.shape[1]
    block = count // BLOCKS
    small = [
        pltpu.make_async_copy(source, target, sem.at[k])
        for k, (source, target) in enumerate(zip(sources[:4], (v_ref, w_ref, collision_ref, solid_ref)))
    ]
    large = [
        pltpu.make_async_copy(
            sources[4].at[pl.ds(k * block, block)], dist_ref.at[pl.ds(k * block, block)], sem.at[4 + k]
        )
        for k in range(BLOCKS)
    ]
    for copy in small + large:
        copy.start()
    for copy in small:
        copy.wait()
    wall = solid_ref[...].astype(jnp.float32)
    wall_ref[...] = wall
    rate_ref[...] = collision_ref[...] + wall_rate * wall
    acc_ref[...] = jnp.zeros_like(acc_ref)
    vw_ref[0:3, :] = v_ref[...]
    vw_ref[3:4, :] = w_ref[...]
    vw_ref[4:8, :] = jnp.zeros((4, count), jnp.float32)
    lines = count // LANES
    for k in range(4):
        for j in range(lines):
            row = 13 * width + k * lines + j
            m_ref[row : row + 1, :] = vw_ref[k : k + 1, j * LANES : (j + 1) * LANES]
    columns = vw_ref[...].T

    def wide(k):
        return jnp.broadcast_to(columns[:, k : k + 1], (count, LANES))

    here = slice(0, count)
    a, b, e = wide(0), wide(1), wide(2)
    t_ref[A, here], t_ref[B, here], t_ref[E, here], t_ref[W, here] = a, b, e, wide(3)
    hb, he = 0.5 * jnp.abs(b), 0.5 * jnp.abs(e)
    t_ref[HB, here], t_ref[HE, here] = hb, he
    t_ref[BASE, here] = pseudo_rate + (hb + he) + jnp.abs(a) * extent
    t_ref[FA, here] = jnp.maximum(a, 0.0) * extent
    t_ref[BA, here] = jnp.maximum(-a, 0.0) * extent
    t_ref[REST, here] = (box_volume * (2.0 * math.pi) ** (-1.5)) * jnp.exp(-0.5 * (a * a + b * b + e * e))
    for k, copy in enumerate(large):
        copy.wait()
        moments_loop(
            acc_ref,
            t_ref,
            k * block,
            block // SUB,
            lambda x, rows, k=k: dist_ref[pl.ds(pl.multiple_of(k * block + rows.start, SUB), SUB), x, :],
        )
    write_moments(m_ref, acc_ref)


def gains_kernel(t_ref, rate_ref, rden_ref, p_ref):
    width, count = rden_ref.shape[0], rden_ref.shape[1]

    def step(g, carry):
        rows = pl.ds(pl.multiple_of(g * SUB, SUB), SUB)
        base = t_ref[BASE, rows, :]
        gain = t_ref[FA, rows, :] + t_ref[BA, rows, :]
        ahead = t_ref[A, rows, :] >= 0.0
        steps = []
        for x in range(width):
            rden = 1.0 / (base + rate_ref[x : x + 1, :])
            rden_ref[x, rows, :] = rden
            steps.append(gain * rden)
        up, down = [steps[0]], [steps[-1]]
        for x in range(1, width):
            up.append(up[-1] * steps[x])
            down.append(down[-1] * steps[width - 1 - x])
        for x in range(width):
            p_ref[x, rows, :] = jnp.where(ahead, up[x], down[width - 1 - x])
        return carry

    lax.fori_loop(0, count // SUB, step, 0, unroll=2)


def slabs_kernel(peers, width, me_ref, t_ref, c_ref, g_ref):
    count = g_ref.shape[1]
    below = c_ref.shape[1] - width
    me = me_ref[0]

    def step(g, carry):
        rows = pl.ds(pl.multiple_of(g * SUB, SUB), SUB)
        base = t_ref[BASE, rows, :]
        gain = t_ref[FA, rows, :] + t_ref[BA, rows, :]
        for d in range(peers):
            slab = jnp.ones_like(gain)
            for x in range(0, width, 2):
                product = base + c_ref[d ^ me, below + x : below + x + 1, :]
                power = gain
                if x + 1 < width:
                    product = product * (base + c_ref[d ^ me, below + x + 1 : below + x + 2, :])
                    power = power * gain
                slab = slab * (power / product)
            g_ref[d, rows, :] = slab
        return carry

    lax.fori_loop(0, count // SUB, step, 0, unroll=2)


def features_kernel(v_ref, f_ref, row_ref):
    blocks = v_ref.shape[0]
    part = v_ref.shape[1] // 4
    for k in range(blocks):
        a, b, e, w = (v_ref[k, i * part : (i + 1) * part, :] for i in range(4))
        sides = [split(value) for value in (a, b, e, a * a + b * b + e * e)]
        one, zero = jnp.ones_like(a), jnp.zeros_like(a)
        rows = [side[i] for side in sides for i, _ in PAIRS] + [one] * 3 + split(jnp.log2(w))
        rows = rows + [zero] * (FEATURES - len(rows))
        for i, row in enumerate(rows):
            for j in range(part):
                row_ref[k * part + j, i : i + 1, :] = row[j : j + 1, :]

    def turn(r, carry):
        where = pl.ds(pl.multiple_of(r * LANES, LANES), LANES)
        f_ref[where, :] = row_ref[r].T.astype(jnp.bfloat16)
        return carry

    lax.fori_loop(0, blocks * part, turn, 0, unroll=4)


def split(value):
    parts = []
    for _ in range(3):
        part = value.astype(jnp.bfloat16).astype(jnp.float32)
        parts.append(part)
        value = value - part
    return parts


def lane_z():
    return lax.broadcasted_iota(jnp.int32, (1, LANES), 1) % NZ


def y_less(v):
    return pltpu.roll(v, NZ, 1)


def y_more(v):
    return pltpu.roll(v, LANES - NZ, 1)


def z_less(v):
    return jnp.where(lane_z() == 0, pltpu.roll(v, LANES - NZ + 1, 1), pltpu.roll(v, 1, 1))


def z_more(v):
    return jnp.where(lane_z() == NZ - 1, pltpu.roll(v, NZ - 1, 1), pltpu.roll(v, LANES - 1, 1))


def dy(v):
    return 0.5 * (y_more(v) - y_less(v))


def dz(v):
    return 0.5 * (z_more(v) - z_less(v))


def x_less(v):
    return pltpu.roll(v, 1, 0)


def x_more(v):
    return pltpu.roll(v, v.shape[0] - 1, 0)


def fields_of(m):
    rho = m[0]
    inverse = 1.0 / rho
    u = [m[1 + i] * inverse for i in range(3)]
    square = u[0] * u[0] + u[1] * u[1] + u[2] * u[2]
    warm = (m[4] * inverse - square) * (1.0 / 3.0)
    force = rho * warm
    second = [[m[5], m[7], m[8]], [m[7], m[6], m[9]], [m[8], m[9], m[4] - m[5] - m[6]]]
    xx = second[0][0] - rho * u[0] * u[0] - force
    yy = second[1][1] - rho * u[1] * u[1] - force
    xy = second[0][1] - rho * u[0] * u[1]
    xz = second[0][2] - rho * u[0] * u[2]
    yz = second[1][2] - rho * u[1] * u[2]
    heat = []
    for i in range(3):
        inner = u[0] * second[i][0] + u[1] * second[i][1] + u[2] * second[i][2]
        heat.append(0.5 * (m[10 + i] - 2.0 * inner - u[i] * m[4] + 2.0 * rho * u[i] * square))
    return rho, inverse, u, warm, (xx, yy, xy, xz, yz), heat


def correction(rho, inverse, u, warm, stress, heat, inside):
    xx, yy, xy, xz, yz = stress
    zz = -(xx + yy)

    def dx(v):
        v = jnp.where(inside, v, 0.0)
        return 0.5 * (x_more(v) - x_less(v))

    source = [
        dx(rho * u[0]) + dy(rho * u[1]) + dz(rho * u[2]),
        dx(xx) + dy(xy) + dz(xz),
        dx(xy) + dy(yy) + dz(yz),
        dx(xz) + dy(yz) + dz(zz),
        dx(heat[0]) + dy(heat[1]) + dz(heat[2]),
    ]
    scale = [-source_gain * inverse] * 4 + [(-source_gain * 2.0 / 3.0) / (rho * warm)]
    source = [jnp.where(inside, s * c, 0.0) for s, c in zip(source, scale)]
    delta = source
    for _ in range(JACOBI):
        fresh = []
        for mu, s, d in zip(diffusion, source, delta):
            beside = x_less(d) + x_more(d) + y_less(d) + y_more(d) + z_less(d) + z_more(d)
            fresh.append(jnp.where(inside, (s + mu * beside) * (1.0 / (1.0 + 6.0 * mu)), 0.0))
        delta = fresh
    return delta


def transport_kernel(first, t_ref, s_ref, drive_ref):
    transport(first, 0, drive_ref.shape[1], t_ref, lambda x, rows: s_ref[x, rows, :], drive_ref)


def first_transport_kernel(first, t_ref, dist_ref, drive_ref, held_ref, sem):
    block = drive_ref.shape[1] // BLOCKS
    copies = [
        pltpu.make_async_copy(
            dist_ref.at[pl.ds(first + k * block, block)], held_ref.at[pl.ds(k * block, block)], sem.at[k]
        )
        for k in range(BLOCKS)
    ]
    for copy in copies:
        copy.start()
    for k, copy in enumerate(copies):
        copy.wait()
        transport(first, k * block, block, t_ref, lambda x, rows: held_ref[rows, x, :], drive_ref)


def transport(first, start, count, t_ref, state_at, drive_ref):
    width = drive_ref.shape[0]
    lane = lax.broadcasted_iota(jnp.int32, (SUB, LANES), 1)
    z = lane % NZ
    y_down, y_up = (lane + LANES - NZ) % LANES, (lane + NZ) % LANES
    z_down, z_up = lane - z + (z + NZ - 1) % NZ, lane - z + (z + 1) % NZ

    def step(g, carry):
        rows = pl.ds(pl.multiple_of(start + g * SUB, SUB), SUB)
        table_rows = pl.ds(pl.multiple_of(first + start + g * SUB, SUB), SUB)
        hb, he = t_ref[HB, table_rows, :], t_ref[HE, table_rows, :]
        from_y = jnp.where(t_ref[B, table_rows, :] > 0.0, y_down, y_up)
        from_z = jnp.where(t_ref[E, table_rows, :] > 0.0, z_down, z_up)
        for x in range(width):
            s = state_at(x, rows)
            sy = jnp.take_along_axis(s, from_y, axis=1, mode="promise_in_bounds")
            sz = jnp.take_along_axis(s, from_z, axis=1, mode="promise_in_bounds")
            drive_ref[x, rows, :] = pseudo_rate * s + hb * sy + he * sz
        return carry

    lax.fori_loop(0, count // SUB, step, 0, unroll=min(8, count // SUB))


def kinetic_kernel(
    peers, me_ref, before_ref, m_ref, after_ref, f_ref, t_ref, rate_ref, wall_ref, drive_ref, rden_ref,
    s_ref, c_ref, macro_ref, field_ref, pad_ref, cell_ref, total_ref,
):
    width, count = s_ref.shape[0], s_ref.shape[1]
    me = me_ref[0]
    tall = width + 2 * SUB
    own = slice(SUB, SUB + width)
    pad_ref[...] = jnp.ones_like(pad_ref)
    for k in range(13):
        pad_ref[k, SUB - HALO : SUB, :] = before_ref[k]
        pad_ref[k, own, :] = m_ref[k]
        pad_ref[k, SUB + width : SUB + width + HALO, :] = after_ref[k]
    row = lax.broadcasted_iota(jnp.int32, (tall, LANES), 0) + (me * width - SUB)
    inside = (row >= 0) & (row < peers * width)
    rho, inverse, u, warm, stress, heat = fields_of([pad_ref[k] for k in range(13)])
    delta = correction(rho, inverse, u, warm, stress, heat, inside)
    for k, value in enumerate(
        (rho * jnp.exp(delta[0]), u[0] + delta[1], u[1] + delta[2], u[2] + delta[3], warm * jnp.exp(delta[4]))
    ):
        pad_ref[k] = value
        macro_ref[k] = pad_ref[k, own, :]
    for k in range(3):
        pad_ref[5 + k] = heat[k]
    R, U, T = macro_ref[0], [macro_ref[1 + k] for k in range(3)], macro_ref[4]
    q = [pad_ref[5 + k, own, :] for k in range(3)]
    cold = 1.0 / T
    beta = (-0.5 * LOG2E) * cold
    alpha = [(LOG2E * cold) * U[k] for k in range(3)]
    gamma = beta * (U[0] * U[0] + U[1] * U[1] + U[2] * U[2])
    rows = [side[j] for side in (split(v) for v in (*alpha, beta)) for _, j in PAIRS]
    rows = rows + split(gamma) + [jnp.ones_like(T)] * 3
    rows = rows + [jnp.zeros_like(T)] * (FEATURES - len(rows))
    for i, value in enumerate(rows):
        for x in range(width):
            cell_ref[i : i + 1, x * LANES : (x + 1) * LANES] = value[x : x + 1, :]
    cells = cell_ref[...].astype(jnp.bfloat16)

    def mass(r, acc):
        some = f_ref[pl.ds(pl.multiple_of(r * LANES, LANES), LANES), :]
        power = jnp.dot(some, cells, preferred_element_type=jnp.float32)
        weight = jnp.exp2(power)
        return acc + jnp.sum(weight.reshape(LANES // SUB, SUB, width * LANES), axis=0)

    acc = lax.fori_loop(0, f_ref.shape[0] // LANES, mass, jnp.zeros((SUB, width * LANES), jnp.float32), unroll=8)
    acc = jnp.sum(acc, axis=0, keepdims=True)
    for x in range(width):
        total_ref[x : x + 1, :] = acc[:, x * LANES : (x + 1) * LANES]
    wall, rate = wall_ref[...], rate_ref[...]
    third = (1.0 - viscous_conduction_ratio) / (5.0 * R * T * T)
    values = [*U, beta, *(v * third for v in q), cold]
    values += [(1.0 - wall) * R * rate / total_ref[...], wall * R * rate]
    for k, value in enumerate(values):
        field_ref[k] = value

    sweep(0, field_ref, t_ref, drive_ref, rden_ref, s_ref, c_ref)
    c_ref[count : count + width, :] = rate


def sweep_kernel(first, t_ref, field_ref, drive_ref, rden_ref, s_ref, c_ref):
    sweep(first, field_ref, t_ref, drive_ref, rden_ref, s_ref, c_ref)


def sweep(first, field_ref, t_ref, drive_ref, rden_ref, s_ref, c_ref):
    width, count = s_ref.shape[0], s_ref.shape[1]

    def both(g):
        return (
            pl.ds(pl.multiple_of(g * SUB, SUB), SUB),
            pl.ds(pl.multiple_of(first + g * SUB, SUB), SUB),
        )

    for x in range(width):
        ux, uy, uz, power, qx, qy, qz, inv, maxwell, rest = (
            jnp.broadcast_to(field_ref[k, x : x + 1, :], (SUB, LANES)) for k in range(10)
        )

        def ahead(g, carry):
            rows, wide = both(g)
            a, b, e = (t_ref[k, wide, :] for k in (A, B, E))
            cx, cy, cz = a - ux, b - uy, e - uz
            square = cx * cx + cy * cy + cz * cz
            expo = jnp.exp2(square * power)
            flux = cx * qx + cy * qy + cz * qz
            target = (expo * maxwell) * (1.0 + flux * (square * inv - 5.0)) + rest * t_ref[REST, wide, :]
            rden = rden_ref[x, wide, :]
            value = (drive_ref[x, rows, :] + target) * rden
            if x:
                value = value + (t_ref[FA, wide, :] * rden) * s_ref[x - 1, rows, :]
            s_ref[x, rows, :] = value
            return carry

        lax.fori_loop(0, count // SUB, ahead, 0, unroll=min(32, count // SUB))

    def back(g, carry):
        rows, wide = both(g)
        ba = t_ref[BA, wide, :]
        value = s_ref[width - 1, rows, :]
        last = value
        for x in range(width - 2, -1, -1):
            value = s_ref[x, rows, :] + (ba * rden_ref[x, wide, :]) * value
            s_ref[x, rows, :] = value
        c_ref[rows, :] = jnp.where(t_ref[A, wide, :] >= 0.0, last, value)
        return carry

    lax.fori_loop(0, count // SUB, back, 0, unroll=4)


def entering(peers, me, first, rows, t_ref, c_ref, g_ref, flow_ref):
    wide = pl.ds(pl.multiple_of(first + rows.start, SUB), SUB)
    up, down = flow_ref[0, wide, :], flow_ref[1, wide, :]
    for d in range(peers - 1):
        up = jnp.where(d < me, g_ref[d, wide, :] * up + c_ref[d ^ me, rows, :], up)
    for d in range(peers - 1, 0, -1):
        down = jnp.where(d > me, g_ref[d, wide, :] * down + c_ref[d ^ me, rows, :], down)
    return jnp.where(t_ref[A, wide, :] >= 0.0, up, down)


def next_kernel(peers, first, me_ref, t_ref, c_ref, g_ref, flow_ref, s_ref, p_ref, *refs):
    partial_ref, (m_ref, state_ref, enter_ref, acc_ref) = refs[:-4], refs[-4:]
    count = s_ref.shape[1]
    me = me_ref[0]

    def enter(g, carry):
        rows = pl.ds(pl.multiple_of(g * SUB, SUB), SUB)
        enter_ref[rows, :] = entering(peers, me, first, rows, t_ref, c_ref, g_ref, flow_ref)
        return carry

    lax.fori_loop(0, count // SUB, enter, 0, unroll=2)
    acc_ref[...] = jnp.zeros_like(acc_ref)

    def state_at(x, rows):
        wide = pl.ds(pl.multiple_of(first + rows.start, SUB), SUB)
        s = s_ref[x, rows, :] + p_ref[x, wide, :] * enter_ref[rows, :]
        state_ref[x, rows, :] = s
        return s

    moments_loop(acc_ref, t_ref, first, count // SUB, state_at)
    write_moments(m_ref, acc_ref)
    if partial_ref:
        m_ref[...] += partial_ref[0][...]


def last_kernel(peers, first, me_ref, t_ref, c_ref, g_ref, flow_ref, s_ref, p_ref, *refs):
    out_ref = refs[-1]
    width, block = out_ref.shape[1], out_ref.shape[0]
    me = me_ref[0]
    start = pl.program_id(0) * block

    def step(g, carry):
        rows = pl.ds(pl.multiple_of(start + g * SUB, SUB), SUB)
        wide = pl.ds(pl.multiple_of(first + start + g * SUB, SUB), SUB)
        out = pl.ds(pl.multiple_of(g * SUB, SUB), SUB)
        enter = entering(peers, me, first, rows, t_ref, c_ref, g_ref, flow_ref)
        for x in range(width):
            out_ref[out, x, :] = s_ref[x, rows, :] + p_ref[x, wide, :] * enter
        return carry

    lax.fori_loop(0, block // SUB, step, 0, unroll=2)


def stages(size):
    found, stride = [], 1
    while size > 1:
        factor = next(f for f in range(2, size + 1) if size % f == 0)
        if factor == 2 and size % 4 == 0 and (stride > 1 or size % 8):
            factor = 4
        found.append((factor, stride))
        size, stride = size // factor, stride * factor
    return found


def reduce_over(axis, value, rows):
    size = lax.axis_size(axis)
    value, extra = value[:rows], value[None, rows:]
    done = []
    for factor, stride in stages(size):
        sent = jnp.concatenate([value, extra.reshape(-1, LANES)]) if extra.size else value
        got = []
        for turn in range(1, factor):
            pairs = []
            for i in range(size):
                digit = i // stride % factor
                pairs.append((i, i + ((digit + turn) % factor - digit) * stride))
            got.append(lax.ppermute(sent, axis, pairs))
        done.append(factor)
        for piece in got:
            value = value + piece[:rows]
        if extra.size:
            shape = (-1,) + extra.shape[1:]
            extra = jnp.concatenate([extra] + [piece[rows:].reshape(shape) for piece in got])
    return value, extra


def gather_over(axis, value):
    size = lax.axis_size(axis)
    blocks = value[None]
    order = [0]
    bit = size // 2
    while bit:
        got = lax.ppermute(blocks, axis, [(i, i ^ bit) for i in range(size)])
        blocks = jnp.concatenate([blocks, got])
        order = order + [k ^ bit for k in order]
        bit //= 2
    return jnp.concatenate([blocks[order.index(k)][None] for k in range(size)])


def neighbours(axis, value, width):
    size, me = lax.axis_size(axis), lax.axis_index(axis)
    odd = me % 2 == 1
    first, last = value[:, :width], value[:, value.shape[1] - width :]
    near = [(i, i ^ 1) for i in range(size)]
    far = [(i, i + 1) for i in range(1, size - 1, 2)]
    far = lax.ppermute(jnp.where(odd, last, first), axis, far + [(j, i) for i, j in far])
    near = lax.ppermute(jnp.where(odd, first, last), axis, near)
    return jnp.where(odd, near, far), jnp.where(odd, far, near)


def iteration(repeat, m, states, table, rate, wall, me, inflow, kept):
    width, cells = rate.shape
    count, peers = table.shape[1] - PAD, lax.axis_size("gx")
    chunk = count // len(states)
    block = chunk // 2
    if repeat == 0:
        kept["gains"] = run(gains_kernel, (f32(width, count, cells),) * 2, (table, rate), scalar=False)
    rden, prefix = kept["gains"]
    drives = []
    for k, state in enumerate(states):
        if repeat:
            kernel = functools.partial(transport_kernel, k * chunk)
            drives.append(run(kernel, f32(width, chunk, cells), (table, state), scalar=False))
            continue
        drives.append(
            pl.pallas_call(
                functools.partial(first_transport_kernel, k * chunk),
                out_shape=f32(width, chunk, cells),
                in_specs=[VMEM, HBM],
                out_specs=VMEM,
                scratch_shapes=[
                    pltpu.VMEM((chunk, width, cells), jnp.float32),
                    pltpu.SemaphoreType.DMA((BLOCKS,)),
                ],
                compiler_params=PARAMS,
            )(table, state)
        )
    m, extra = reduce_over("vel", m, 13 * width)
    m = m.reshape(13, width, cells)
    before, after = neighbours("gx", m, HALO)
    if repeat == 0:
        total = extra.shape[0] * extra.shape[1] // 4
        kept["features"] = run(
            features_kernel,
            jax.ShapeDtypeStruct((total * LANES, FEATURES), jnp.bfloat16),
            (extra,),
            scratch=(pltpu.VMEM((total, FEATURES, LANES), jnp.float32),),
            scalar=False,
        )
    local, carry, macro, fields = run(
        functools.partial(kinetic_kernel, peers),
        (f32(width, chunk, cells), f32(chunk + width, cells), f32(5, width, cells), f32(10, width, cells)),
        (me, before, m, after, kept["features"], table, rate, wall, drives[0], rden),
        scratch=(
            pltpu.VMEM((13, width + 2 * SUB, cells), jnp.float32),
            pltpu.VMEM((FEATURES, width * cells), jnp.float32),
            pltpu.VMEM((width, cells), jnp.float32),
        ),
    )
    locals_, carries = [local], [gather_over("gx", carry)]
    for k in range(1, len(states)):
        local, carry = run(
            functools.partial(sweep_kernel, k * chunk),
            (f32(width, chunk, cells), f32(chunk, cells)),
            (table, fields, drives[k], rden),
            scalar=False,
        )
        locals_.append(local)
        carries.append(gather_over("gx", carry))
    if repeat == 0:
        kernel = functools.partial(slabs_kernel, peers, width)
        kept["slabs"] = run(kernel, f32(peers, count, cells), (me, table, carries[0]))
    states, m, state = [], None, None
    for k in range(len(locals_)):
        args = (me, table, carries[k], kept["slabs"], inflow, locals_[k], prefix)
        if repeat < ITERS - 1:
            m, state = run(
                functools.partial(next_kernel, peers, k * chunk),
                (f32(13 * width, cells), f32(width, chunk, cells)),
                args if m is None else args + (m,),
                (pltpu.VMEM((chunk, cells), jnp.float32), pltpu.VMEM((13, width, SUB, cells), jnp.float32)),
            )
            states.append(state)
        else:
            rest = [] if k == 0 else [states]
            states = pl.pallas_call(
                functools.partial(last_kernel, peers, k * chunk),
                grid=(2,),
                out_shape=f32(count, width, cells),
                in_specs=[SMEM] + [VMEM] * 6 + [pl.BlockSpec(memory_space=pl.ANY)] * len(rest),
                out_specs=pl.BlockSpec((block, width, cells), lambda i, k=k: (k * 2 + i, 0, 0)),
                input_output_aliases={len(args): 0} if rest else {},
                compiler_params=PARAMS,
            )(*args, *rest)
    return m, states, macro


def per_device(distribution, velocity, weights, collision, solid, inflow):
    count, width, cells = distribution.shape
    peers = lax.axis_size("gx")
    me = lax.axis_index("gx").astype(jnp.int32).reshape(1)
    lines = 4 * count // LANES
    far = functools.partial(pltpu.with_memory_space_constraint, memory_space=pltpu.HBM)
    given = tuple(far(x) for x in (velocity, weights.reshape(1, count), collision, solid, distribution))
    m, table, rate, wall = pl.pallas_call(
        functools.partial(first_kernel, float(width * peers)),
        out_shape=(
            f32(13 * width + lines, cells),
            f32(TABLE, count + PAD, cells),
            f32(width, cells),
            f32(width, cells),
        ),
        in_specs=[HBM] * len(given),
        out_specs=(VMEM,) * 4,
        scratch_shapes=[pltpu.VMEM(x.shape, x.dtype) for x in given]
        + [
            pltpu.VMEM((SUB, count), jnp.float32),
            pltpu.VMEM((13, width, SUB, cells), jnp.float32),
            pltpu.SemaphoreType.DMA((4 + BLOCKS,)),
        ],
        compiler_params=PARAMS,
    )(*given)
    kept, states = {}, given[-1:] * CHUNKS
    for repeat in range(ITERS):
        m, states, macro = iteration(repeat, m, states, table, rate, wall, me, inflow, kept)
    return states, macro


def solution(mesh):
    return jax.shard_map(
        per_device,
        mesh=mesh,
        in_specs=(
            P("vel", "gx", None),
            P(None, "vel"),
            P("vel"),
            P("gx", None),
            P("gx", None),
            P(None, "vel", None),
        ),
        out_specs=(P("vel", "gx", None), P(None, "gx", None)),
        check_vma=False,
    )
```

```python
import functools
import math

import jax
import jax.numpy as jnp
from jax import lax
from jax.experimental import pallas as pl
from jax.experimental.pallas import tpu as pltpu
from jax.sharding import PartitionSpec as P


NZ = 8
ITERS = 2
JACOBI = 2
HALO = JACOBI + 1
pseudo_rate = 0.5
source_gain = 0.5
diffusion = (0.6, 0.8, 0.8, 0.8, 1.0)
viscous_conduction_ratio = 2.0 / 3.0
wall_rate = 4.0
box_volume = 216.0
LOG2E = math.log2(math.e)
LANES = 128
SUB = 8
PAIRS = ((0, 0), (0, 1), (1, 0), (0, 2), (2, 0), (1, 1))
FEATURES = 32
A, B, E, W, HB, HE, BASE, FA, BA, REST = range(10)
TABLE = 10
CHUNKS = 2
BLOCKS = 4
PAD = 8


SMEM = pl.BlockSpec(memory_space=pltpu.SMEM)
VMEM = pl.BlockSpec(memory_space=pltpu.VMEM)
HBM = pl.BlockSpec(memory_space=pltpu.HBM)
PARAMS = pltpu.CompilerParams(vmem_limit_bytes=16 * 1024 * 1024)


def run(kernel, out_shape, args, scratch=(), scalar=True):
    return pl.pallas_call(
        kernel,
        out_shape=out_shape,
        in_specs=([SMEM] if scalar else []) + [VMEM] * (len(args) - (1 if scalar else 0)),
        out_specs=jax.tree.map(lambda _: VMEM, out_shape),
        scratch_shapes=scratch,
        compiler_params=PARAMS,
    )(*args)


def f32(*shape):
    return jax.ShapeDtypeStruct(shape, jnp.float32)


def add_moments(acc, s, t_ref, rows):
    a, b, e = (t_ref[k, rows, :] for k in (A, B, E))
    g = s * t_ref[W, rows, :]
    ga, gb, ge = g * a, g * b, g * e
    gaa, gbb, gee = ga * a, gb * b, ge * e
    gs = gaa + gbb + gee
    terms = (g, ga, gb, ge, gs, gaa, gbb, ga * b, ga * e, gb * e, gs * a, gs * b, gs * e)
    return tuple(old + new for old, new in zip(acc, terms))


def write_moments(m_ref, x, acc):
    for field, value in enumerate(acc):
        m_ref[field, x : x + 1, :] = jnp.sum(value, axis=0, keepdims=True)


def moments_loop(acc_ref, t_ref, first, groups, state_at):
    for x in range(acc_ref.shape[1]):

        def step(g, acc):
            rows = pl.ds(pl.multiple_of(g * SUB, SUB), SUB)
            table_rows = pl.ds(pl.multiple_of(first + g * SUB, SUB), SUB)
            return add_moments(acc, state_at(x, rows), t_ref, table_rows)

        acc = tuple(acc_ref[k, x] for k in range(13))
        acc = lax.fori_loop(0, groups, step, acc, unroll=min(16, groups))
        for k, value in enumerate(acc):
            acc_ref[k, x] = value


def write_moments(m_ref, acc_ref):
    width = acc_ref.shape[1]
    for k in range(13):
        m_ref[k * width : (k + 1) * width, :] = jnp.sum(acc_ref[k], axis=1)


def first_kernel(extent, *refs):
    sources, (m_ref, t_ref, rate_ref, wall_ref), rest = refs[:5], refs[5:9], refs[9:]
    v_ref, w_ref, collision_ref, solid_ref, dist_ref, vw_ref, acc_ref, sem = rest
    count, width = dist_ref.shape[0], dist_ref.shape[1]
    block = count // BLOCKS
    small = [
        pltpu.make_async_copy(source, target, sem.at[k])
        for k, (source, target) in enumerate(zip(sources[:4], (v_ref, w_ref, collision_ref, solid_ref)))
    ]
    large = [
        pltpu.make_async_copy(
            sources[4].at[pl.ds(k * block, block)], dist_ref.at[pl.ds(k * block, block)], sem.at[4 + k]
        )
        for k in range(BLOCKS)
    ]
    for copy in small + large:
        copy.start()
    for copy in small:
        copy.wait()
    wall = solid_ref[...].astype(jnp.float32)
    wall_ref[...] = wall
    rate_ref[...] = collision_ref[...] + wall_rate * wall
    acc_ref[...] = jnp.zeros_like(acc_ref)
    vw_ref[0:3, :] = v_ref[...]
    vw_ref[3:4, :] = w_ref[...]
    vw_ref[4:8, :] = jnp.zeros((4, count), jnp.float32)
    lines = count // LANES
    for k in range(4):
        for j in range(lines):
            row = 13 * width + k * lines + j
            m_ref[row : row + 1, :] = vw_ref[k : k + 1, j * LANES : (j + 1) * LANES]
    columns = vw_ref[...].T

    def wide(k):
        return jnp.broadcast_to(columns[:, k : k + 1], (count, LANES))

    here = slice(0, count)
    a, b, e = wide(0), wide(1), wide(2)
    t_ref[A, here], t_ref[B, here], t_ref[E, here], t_ref[W, here] = a, b, e, wide(3)
    hb, he = 0.5 * jnp.abs(b), 0.5 * jnp.abs(e)
    t_ref[HB, here], t_ref[HE, here] = hb, he
    t_ref[BASE, here] = pseudo_rate + (hb + he) + jnp.abs(a) * extent
    t_ref[FA, here] = jnp.maximum(a, 0.0) * extent
    t_ref[BA, here] = jnp.maximum(-a, 0.0) * extent
    t_ref[REST, here] = (box_volume * (2.0 * math.pi) ** (-1.5)) * jnp.exp(-0.5 * (a * a + b * b + e * e))
    for k, copy in enumerate(large):
        copy.wait()
        moments_loop(
            acc_ref,
            t_ref,
            k * block,
            block // SUB,
            lambda x, rows, k=k: dist_ref[pl.ds(pl.multiple_of(k * block + rows.start, SUB), SUB), x, :],
        )
    write_moments(m_ref, acc_ref)


def gains_kernel(t_ref, rate_ref, rden_ref, p_ref):
    width, count = rden_ref.shape[0], rden_ref.shape[1]

    def step(g, carry):
        rows = pl.ds(pl.multiple_of(g * SUB, SUB), SUB)
        base = t_ref[BASE, rows, :]
        gain = t_ref[FA, rows, :] + t_ref[BA, rows, :]
        ahead = t_ref[A, rows, :] >= 0.0
        steps = []
        for x in range(width):
            rden = 1.0 / (base + rate_ref[x : x + 1, :])
            rden_ref[x, rows, :] = rden
            steps.append(gain * rden)
        up, down = [steps[0]], [steps[-1]]
        for x in range(1, width):
            up.append(up[-1] * steps[x])
            down.append(down[-1] * steps[width - 1 - x])
        for x in range(width):
            p_ref[x, rows, :] = jnp.where(ahead, up[x], down[width - 1 - x])
        return carry

    lax.fori_loop(0, count // SUB, step, 0, unroll=2)


def slabs_kernel(peers, width, me_ref, t_ref, c_ref, g_ref):
    count = g_ref.shape[1]
    below = c_ref.shape[1] - width
    me = me_ref[0]

    def step(g, carry):
        rows = pl.ds(pl.multiple_of(g * SUB, SUB), SUB)
        base = t_ref[BASE, rows, :]
        gain = t_ref[FA, rows, :] + t_ref[BA, rows, :]
        for other in range(1, peers):
            products, powers = [], []
            for x in range(width):
                products.append(base + c_ref[other, below + x : below + x + 1, :])
                powers.append(gain)
            g_ref[other ^ me, rows, :] = times(powers) / times(products)
        return carry

    lax.fori_loop(0, count // SUB, step, 0, unroll=2)


def times(values):
    while len(values) > 1:
        values = [a * b for a, b in zip(values[::2], values[1::2])] + values[len(values) // 2 * 2 :]
    return values[0]


def features_kernel(v_ref, f_ref, row_ref):
    blocks = v_ref.shape[0]
    part = v_ref.shape[1] // 4
    for k in range(blocks):
        a, b, e, w = (v_ref[k, i * part : (i + 1) * part, :] for i in range(4))
        sides = [split(value) for value in (a, b, e, a * a + b * b + e * e)]
        one, zero = jnp.ones_like(a), jnp.zeros_like(a)
        rows = [side[i] for side in sides for i, _ in PAIRS] + [one] * 3 + split(jnp.log2(w))
        rows = rows + [zero] * (FEATURES - len(rows))
        for i, row in enumerate(rows):
            for j in range(part):
                row_ref[k * part + j, i : i + 1, :] = row[j : j + 1, :]

    def turn(r, carry):
        where = pl.ds(pl.multiple_of(r * LANES, LANES), LANES)
        f_ref[where, :] = row_ref[r].T.astype(jnp.bfloat16)
        return carry

    lax.fori_loop(0, blocks * part, turn, 0, unroll=4)


def split(value):
    parts = []
    for _ in range(3):
        part = value.astype(jnp.bfloat16).astype(jnp.float32)
        parts.append(part)
        value = value - part
    return parts


def lane_z():
    return lax.broadcasted_iota(jnp.int32, (1, LANES), 1) % NZ


def y_less(v):
    return pltpu.roll(v, NZ, 1)


def y_more(v):
    return pltpu.roll(v, LANES - NZ, 1)


def z_less(v):
    return jnp.where(lane_z() == 0, pltpu.roll(v, LANES - NZ + 1, 1), pltpu.roll(v, 1, 1))


def z_more(v):
    return jnp.where(lane_z() == NZ - 1, pltpu.roll(v, NZ - 1, 1), pltpu.roll(v, LANES - 1, 1))


def dy(v):
    return 0.5 * (y_more(v) - y_less(v))


def dz(v):
    return 0.5 * (z_more(v) - z_less(v))


def x_less(v):
    return pltpu.roll(v, 1, 0)


def x_more(v):
    return pltpu.roll(v, v.shape[0] - 1, 0)


def fields_of(m):
    rho = m[0]
    inverse = 1.0 / rho
    u = [m[1 + i] * inverse for i in range(3)]
    square = u[0] * u[0] + u[1] * u[1] + u[2] * u[2]
    warm = (m[4] * inverse - square) * (1.0 / 3.0)
    force = rho * warm
    second = [[m[5], m[7], m[8]], [m[7], m[6], m[9]], [m[8], m[9], m[4] - m[5] - m[6]]]
    xx = second[0][0] - rho * u[0] * u[0] - force
    yy = second[1][1] - rho * u[1] * u[1] - force
    xy = second[0][1] - rho * u[0] * u[1]
    xz = second[0][2] - rho * u[0] * u[2]
    yz = second[1][2] - rho * u[1] * u[2]
    heat = []
    for i in range(3):
        inner = u[0] * second[i][0] + u[1] * second[i][1] + u[2] * second[i][2]
        heat.append(0.5 * (m[10 + i] - 2.0 * inner - u[i] * m[4] + 2.0 * rho * u[i] * square))
    return rho, inverse, u, warm, (xx, yy, xy, xz, yz), heat


def correction(rho, inverse, u, warm, stress, heat, inside):
    xx, yy, xy, xz, yz = stress
    zz = -(xx + yy)

    def dx(v):
        v = jnp.where(inside, v, 0.0)
        return 0.5 * (x_more(v) - x_less(v))

    source = [
        dx(rho * u[0]) + dy(rho * u[1]) + dz(rho * u[2]),
        dx(xx) + dy(xy) + dz(xz),
        dx(xy) + dy(yy) + dz(yz),
        dx(xz) + dy(yz) + dz(zz),
        dx(heat[0]) + dy(heat[1]) + dz(heat[2]),
    ]
    scale = [-source_gain * inverse] * 4 + [(-source_gain * 2.0 / 3.0) / (rho * warm)]
    source = [jnp.where(inside, s * c, 0.0) for s, c in zip(source, scale)]
    delta = source
    for _ in range(JACOBI):
        fresh = []
        for mu, s, d in zip(diffusion, source, delta):
            beside = x_less(d) + x_more(d) + y_less(d) + y_more(d) + z_less(d) + z_more(d)
            fresh.append(jnp.where(inside, (s + mu * beside) * (1.0 / (1.0 + 6.0 * mu)), 0.0))
        delta = fresh
    return delta


def transport_kernel(first, t_ref, s_ref, drive_ref):
    transport(first, 0, drive_ref.shape[1], t_ref, lambda x, rows: s_ref[x, rows, :], drive_ref)


def first_transport_kernel(first, t_ref, dist_ref, drive_ref, held_ref, sem):
    block = drive_ref.shape[1] // BLOCKS
    copies = [
        pltpu.make_async_copy(
            dist_ref.at[pl.ds(first + k * block, block)], held_ref.at[pl.ds(k * block, block)], sem.at[k]
        )
        for k in range(BLOCKS)
    ]
    for copy in copies:
        copy.start()
    for k, copy in enumerate(copies):
        copy.wait()
        transport(first, k * block, block, t_ref, lambda x, rows: held_ref[rows, x, :], drive_ref)


def transport(first, start, count, t_ref, state_at, drive_ref):
    width = drive_ref.shape[0]
    lane = lax.broadcasted_iota(jnp.int32, (SUB, LANES), 1)
    z = lane % NZ
    y_down, y_up = (lane + LANES - NZ) % LANES, (lane + NZ) % LANES
    z_down, z_up = lane - z + (z + NZ - 1) % NZ, lane - z + (z + 1) % NZ

    def step(g, carry):
        rows = pl.ds(pl.multiple_of(start + g * SUB, SUB), SUB)
        table_rows = pl.ds(pl.multiple_of(first + start + g * SUB, SUB), SUB)
        hb, he = t_ref[HB, table_rows, :], t_ref[HE, table_rows, :]
        from_y = jnp.where(t_ref[B, table_rows, :] > 0.0, y_down, y_up)
        from_z = jnp.where(t_ref[E, table_rows, :] > 0.0, z_down, z_up)
        for x in range(width):
            s = state_at(x, rows)
            sy = jnp.take_along_axis(s, from_y, axis=1, mode="promise_in_bounds")
            sz = jnp.take_along_axis(s, from_z, axis=1, mode="promise_in_bounds")
            drive_ref[x, rows, :] = pseudo_rate * s + hb * sy + he * sz
        return carry

    lax.fori_loop(0, count // SUB, step, 0, unroll=min(8, count // SUB))


def kinetic_kernel(
    peers, me_ref, before_ref, m_ref, after_ref, f_ref, t_ref, rate_ref, wall_ref, drive_ref, rden_ref,
    s_ref, c_ref, macro_ref, field_ref, pad_ref, cell_ref, total_ref,
):
    width, count = s_ref.shape[0], s_ref.shape[1]
    me = me_ref[0]
    tall = width + 2 * SUB
    own = slice(SUB, SUB + width)
    pad_ref[...] = jnp.ones_like(pad_ref)
    for k in range(13):
        pad_ref[k, SUB - HALO : SUB, :] = before_ref[k]
        pad_ref[k, own, :] = m_ref[k]
        pad_ref[k, SUB + width : SUB + width + HALO, :] = after_ref[k]
    row = lax.broadcasted_iota(jnp.int32, (tall, LANES), 0) + (me * width - SUB)
    inside = (row >= 0) & (row < peers * width)
    rho, inverse, u, warm, stress, heat = fields_of([pad_ref[k] for k in range(13)])
    delta = correction(rho, inverse, u, warm, stress, heat, inside)
    for k, value in enumerate(
        (rho * jnp.exp(delta[0]), u[0] + delta[1], u[1] + delta[2], u[2] + delta[3], warm * jnp.exp(delta[4]))
    ):
        pad_ref[k] = value
        macro_ref[k] = pad_ref[k, own, :]
    for k in range(3):
        pad_ref[5 + k] = heat[k]
    R, U, T = macro_ref[0], [macro_ref[1 + k] for k in range(3)], macro_ref[4]
    q = [pad_ref[5 + k, own, :] for k in range(3)]
    cold = 1.0 / T
    beta = (-0.5 * LOG2E) * cold
    alpha = [(LOG2E * cold) * U[k] for k in range(3)]
    gamma = beta * (U[0] * U[0] + U[1] * U[1] + U[2] * U[2])
    rows = [side[j] for side in (split(v) for v in (*alpha, beta)) for _, j in PAIRS]
    rows = rows + split(gamma) + [jnp.ones_like(T)] * 3
    rows = rows + [jnp.zeros_like(T)] * (FEATURES - len(rows))
    for i, value in enumerate(rows):
        for x in range(width):
            cell_ref[i : i + 1, x * LANES : (x + 1) * LANES] = value[x : x + 1, :]
    cells = cell_ref[...].astype(jnp.bfloat16)

    def mass(r, acc):
        some = f_ref[pl.ds(pl.multiple_of(r * LANES, LANES), LANES), :]
        power = jnp.dot(some, cells, preferred_element_type=jnp.float32)
        weight = jnp.exp2(power)
        return acc + jnp.sum(weight.reshape(LANES // SUB, SUB, width * LANES), axis=0)

    acc = lax.fori_loop(0, f_ref.shape[0] // LANES, mass, jnp.zeros((SUB, width * LANES), jnp.float32), unroll=8)
    acc = jnp.sum(acc, axis=0, keepdims=True)
    for x in range(width):
        total_ref[x : x + 1, :] = acc[:, x * LANES : (x + 1) * LANES]
    wall, rate = wall_ref[...], rate_ref[...]
    third = (1.0 - viscous_conduction_ratio) / (5.0 * R * T * T)
    values = [*U, beta, *(v * third for v in q), cold]
    values += [(1.0 - wall) * R * rate / total_ref[...], wall * R * rate]
    for k, value in enumerate(values):
        field_ref[k] = value

    sweep(0, field_ref, t_ref, drive_ref, rden_ref, s_ref, c_ref)
    c_ref[count : count + width, :] = rate


def sweep_kernel(first, t_ref, field_ref, drive_ref, rden_ref, s_ref, c_ref):
    sweep(first, field_ref, t_ref, drive_ref, rden_ref, s_ref, c_ref)


def sweep(first, field_ref, t_ref, drive_ref, rden_ref, s_ref, c_ref):
    width, count = s_ref.shape[0], s_ref.shape[1]

    def both(g):
        return (
            pl.ds(pl.multiple_of(g * SUB, SUB), SUB),
            pl.ds(pl.multiple_of(first + g * SUB, SUB), SUB),
        )

    for x in range(width):
        ux, uy, uz, power, qx, qy, qz, inv, maxwell, rest = (
            jnp.broadcast_to(field_ref[k, x : x + 1, :], (SUB, LANES)) for k in range(10)
        )

        def ahead(g, carry):
            rows, wide = both(g)
            a, b, e = (t_ref[k, wide, :] for k in (A, B, E))
            cx, cy, cz = a - ux, b - uy, e - uz
            square = cx * cx + cy * cy + cz * cz
            expo = jnp.exp2(square * power)
            flux = cx * qx + cy * qy + cz * qz
            target = (expo * maxwell) * (1.0 + flux * (square * inv - 5.0)) + rest * t_ref[REST, wide, :]
            rden = rden_ref[x, wide, :]
            value = (drive_ref[x, rows, :] + target) * rden
            if x:
                value = value + (t_ref[FA, wide, :] * rden) * s_ref[x - 1, rows, :]
            s_ref[x, rows, :] = value
            return carry

        lax.fori_loop(0, count // SUB, ahead, 0, unroll=min(32, count // SUB))

    def back(g, carry):
        rows, wide = both(g)
        ba = t_ref[BA, wide, :]
        value = s_ref[width - 1, rows, :]
        last = value
        for x in range(width - 2, -1, -1):
            value = s_ref[x, rows, :] + (ba * rden_ref[x, wide, :]) * value
            s_ref[x, rows, :] = value
        c_ref[rows, :] = jnp.where(t_ref[A, wide, :] >= 0.0, last, value)
        return carry

    lax.fori_loop(0, count // SUB, back, 0, unroll=4)


def entering(peers, me, first, rows, t_ref, c_ref, g_ref, flow_ref):
    wide = pl.ds(pl.multiple_of(first + rows.start, SUB), SUB)
    up, down = flow_ref[0, wide, :], flow_ref[1, wide, :]
    for d in range(peers - 1):
        up = jnp.where(d < me, g_ref[d, wide, :] * up + c_ref[d ^ me, rows, :], up)
    for d in range(peers - 1, 0, -1):
        down = jnp.where(d > me, g_ref[d, wide, :] * down + c_ref[d ^ me, rows, :], down)
    return jnp.where(t_ref[A, wide, :] >= 0.0, up, down)


def next_kernel(peers, first, me_ref, t_ref, c_ref, g_ref, flow_ref, s_ref, p_ref, *refs):
    partial_ref, (m_ref, state_ref, enter_ref, acc_ref) = refs[:-4], refs[-4:]
    count = s_ref.shape[1]
    me = me_ref[0]

    def enter(g, carry):
        rows = pl.ds(pl.multiple_of(g * SUB, SUB), SUB)
        enter_ref[rows, :] = entering(peers, me, first, rows, t_ref, c_ref, g_ref, flow_ref)
        return carry

    lax.fori_loop(0, count // SUB, enter, 0, unroll=2)
    acc_ref[...] = jnp.zeros_like(acc_ref)

    def state_at(x, rows):
        wide = pl.ds(pl.multiple_of(first + rows.start, SUB), SUB)
        s = s_ref[x, rows, :] + p_ref[x, wide, :] * enter_ref[rows, :]
        state_ref[x, rows, :] = s
        return s

    moments_loop(acc_ref, t_ref, first, count // SUB, state_at)
    write_moments(m_ref, acc_ref)
    if partial_ref:
        m_ref[...] += partial_ref[0][...]


def last_kernel(peers, first, me_ref, t_ref, c_ref, g_ref, flow_ref, s_ref, p_ref, *refs):
    out_ref, held_ref, sem = refs[-3:]
    count, width = held_ref.shape[0], held_ref.shape[1]
    block = count // BLOCKS
    me = me_ref[0]
    copies = [
        pltpu.make_async_copy(
            held_ref.at[pl.ds(k * block, block)], out_ref.at[pl.ds(first + k * block, block)], sem.at[k]
        )
        for k in range(BLOCKS)
    ]
    for k, copy in enumerate(copies):

        def step(g, carry, k=k):
            rows = pl.ds(pl.multiple_of(k * block + g * SUB, SUB), SUB)
            wide = pl.ds(pl.multiple_of(first + k * block + g * SUB, SUB), SUB)
            enter = entering(peers, me, first, rows, t_ref, c_ref, g_ref, flow_ref)
            for x in range(width):
                held_ref[rows, x, :] = s_ref[x, rows, :] + p_ref[x, wide, :] * enter
            return carry

        lax.fori_loop(0, block // SUB, step, 0, unroll=4)
        copy.start()
    for copy in copies:
        copy.wait()


def stages(size):
    found, stride = [], 1
    while size > 1:
        factor = next(f for f in range(2, size + 1) if size % f == 0)
        if factor == 2 and size % 4 == 0 and (stride > 1 or size % 8):
            factor = 4
        found.append((factor, stride))
        size, stride = size // factor, stride * factor
    return found


def reduce_over(axis, value, rows):
    size = lax.axis_size(axis)
    value, extra = value[:rows], value[None, rows:]
    done = []
    for factor, stride in stages(size):
        sent = jnp.concatenate([value, extra.reshape(-1, LANES)]) if extra.size else value
        got = []
        for turn in range(1, factor):
            pairs = []
            for i in range(size):
                digit = i // stride % factor
                pairs.append((i, i + ((digit + turn) % factor - digit) * stride))
            got.append(lax.ppermute(sent, axis, pairs))
        done.append(factor)
        for piece in got:
            value = value + piece[:rows]
        if extra.size:
            shape = (-1,) + extra.shape[1:]
            extra = jnp.concatenate([extra] + [piece[rows:].reshape(shape) for piece in got])
    return value, extra


def gather_over(axis, value):
    size = lax.axis_size(axis)
    blocks = value[None]
    order = [0]
    bit = size // 2
    while bit:
        got = lax.ppermute(blocks, axis, [(i, i ^ bit) for i in range(size)])
        blocks = jnp.concatenate([blocks, got])
        order = order + [k ^ bit for k in order]
        bit //= 2
    return jnp.concatenate([blocks[order.index(k)][None] for k in range(size)])


def neighbours(axis, value, width):
    size, me = lax.axis_size(axis), lax.axis_index(axis)
    odd = me % 2 == 1
    first, last = value[:, :width], value[:, value.shape[1] - width :]
    near = [(i, i ^ 1) for i in range(size)]
    far = [(i, i + 1) for i in range(1, size - 1, 2)]
    far = lax.ppermute(jnp.where(odd, last, first), axis, far + [(j, i) for i, j in far])
    near = lax.ppermute(jnp.where(odd, first, last), axis, near)
    return jnp.where(odd, near, far), jnp.where(odd, far, near)


def iteration(repeat, m, states, table, rate, wall, me, inflow, kept):
    width, cells = rate.shape
    count, peers = table.shape[1] - PAD, lax.axis_size("gx")
    chunk = count // len(states)
    if repeat == 0:
        kept["gains"] = run(gains_kernel, (f32(width, count, cells),) * 2, (table, rate), scalar=False)
    rden, prefix = kept["gains"]
    drives = []
    for k, state in enumerate(states):
        if repeat:
            kernel = functools.partial(transport_kernel, k * chunk)
            drives.append(run(kernel, f32(width, chunk, cells), (table, state), scalar=False))
            continue
        drives.append(
            pl.pallas_call(
                functools.partial(first_transport_kernel, k * chunk),
                out_shape=f32(width, chunk, cells),
                in_specs=[VMEM, HBM],
                out_specs=VMEM,
                scratch_shapes=[
                    pltpu.VMEM((chunk, width, cells), jnp.float32),
                    pltpu.SemaphoreType.DMA((BLOCKS,)),
                ],
                compiler_params=PARAMS,
            )(table, state)
        )
    m, extra = reduce_over("vel", m, 13 * width)
    m = m.reshape(13, width, cells)
    before, after = neighbours("gx", m, HALO)
    if repeat == 0:
        total = extra.shape[0] * extra.shape[1] // 4
        kept["features"] = run(
            features_kernel,
            jax.ShapeDtypeStruct((total * LANES, FEATURES), jnp.bfloat16),
            (extra,),
            scratch=(pltpu.VMEM((total, FEATURES, LANES), jnp.float32),),
            scalar=False,
        )
    local, carry, macro, fields = run(
        functools.partial(kinetic_kernel, peers),
        (f32(width, chunk, cells), f32(chunk + width, cells), f32(5, width, cells), f32(10, width, cells)),
        (me, before, m, after, kept["features"], table, rate, wall, drives[0], rden),
        scratch=(
            pltpu.VMEM((13, width + 2 * SUB, cells), jnp.float32),
            pltpu.VMEM((FEATURES, width * cells), jnp.float32),
            pltpu.VMEM((width, cells), jnp.float32),
        ),
    )
    locals_, carries = [local], [gather_over("gx", carry)]
    for k in range(1, len(states)):
        local, carry = run(
            functools.partial(sweep_kernel, k * chunk),
            (f32(width, chunk, cells), f32(chunk, cells)),
            (table, fields, drives[k], rden),
            scalar=False,
        )
        locals_.append(local)
        carries.append(gather_over("gx", carry))
    if repeat == 0:
        kernel = functools.partial(slabs_kernel, peers, width)
        kept["slabs"] = run(kernel, f32(peers, count, cells), (me, table, carries[0]))
    states, m, state = [], None, None
    for k in range(len(locals_)):
        args = (me, table, carries[k], kept["slabs"], inflow, locals_[k], prefix)
        if repeat < ITERS - 1:
            m, state = run(
                functools.partial(next_kernel, peers, k * chunk),
                (f32(13 * width, cells), f32(width, chunk, cells)),
                args if m is None else args + (m,),
                (pltpu.VMEM((chunk, cells), jnp.float32), pltpu.VMEM((13, width, SUB, cells), jnp.float32)),
            )
            states.append(state)
        else:
            rest = [] if k == 0 else [states]
            states = pl.pallas_call(
                functools.partial(last_kernel, peers, k * chunk),
                out_shape=f32(count, width, cells),
                in_specs=[SMEM] + [VMEM] * 6 + [HBM] * len(rest),
                out_specs=HBM,
                scratch_shapes=[
                    pltpu.VMEM((chunk, width, cells), jnp.float32),
                    pltpu.SemaphoreType.DMA((BLOCKS,)),
                ],
                input_output_aliases={len(args): 0} if rest else {},
                compiler_params=PARAMS,
            )(*args, *rest)
    return m, states, macro


def per_device(distribution, velocity, weights, collision, solid, inflow):
    count, width, cells = distribution.shape
    peers = lax.axis_size("gx")
    me = lax.axis_index("gx").astype(jnp.int32).reshape(1)
    lines = 4 * count // LANES
    far = functools.partial(pltpu.with_memory_space_constraint, memory_space=pltpu.HBM)
    given = tuple(far(x) for x in (velocity, weights.reshape(1, count), collision, solid, distribution))
    m, table, rate, wall = pl.pallas_call(
        functools.partial(first_kernel, float(width * peers)),
        out_shape=(
            f32(13 * width + lines, cells),
            f32(TABLE, count + PAD, cells),
            f32(width, cells),
            f32(width, cells),
        ),
        in_specs=[HBM] * len(given),
        out_specs=(VMEM,) * 4,
        scratch_shapes=[pltpu.VMEM(x.shape, x.dtype) for x in given]
        + [
            pltpu.VMEM((SUB, count), jnp.float32),
            pltpu.VMEM((13, width, SUB, cells), jnp.float32),
            pltpu.SemaphoreType.DMA((4 + BLOCKS,)),
        ],
        compiler_params=PARAMS,
    )(*given)
    kept, states = {}, given[-1:] * CHUNKS
    for repeat in range(ITERS):
        m, states, macro = iteration(repeat, m, states, table, rate, wall, me, inflow, kept)
    return states, macro


def solution(mesh):
    return jax.shard_map(
        per_device,
        mesh=mesh,
        in_specs=(
            P("vel", "gx", None),
            P(None, "vel"),
            P("vel"),
            P("gx", None),
            P("gx", None),
            P(None, "vel", None),
        ),
        out_specs=(P("vel", "gx", None), P(None, "gx", None)),
        check_vma=False,
    )
```

```python
import functools
import math

import jax
import jax.numpy as jnp
from jax import lax
from jax.experimental import pallas as pl
from jax.experimental.pallas import tpu as pltpu
from jax.sharding import PartitionSpec as P


NZ = 8
ITERS = 2
JACOBI = 2
HALO = JACOBI + 1
pseudo_rate = 0.5
source_gain = 0.5
diffusion = (0.6, 0.8, 0.8, 0.8, 1.0)
viscous_conduction_ratio = 2.0 / 3.0
wall_rate = 4.0
box_volume = 216.0
LOG2E = math.log2(math.e)
LANES = 128
SUB = 8
PAIRS = ((0, 0), (0, 1), (1, 0), (0, 2), (2, 0), (1, 1))
FEATURES = 32
A, B, E, W, BASE, FA, BA, REST = range(8)
BASIC = 4
TABLE = 8
CHUNKS = 2
FIRST = 4
BLOCKS = 4
PAD = 8


SMEM = pl.BlockSpec(memory_space=pltpu.SMEM)
VMEM = pl.BlockSpec(memory_space=pltpu.VMEM)
HBM = pl.BlockSpec(memory_space=pltpu.HBM)
PARAMS = pltpu.CompilerParams(vmem_limit_bytes=16 * 1024 * 1024)


def run(kernel, out_shape, args, scratch=(), scalar=True):
    return pl.pallas_call(
        kernel,
        out_shape=out_shape,
        in_specs=([SMEM] if scalar else []) + [VMEM] * (len(args) - (1 if scalar else 0)),
        out_specs=jax.tree.map(lambda _: VMEM, out_shape),
        scratch_shapes=scratch,
        compiler_params=PARAMS,
    )(*args)


def fit(trips, most):
    return max(u for u in range(1, most + 1) if trips % u == 0)


def f32(*shape):
    return jax.ShapeDtypeStruct(shape, jnp.float32)


def add_moments(acc, s, t_ref, rows):
    a, b, e = (t_ref[k, rows, :] for k in (A, B, E))
    g = s * t_ref[W, rows, :]
    ga, gb, ge = g * a, g * b, g * e
    gaa, gbb, gee = ga * a, gb * b, ge * e
    gs = gaa + gbb + gee
    terms = (g, ga, gb, ge, gs, gaa, gbb, ga * b, ga * e, gb * e, gs * a, gs * b, gs * e)
    return tuple(old + new for old, new in zip(acc, terms))


def write_moments(m_ref, x, acc):
    for field, value in enumerate(acc):
        m_ref[field, x : x + 1, :] = jnp.sum(value, axis=0, keepdims=True)


def moments_loop(acc_ref, t_ref, first, groups, state_at):
    for x in range(acc_ref.shape[1]):

        def step(g, acc):
            rows = pl.ds(pl.multiple_of(g * SUB, SUB), SUB)
            table_rows = pl.ds(pl.multiple_of(first + g * SUB, SUB), SUB)
            return add_moments(acc, state_at(x, rows), t_ref, table_rows)

        acc = tuple(acc_ref[k, x] for k in range(13))
        acc = lax.fori_loop(0, groups, step, acc, unroll=fit(groups, 16))
        for k, value in enumerate(acc):
            acc_ref[k, x] = value


def write_moments(m_ref, acc_ref):
    width = acc_ref.shape[1]
    for k in range(13):
        m_ref[k * width : (k + 1) * width, :] = jnp.sum(acc_ref[k], axis=1)


def first_kernel(*refs):
    sources, (m_ref, t_ref, rate_ref, wall_ref), rest = refs[:5], refs[5:9], refs[9:]
    v_ref, w_ref, collision_ref, solid_ref, dist_ref, vw_ref, acc_ref, sem = rest
    count, width = dist_ref.shape[0], dist_ref.shape[1]
    block = count // BLOCKS
    small = [
        pltpu.make_async_copy(source, target, sem.at[k])
        for k, (source, target) in enumerate(zip(sources[:4], (v_ref, w_ref, collision_ref, solid_ref)))
    ]
    large = [
        pltpu.make_async_copy(
            sources[4].at[pl.ds(k * block, block)], dist_ref.at[pl.ds(k * block, block)], sem.at[4 + k]
        )
        for k in range(BLOCKS)
    ]
    for copy in small + large:
        copy.start()
    for copy in small:
        copy.wait()
    wall = solid_ref[...].astype(jnp.float32)
    wall_ref[...] = wall
    rate_ref[...] = collision_ref[...] + wall_rate * wall
    acc_ref[...] = jnp.zeros_like(acc_ref)
    vw_ref[0:3, :] = v_ref[...]
    vw_ref[3:4, :] = w_ref[...]
    vw_ref[4:8, :] = jnp.zeros((4, count), jnp.float32)
    lines = count // LANES
    for k in range(4):
        for j in range(lines):
            row = 13 * width + k * lines + j
            m_ref[row : row + 1, :] = vw_ref[k : k + 1, j * LANES : (j + 1) * LANES]
    columns = vw_ref[...].T

    def wide(k):
        return jnp.broadcast_to(columns[:, k : k + 1], (count, LANES))

    here = slice(0, count)
    a, b, e = wide(0), wide(1), wide(2)
    t_ref[A, here], t_ref[B, here], t_ref[E, here], t_ref[W, here] = a, b, e, wide(3)
    for k, copy in enumerate(large):
        copy.wait()
        moments_loop(
            acc_ref,
            t_ref,
            k * block,
            block // SUB,
            lambda x, rows, k=k: dist_ref[pl.ds(pl.multiple_of(k * block + rows.start, SUB), SUB), x, :],
        )
    write_moments(m_ref, acc_ref)


def gains_kernel(extent, v_ref, rate_ref, t_ref, rden_ref, p_ref):
    width, count = rden_ref.shape[0], rden_ref.shape[1]

    def step(g, carry):
        rows = pl.ds(pl.multiple_of(g * SUB, SUB), SUB)
        a, b, e, w = (v_ref[k, rows, :] for k in (A, B, E, W))
        base = pseudo_rate + (0.5 * jnp.abs(b) + 0.5 * jnp.abs(e)) + jnp.abs(a) * extent
        gain = jnp.abs(a) * extent
        ahead = a >= 0.0
        rest = (box_volume * (2.0 * math.pi) ** (-1.5)) * jnp.exp(-0.5 * (a * a + b * b + e * e))
        whole = (a, b, e, w, base, jnp.maximum(a, 0.0) * extent, jnp.maximum(-a, 0.0) * extent, rest)
        for k, value in enumerate(whole):
            t_ref[k, rows, :] = value
        steps = []
        for x in range(width):
            rden = 1.0 / (base + rate_ref[x : x + 1, :])
            rden_ref[x, rows, :] = rden
            steps.append(gain * rden)
        up, down = [steps[0]], [steps[-1]]
        for x in range(1, width):
            up.append(up[-1] * steps[x])
            down.append(down[-1] * steps[width - 1 - x])
        for x in range(width):
            p_ref[x, rows, :] = jnp.where(ahead, up[x], down[width - 1 - x])
        return carry

    lax.fori_loop(0, count // SUB, step, 0, unroll=2)


def slabs_kernel(peers, width, me_ref, t_ref, c_ref, g_ref):
    count = g_ref.shape[1]
    below = c_ref.shape[1] - width
    me = me_ref[0]

    def step(g, carry):
        rows = pl.ds(pl.multiple_of(g * SUB, SUB), SUB)
        base = t_ref[BASE, rows, :]
        gain = t_ref[FA, rows, :] + t_ref[BA, rows, :]
        for other in range(1, peers):
            products, powers = [], []
            for x in range(width):
                products.append(base + c_ref[other, below + x : below + x + 1, :])
                powers.append(gain)
            g_ref[other ^ me, rows, :] = times(powers) / times(products)
        return carry

    lax.fori_loop(0, count // SUB, step, 0, unroll=2)


def times(values):
    while len(values) > 1:
        values = [a * b for a, b in zip(values[::2], values[1::2])] + values[len(values) // 2 * 2 :]
    return values[0]


def features_kernel(v_ref, f_ref, row_ref):
    blocks = v_ref.shape[0]
    part = v_ref.shape[1] // 4
    for k in range(blocks):
        a, b, e, w = (v_ref[k, i * part : (i + 1) * part, :] for i in range(4))
        sides = [split(value) for value in (a, b, e, a * a + b * b + e * e)]
        one, zero = jnp.ones_like(a), jnp.zeros_like(a)
        rows = [side[i] for side in sides for i, _ in PAIRS] + [one] * 3 + split(jnp.log2(w))
        rows = rows + [zero] * (FEATURES - len(rows))
        for i, row in enumerate(rows):
            for j in range(part):
                row_ref[k * part + j, i : i + 1, :] = row[j : j + 1, :]

    def turn(r, carry):
        where = pl.ds(pl.multiple_of(r * LANES, LANES), LANES)
        f_ref[where, :] = row_ref[r].T.astype(jnp.bfloat16)
        return carry

    lax.fori_loop(0, blocks * part, turn, 0, unroll=4)


def split(value):
    parts = []
    for _ in range(3):
        part = value.astype(jnp.bfloat16).astype(jnp.float32)
        parts.append(part)
        value = value - part
    return parts


def lane_z():
    return lax.broadcasted_iota(jnp.int32, (1, LANES), 1) % NZ


def y_less(v):
    return pltpu.roll(v, NZ, 1)


def y_more(v):
    return pltpu.roll(v, LANES - NZ, 1)


def z_less(v):
    return jnp.where(lane_z() == 0, pltpu.roll(v, LANES - NZ + 1, 1), pltpu.roll(v, 1, 1))


def z_more(v):
    return jnp.where(lane_z() == NZ - 1, pltpu.roll(v, NZ - 1, 1), pltpu.roll(v, LANES - 1, 1))


def dy(v):
    return 0.5 * (y_more(v) - y_less(v))


def dz(v):
    return 0.5 * (z_more(v) - z_less(v))


def x_less(v):
    return pltpu.roll(v, 1, 0)


def x_more(v):
    return pltpu.roll(v, v.shape[0] - 1, 0)


def fields_of(m):
    rho = m[0]
    inverse = 1.0 / rho
    u = [m[1 + i] * inverse for i in range(3)]
    square = u[0] * u[0] + u[1] * u[1] + u[2] * u[2]
    warm = (m[4] * inverse - square) * (1.0 / 3.0)
    force = rho * warm
    second = [[m[5], m[7], m[8]], [m[7], m[6], m[9]], [m[8], m[9], m[4] - m[5] - m[6]]]
    xx = second[0][0] - rho * u[0] * u[0] - force
    yy = second[1][1] - rho * u[1] * u[1] - force
    xy = second[0][1] - rho * u[0] * u[1]
    xz = second[0][2] - rho * u[0] * u[2]
    yz = second[1][2] - rho * u[1] * u[2]
    heat = []
    for i in range(3):
        inner = u[0] * second[i][0] + u[1] * second[i][1] + u[2] * second[i][2]
        heat.append(0.5 * (m[10 + i] - 2.0 * inner - u[i] * m[4] + 2.0 * rho * u[i] * square))
    return rho, inverse, u, warm, (xx, yy, xy, xz, yz), heat


def correction(rho, inverse, u, warm, stress, heat, inside):
    xx, yy, xy, xz, yz = stress
    zz = -(xx + yy)

    def dx(v):
        v = jnp.where(inside, v, 0.0)
        return 0.5 * (x_more(v) - x_less(v))

    source = [
        dx(rho * u[0]) + dy(rho * u[1]) + dz(rho * u[2]),
        dx(xx) + dy(xy) + dz(xz),
        dx(xy) + dy(yy) + dz(yz),
        dx(xz) + dy(yz) + dz(zz),
        dx(heat[0]) + dy(heat[1]) + dz(heat[2]),
    ]
    scale = [-source_gain * inverse] * 4 + [(-source_gain * 2.0 / 3.0) / (rho * warm)]
    source = [jnp.where(inside, s * c, 0.0) for s, c in zip(source, scale)]
    delta = source
    for _ in range(JACOBI):
        fresh = []
        for mu, s, d in zip(diffusion, source, delta):
            beside = x_less(d) + x_more(d) + y_less(d) + y_more(d) + z_less(d) + z_more(d)
            fresh.append(jnp.where(inside, (s + mu * beside) * (1.0 / (1.0 + 6.0 * mu)), 0.0))
        delta = fresh
    return delta


def transport_kernel(first, t_ref, s_ref, drive_ref):
    transport(first, 0, drive_ref.shape[1], t_ref, lambda x, rows: s_ref[x, rows, :], drive_ref)


def first_transport_kernel(first, t_ref, dist_ref, drive_ref, held_ref, sem):
    block = drive_ref.shape[1] // BLOCKS
    copies = [
        pltpu.make_async_copy(
            dist_ref.at[pl.ds(first + k * block, block)], held_ref.at[pl.ds(k * block, block)], sem.at[k]
        )
        for k in range(BLOCKS)
    ]
    for copy in copies:
        copy.start()
    for k, copy in enumerate(copies):
        copy.wait()
        transport(first, k * block, block, t_ref, lambda x, rows: held_ref[rows, x, :], drive_ref)


def transport(first, start, count, t_ref, state_at, drive_ref):
    width = drive_ref.shape[0]
    lane = lax.broadcasted_iota(jnp.int32, (SUB, LANES), 1)
    z = lane % NZ
    y_down, y_up = (lane + LANES - NZ) % LANES, (lane + NZ) % LANES
    z_down, z_up = lane - z + (z + NZ - 1) % NZ, lane - z + (z + 1) % NZ

    def step(g, carry):
        rows = pl.ds(pl.multiple_of(start + g * SUB, SUB), SUB)
        table_rows = pl.ds(pl.multiple_of(first + start + g * SUB, SUB), SUB)
        b, e = t_ref[B, table_rows, :], t_ref[E, table_rows, :]
        hb, he = 0.5 * jnp.abs(b), 0.5 * jnp.abs(e)
        from_y = jnp.where(b > 0.0, y_down, y_up)
        from_z = jnp.where(e > 0.0, z_down, z_up)
        for x in range(width):
            s = state_at(x, rows)
            sy = jnp.take_along_axis(s, from_y, axis=1, mode="promise_in_bounds")
            sz = jnp.take_along_axis(s, from_z, axis=1, mode="promise_in_bounds")
            drive_ref[x, rows, :] = pseudo_rate * s + hb * sy + he * sz
        return carry

    lax.fori_loop(0, count // SUB, step, 0, unroll=fit(count // SUB, 8))


def kinetic_kernel(
    peers, me_ref, before_ref, m_ref, after_ref, f_ref, t_ref, rate_ref, wall_ref, drive_ref, rden_ref,
    s_ref, c_ref, macro_ref, field_ref, pad_ref, cell_ref, total_ref,
):
    width, count = s_ref.shape[0], s_ref.shape[1]
    me = me_ref[0]
    tall = width + 2 * SUB
    own = slice(SUB, SUB + width)
    pad_ref[...] = jnp.ones_like(pad_ref)
    for k in range(13):
        pad_ref[k, SUB - HALO : SUB, :] = before_ref[k]
        pad_ref[k, own, :] = m_ref[k]
        pad_ref[k, SUB + width : SUB + width + HALO, :] = after_ref[k]
    row = lax.broadcasted_iota(jnp.int32, (tall, LANES), 0) + (me * width - SUB)
    inside = (row >= 0) & (row < peers * width)
    rho, inverse, u, warm, stress, heat = fields_of([pad_ref[k] for k in range(13)])
    delta = correction(rho, inverse, u, warm, stress, heat, inside)
    for k, value in enumerate(
        (rho * jnp.exp(delta[0]), u[0] + delta[1], u[1] + delta[2], u[2] + delta[3], warm * jnp.exp(delta[4]))
    ):
        pad_ref[k] = value
        macro_ref[k] = pad_ref[k, own, :]
    for k in range(3):
        pad_ref[5 + k] = heat[k]
    R, U, T = macro_ref[0], [macro_ref[1 + k] for k in range(3)], macro_ref[4]
    q = [pad_ref[5 + k, own, :] for k in range(3)]
    cold = 1.0 / T
    beta = (-0.5 * LOG2E) * cold
    alpha = [(LOG2E * cold) * U[k] for k in range(3)]
    gamma = beta * (U[0] * U[0] + U[1] * U[1] + U[2] * U[2])
    rows = [side[j] for side in (split(v) for v in (*alpha, beta)) for _, j in PAIRS]
    rows = rows + split(gamma) + [jnp.ones_like(T)] * 3
    rows = rows + [jnp.zeros_like(T)] * (FEATURES - len(rows))
    for i, value in enumerate(rows):
        for x in range(width):
            cell_ref[i : i + 1, x * LANES : (x + 1) * LANES] = value[x : x + 1, :]
    cells = cell_ref[...].astype(jnp.bfloat16)

    def mass(r, acc):
        some = f_ref[pl.ds(pl.multiple_of(r * LANES, LANES), LANES), :]
        power = jnp.dot(some, cells, preferred_element_type=jnp.float32)
        weight = jnp.exp2(power)
        return acc + jnp.sum(weight.reshape(LANES // SUB, SUB, width * LANES), axis=0)

    acc = lax.fori_loop(0, f_ref.shape[0] // LANES, mass, jnp.zeros((SUB, width * LANES), jnp.float32), unroll=fit(f_ref.shape[0] // LANES, 32))
    acc = jnp.sum(acc, axis=0, keepdims=True)
    for x in range(width):
        total_ref[x : x + 1, :] = acc[:, x * LANES : (x + 1) * LANES]
    wall, rate = wall_ref[...], rate_ref[...]
    third = (1.0 - viscous_conduction_ratio) / (5.0 * R * T * T)
    values = [*U, beta, *(v * third for v in q), cold]
    values += [(1.0 - wall) * R * rate / total_ref[...], wall * R * rate]
    for k, value in enumerate(values):
        field_ref[k] = value

    sweep(0, field_ref, t_ref, drive_ref, rden_ref, s_ref, c_ref)
    c_ref[count : count + width, :] = rate


def sweep_kernel(first, t_ref, field_ref, drive_ref, rden_ref, s_ref, c_ref):
    sweep(first, field_ref, t_ref, drive_ref, rden_ref, s_ref, c_ref)


def sweep(first, field_ref, t_ref, drive_ref, rden_ref, s_ref, c_ref):
    width, count = s_ref.shape[0], s_ref.shape[1]

    def both(g):
        return (
            pl.ds(pl.multiple_of(g * SUB, SUB), SUB),
            pl.ds(pl.multiple_of(first + g * SUB, SUB), SUB),
        )

    for x in range(width):
        ux, uy, uz, power, qx, qy, qz, inv, maxwell, rest = (
            jnp.broadcast_to(field_ref[k, x : x + 1, :], (SUB, LANES)) for k in range(10)
        )

        def ahead(g, carry):
            rows, wide = both(g)
            a, b, e = (t_ref[k, wide, :] for k in (A, B, E))
            cx, cy, cz = a - ux, b - uy, e - uz
            square = cx * cx + cy * cy + cz * cz
            expo = jnp.exp2(square * power)
            flux = cx * qx + cy * qy + cz * qz
            target = (expo * maxwell) * (1.0 + flux * (square * inv - 5.0)) + rest * t_ref[REST, wide, :]
            rden = rden_ref[x, wide, :]
            value = (drive_ref[x, rows, :] + target) * rden
            if x:
                value = value + (t_ref[FA, wide, :] * rden) * s_ref[x - 1, rows, :]
            s_ref[x, rows, :] = value
            return carry

        lax.fori_loop(0, count // SUB, ahead, 0, unroll=fit(count // SUB, 32))

    def back(g, carry):
        rows, wide = both(g)
        ba = t_ref[BA, wide, :]
        value = s_ref[width - 1, rows, :]
        last = value
        for x in range(width - 2, -1, -1):
            value = s_ref[x, rows, :] + (ba * rden_ref[x, wide, :]) * value
            s_ref[x, rows, :] = value
        c_ref[rows, :] = jnp.where(t_ref[A, wide, :] >= 0.0, last, value)
        return carry

    lax.fori_loop(0, count // SUB, back, 0, unroll=fit(count // SUB, 4))


def entering(peers, me, first, rows, t_ref, c_ref, g_ref, flow_ref):
    wide = pl.ds(pl.multiple_of(first + rows.start, SUB), SUB)
    up, down = flow_ref[0, wide, :], flow_ref[1, wide, :]
    for d in range(peers - 1):
        up = jnp.where(d < me, g_ref[d, wide, :] * up + c_ref[d ^ me, rows, :], up)
    for d in range(peers - 1, 0, -1):
        down = jnp.where(d > me, g_ref[d, wide, :] * down + c_ref[d ^ me, rows, :], down)
    return jnp.where(t_ref[A, wide, :] >= 0.0, up, down)


def next_kernel(peers, first, me_ref, t_ref, c_ref, g_ref, flow_ref, s_ref, p_ref, *refs):
    partial_ref, (m_ref, state_ref, enter_ref, acc_ref) = refs[:-4], refs[-4:]
    count = s_ref.shape[1]
    me = me_ref[0]

    def enter(g, carry):
        rows = pl.ds(pl.multiple_of(g * SUB, SUB), SUB)
        enter_ref[rows, :] = entering(peers, me, first, rows, t_ref, c_ref, g_ref, flow_ref)
        return carry

    lax.fori_loop(0, count // SUB, enter, 0, unroll=2)
    acc_ref[...] = jnp.zeros_like(acc_ref)

    def state_at(x, rows):
        wide = pl.ds(pl.multiple_of(first + rows.start, SUB), SUB)
        s = s_ref[x, rows, :] + p_ref[x, wide, :] * enter_ref[rows, :]
        state_ref[x, rows, :] = s
        return s

    moments_loop(acc_ref, t_ref, first, count // SUB, state_at)
    write_moments(m_ref, acc_ref)
    if partial_ref:
        m_ref[...] += partial_ref[0][...]


def last_kernel(peers, first, me_ref, t_ref, c_ref, g_ref, flow_ref, s_ref, p_ref, *refs):
    out_ref, held_ref, sem = refs[-3:]
    count, width = held_ref.shape[0], held_ref.shape[1]
    block = count // BLOCKS
    me = me_ref[0]
    copies = [
        pltpu.make_async_copy(
            held_ref.at[pl.ds(k * block, block)], out_ref.at[pl.ds(first + k * block, block)], sem.at[k]
        )
        for k in range(BLOCKS)
    ]
    for k, copy in enumerate(copies):

        def step(g, carry, k=k):
            rows = pl.ds(pl.multiple_of(k * block + g * SUB, SUB), SUB)
            wide = pl.ds(pl.multiple_of(first + k * block + g * SUB, SUB), SUB)
            enter = entering(peers, me, first, rows, t_ref, c_ref, g_ref, flow_ref)
            for x in range(width):
                held_ref[rows, x, :] = s_ref[x, rows, :] + p_ref[x, wide, :] * enter
            return carry

        lax.fori_loop(0, block // SUB, step, 0, unroll=fit(block // SUB, 4))
        copy.start()
    for copy in copies:
        copy.wait()


def stages(size):
    found, stride = [], 1
    while size > 1:
        factor = next(f for f in range(2, size + 1) if size % f == 0)
        if factor == 2 and size % 4 == 0 and (stride > 1 or size % 8):
            factor = 4
        found.append((factor, stride))
        size, stride = size // factor, stride * factor
    return found


def reduce_over(axis, value, rows):
    size = lax.axis_size(axis)
    value, extra = value[:rows], value[None, rows:]
    done = []
    for factor, stride in stages(size):
        sent = jnp.concatenate([value, extra.reshape(-1, LANES)]) if extra.size else value
        got = []
        for turn in range(1, factor):
            pairs = []
            for i in range(size):
                digit = i // stride % factor
                pairs.append((i, i + ((digit + turn) % factor - digit) * stride))
            got.append(lax.ppermute(sent, axis, pairs))
        done.append(factor)
        for piece in got:
            value = value + piece[:rows]
        if extra.size:
            shape = (-1,) + extra.shape[1:]
            extra = jnp.concatenate([extra] + [piece[rows:].reshape(shape) for piece in got])
    return value, extra


def gather_over(axis, value):
    size = lax.axis_size(axis)
    blocks = value[None]
    order = [0]
    bit = size // 2
    while bit:
        got = lax.ppermute(blocks, axis, [(i, i ^ bit) for i in range(size)])
        blocks = jnp.concatenate([blocks, got])
        order = order + [k ^ bit for k in order]
        bit //= 2
    return jnp.concatenate([blocks[order.index(k)][None] for k in range(size)])


def neighbours(axis, value, width):
    size, me = lax.axis_size(axis), lax.axis_index(axis)
    odd = me % 2 == 1
    first, last = value[:, :width], value[:, value.shape[1] - width :]
    near = [(i, i ^ 1) for i in range(size)]
    far = [(i, i + 1) for i in range(1, size - 1, 2)]
    far = lax.ppermute(jnp.where(odd, last, first), axis, far + [(j, i) for i, j in far])
    near = lax.ppermute(jnp.where(odd, first, last), axis, near)
    return jnp.where(odd, near, far), jnp.where(odd, far, near)


def iteration(repeat, m, states, basic, rate, wall, me, inflow, kept):
    width, cells = rate.shape
    count, peers = basic.shape[1] - PAD, lax.axis_size("gx")
    share = count * FIRST // 8
    starts, sizes = (0, share), (share, count - share)
    if repeat == 0:
        kept["gains"] = run(
            functools.partial(gains_kernel, float(width * peers)),
            (f32(TABLE, count + PAD, cells),) + (f32(width, count, cells),) * 2,
            (basic, rate),
            scalar=False,
        )
    table, rden, prefix = kept["gains"]
    drives = []
    for state, start, chunk in zip(states, starts, sizes):
        if repeat:
            kernel = functools.partial(transport_kernel, start)
            drives.append(run(kernel, f32(width, chunk, cells), (basic, state), scalar=False))
            continue
        drives.append(
            pl.pallas_call(
                functools.partial(first_transport_kernel, start),
                out_shape=f32(width, chunk, cells),
                in_specs=[VMEM, HBM],
                out_specs=VMEM,
                scratch_shapes=[
                    pltpu.VMEM((chunk, width, cells), jnp.float32),
                    pltpu.SemaphoreType.DMA((BLOCKS,)),
                ],
                compiler_params=PARAMS,
            )(basic, state)
        )
    m, extra = reduce_over("vel", m, 13 * width)
    m = m.reshape(13, width, cells)
    before, after = neighbours("gx", m, HALO)
    if repeat == 0:
        total = extra.shape[0] * extra.shape[1] // 4
        kept["features"] = run(
            features_kernel,
            jax.ShapeDtypeStruct((total * LANES, FEATURES), jnp.bfloat16),
            (extra,),
            scratch=(pltpu.VMEM((total, FEATURES, LANES), jnp.float32),),
            scalar=False,
        )
    chunk = sizes[0]
    local, carry, macro, fields = run(
        functools.partial(kinetic_kernel, peers),
        (f32(width, chunk, cells), f32(chunk + width, cells), f32(5, width, cells), f32(10, width, cells)),
        (me, before, m, after, kept["features"], table, rate, wall, drives[0], rden),
        scratch=(
            pltpu.VMEM((13, width + 2 * SUB, cells), jnp.float32),
            pltpu.VMEM((FEATURES, width * cells), jnp.float32),
            pltpu.VMEM((width, cells), jnp.float32),
        ),
    )
    locals_, carries = [local], [gather_over("gx", carry)]
    for k in range(1, len(states)):
        chunk = sizes[k]
        local, carry = run(
            functools.partial(sweep_kernel, starts[k]),
            (f32(width, chunk, cells), f32(chunk, cells)),
            (table, fields, drives[k], rden),
            scalar=False,
        )
        locals_.append(local)
        carries.append(gather_over("gx", carry))
    if repeat == 0:
        kernel = functools.partial(slabs_kernel, peers, width)
        kept["slabs"] = run(kernel, f32(peers, count, cells), (me, table, carries[0]))
    states, m, state = [], None, None
    for k, chunk in enumerate(sizes):
        args = (me, table, carries[k], kept["slabs"], inflow, locals_[k], prefix)
        if repeat < ITERS - 1:
            m, state = run(
                functools.partial(next_kernel, peers, starts[k]),
                (f32(13 * width, cells), f32(width, chunk, cells)),
                args if m is None else args + (m,),
                (pltpu.VMEM((chunk, cells), jnp.float32), pltpu.VMEM((13, width, SUB, cells), jnp.float32)),
            )
            states.append(state)
        else:
            rest = [] if k == 0 else [states]
            states = pl.pallas_call(
                functools.partial(last_kernel, peers, starts[k]),
                out_shape=f32(count, width, cells),
                in_specs=[SMEM] + [VMEM] * 6 + [HBM] * len(rest),
                out_specs=HBM,
                scratch_shapes=[
                    pltpu.VMEM((chunk, width, cells), jnp.float32),
                    pltpu.SemaphoreType.DMA((BLOCKS,)),
                ],
                input_output_aliases={len(args): 0} if rest else {},
                compiler_params=PARAMS,
            )(*args, *rest)
    return m, states, macro


def per_device(distribution, velocity, weights, collision, solid, inflow):
    count, width, cells = distribution.shape
    me = lax.axis_index("gx").astype(jnp.int32).reshape(1)
    lines = 4 * count // LANES
    far = functools.partial(pltpu.with_memory_space_constraint, memory_space=pltpu.HBM)
    given = tuple(far(x) for x in (velocity, weights.reshape(1, count), collision, solid, distribution))
    m, table, rate, wall = pl.pallas_call(
        first_kernel,
        out_shape=(
            f32(13 * width + lines, cells),
            f32(BASIC, count + PAD, cells),
            f32(width, cells),
            f32(width, cells),
        ),
        in_specs=[HBM] * len(given),
        out_specs=(VMEM,) * 4,
        scratch_shapes=[pltpu.VMEM(x.shape, x.dtype) for x in given]
        + [
            pltpu.VMEM((SUB, count), jnp.float32),
            pltpu.VMEM((13, width, SUB, cells), jnp.float32),
            pltpu.SemaphoreType.DMA((4 + BLOCKS,)),
        ],
        compiler_params=PARAMS,
    )(*given)
    kept, states = {}, given[-1:] * CHUNKS
    for repeat in range(ITERS):
        m, states, macro = iteration(repeat, m, states, table, rate, wall, me, inflow, kept)
    return states, macro


def solution(mesh):
    return jax.shard_map(
        per_device,
        mesh=mesh,
        in_specs=(
            P("vel", "gx", None),
            P(None, "vel"),
            P("vel"),
            P("gx", None),
            P("gx", None),
            P(None, "vel", None),
        ),
        out_specs=(P("vel", "gx", None), P(None, "gx", None)),
        check_vma=False,
    )
```

```python
import functools
import math

import jax
import jax.numpy as jnp
from jax import lax
from jax.experimental import pallas as pl
from jax.experimental.pallas import tpu as pltpu
from jax.sharding import PartitionSpec as P


NZ = 8
ITERS = 2
JACOBI = 2
HALO = JACOBI + 1
pseudo_rate = 0.5
source_gain = 0.5
diffusion = (0.6, 0.8, 0.8, 0.8, 1.0)
viscous_conduction_ratio = 2.0 / 3.0
wall_rate = 4.0
box_volume = 216.0
LOG2E = math.log2(math.e)
LANES = 128
SUB = 8
PAIRS = ((0, 0), (0, 1), (1, 0), (0, 2), (2, 0), (1, 1))
FEATURES = 32
A, B, E, W, BASE, FA, BA, REST = range(8)
BASIC = 4
TABLE = 8
CHUNKS = 2
FIRST = 4
BLOCKS = 4
PAD = 8


SMEM = pl.BlockSpec(memory_space=pltpu.SMEM)
VMEM = pl.BlockSpec(memory_space=pltpu.VMEM)
HBM = pl.BlockSpec(memory_space=pltpu.HBM)
PARAMS = pltpu.CompilerParams(vmem_limit_bytes=16 * 1024 * 1024)


def run(kernel, out_shape, args, scratch=(), scalar=True):
    return pl.pallas_call(
        kernel,
        out_shape=out_shape,
        in_specs=([SMEM] if scalar else []) + [VMEM] * (len(args) - (1 if scalar else 0)),
        out_specs=jax.tree.map(lambda _: VMEM, out_shape),
        scratch_shapes=scratch,
        compiler_params=PARAMS,
    )(*args)


def fit(trips, most):
    return max(u for u in range(1, most + 1) if trips % u == 0)


def f32(*shape):
    return jax.ShapeDtypeStruct(shape, jnp.float32)


def add_moments(acc, s, t_ref, rows):
    a, b, e = (t_ref[k, rows, :] for k in (A, B, E))
    g = s * t_ref[W, rows, :]
    ga, gb, ge = g * a, g * b, g * e
    gaa, gbb, gee = ga * a, gb * b, ge * e
    gs = gaa + gbb + gee
    terms = (g, ga, gb, ge, gs, gaa, gbb, ga * b, ga * e, gb * e, gs * a, gs * b, gs * e)
    return tuple(old + new for old, new in zip(acc, terms))


def write_moments(m_ref, x, acc):
    for field, value in enumerate(acc):
        m_ref[field, x : x + 1, :] = jnp.sum(value, axis=0, keepdims=True)


def moments_loop(acc_ref, t_ref, first, groups, state_at):
    for x in range(acc_ref.shape[1]):

        def step(g, acc):
            rows = pl.ds(pl.multiple_of(g * SUB, SUB), SUB)
            table_rows = pl.ds(pl.multiple_of(first + g * SUB, SUB), SUB)
            return add_moments(acc, state_at(x, rows), t_ref, table_rows)

        acc = tuple(acc_ref[k, x] for k in range(13))
        acc = lax.fori_loop(0, groups, step, acc, unroll=fit(groups, 16))
        for k, value in enumerate(acc):
            acc_ref[k, x] = value


def write_moments(m_ref, acc_ref):
    width = acc_ref.shape[1]
    for k in range(13):
        m_ref[k * width : (k + 1) * width, :] = jnp.sum(acc_ref[k], axis=1)


def first_kernel(*refs):
    sources, (m_ref, t_ref, rate_ref, wall_ref), rest = refs[:5], refs[5:9], refs[9:]
    v_ref, w_ref, collision_ref, solid_ref, dist_ref, vw_ref, acc_ref, sem = rest
    count, width = dist_ref.shape[0], dist_ref.shape[1]
    block = count // BLOCKS
    small = [
        pltpu.make_async_copy(source, target, sem.at[k])
        for k, (source, target) in enumerate(zip(sources[:4], (v_ref, w_ref, collision_ref, solid_ref)))
    ]
    large = [
        pltpu.make_async_copy(
            sources[4].at[pl.ds(k * block, block)], dist_ref.at[pl.ds(k * block, block)], sem.at[4 + k]
        )
        for k in range(BLOCKS)
    ]
    for copy in small + large:
        copy.start()
    for copy in small:
        copy.wait()
    wall = solid_ref[...].astype(jnp.float32)
    wall_ref[...] = wall
    rate_ref[...] = collision_ref[...] + wall_rate * wall
    acc_ref[...] = jnp.zeros_like(acc_ref)
    vw_ref[0:3, :] = v_ref[...]
    vw_ref[3:4, :] = w_ref[...]
    vw_ref[4:8, :] = jnp.zeros((4, count), jnp.float32)
    lines = count // LANES
    for k in range(4):
        for j in range(lines):
            row = 13 * width + k * lines + j
            m_ref[row : row + 1, :] = vw_ref[k : k + 1, j * LANES : (j + 1) * LANES]
    columns = vw_ref[...].T

    def wide(k):
        return jnp.broadcast_to(columns[:, k : k + 1], (count, LANES))

    here = slice(0, count)
    a, b, e = wide(0), wide(1), wide(2)
    t_ref[A, here], t_ref[B, here], t_ref[E, here], t_ref[W, here] = a, b, e, wide(3)
    for k, copy in enumerate(large):
        copy.wait()
        moments_loop(
            acc_ref,
            t_ref,
            k * block,
            block // SUB,
            lambda x, rows, k=k: dist_ref[pl.ds(pl.multiple_of(k * block + rows.start, SUB), SUB), x, :],
        )
    write_moments(m_ref, acc_ref)


def gains_kernel(extent, v_ref, rate_ref, t_ref, rden_ref, p_ref):
    width, count = rden_ref.shape[0], rden_ref.shape[1]

    def step(g, carry):
        rows = pl.ds(pl.multiple_of(g * SUB, SUB), SUB)
        a, b, e, w = (v_ref[k, rows, :] for k in (A, B, E, W))
        base = pseudo_rate + (0.5 * jnp.abs(b) + 0.5 * jnp.abs(e)) + jnp.abs(a) * extent
        gain = jnp.abs(a) * extent
        ahead = a >= 0.0
        rest = (box_volume * (2.0 * math.pi) ** (-1.5)) * jnp.exp(-0.5 * (a * a + b * b + e * e))
        whole = (a, b, e, w, base, jnp.maximum(a, 0.0) * extent, jnp.maximum(-a, 0.0) * extent, rest)
        for k, value in enumerate(whole):
            t_ref[k, rows, :] = value
        steps = []
        for x in range(width):
            rden = 1.0 / (base + rate_ref[x : x + 1, :])
            rden_ref[x, rows, :] = rden
            steps.append(gain * rden)
        up, down = [steps[0]], [steps[-1]]
        for x in range(1, width):
            up.append(up[-1] * steps[x])
            down.append(down[-1] * steps[width - 1 - x])
        for x in range(width):
            p_ref[x, rows, :] = jnp.where(ahead, up[x], down[width - 1 - x])
        return carry

    lax.fori_loop(0, count // SUB, step, 0, unroll=2)


def slabs_kernel(peers, width, me_ref, t_ref, c_ref, g_ref):
    count = g_ref.shape[1]
    below = c_ref.shape[1] - width
    me = me_ref[0]

    def step(g, carry):
        rows = pl.ds(pl.multiple_of(g * SUB, SUB), SUB)
        base = t_ref[BASE, rows, :]
        gain = t_ref[FA, rows, :] + t_ref[BA, rows, :]
        for other in range(1, peers):
            products, powers = [], []
            for x in range(width):
                products.append(base + c_ref[other, below + x : below + x + 1, :])
                powers.append(gain)
            g_ref[other ^ me, rows, :] = times(powers) / times(products)
        return carry

    lax.fori_loop(0, count // SUB, step, 0, unroll=2)


def times(values):
    while len(values) > 1:
        values = [a * b for a, b in zip(values[::2], values[1::2])] + values[len(values) // 2 * 2 :]
    return values[0]


def features_kernel(v_ref, f_ref, center_ref, row_ref):
    blocks = v_ref.shape[0]
    part = v_ref.shape[1] // 4
    centers = []
    for i in range(3):
        total = sum(v_ref[k, i * part : (i + 1) * part, :] for k in range(blocks))
        centers.append(jnp.sum(total, keepdims=True) * (1.0 / (blocks * part * LANES)))
        center_ref[i : i + 1, :] = jnp.broadcast_to(centers[i], (1, LANES))
    for k in range(blocks):
        a, b, e, w = (v_ref[k, i * part : (i + 1) * part, :] for i in range(4))
        a, b, e = (value - center for value, center in zip((a, b, e), centers))
        sides = [split(value) for value in (a, b, e, a * a + b * b + e * e)]
        one, zero = jnp.ones_like(a), jnp.zeros_like(a)
        rows = [side[i] for side in sides for i, _ in PAIRS] + [one] * 3 + split(jnp.log2(w))
        rows = rows + [zero] * (FEATURES - len(rows))
        for i, row in enumerate(rows):
            for j in range(part):
                row_ref[k * part + j, i : i + 1, :] = row[j : j + 1, :]

    def turn(r, carry):
        where = pl.ds(pl.multiple_of(r * LANES, LANES), LANES)
        f_ref[where, :] = row_ref[r].T.astype(jnp.bfloat16)
        return carry

    lax.fori_loop(0, blocks * part, turn, 0, unroll=4)


def split(value):
    parts = []
    for _ in range(3):
        part = value.astype(jnp.bfloat16).astype(jnp.float32)
        parts.append(part)
        value = value - part
    return parts


def lane_z():
    return lax.broadcasted_iota(jnp.int32, (1, LANES), 1) % NZ


def y_less(v):
    return pltpu.roll(v, NZ, 1)


def y_more(v):
    return pltpu.roll(v, LANES - NZ, 1)


def z_less(v):
    return jnp.where(lane_z() == 0, pltpu.roll(v, LANES - NZ + 1, 1), pltpu.roll(v, 1, 1))


def z_more(v):
    return jnp.where(lane_z() == NZ - 1, pltpu.roll(v, NZ - 1, 1), pltpu.roll(v, LANES - 1, 1))


def dy(v):
    return 0.5 * (y_more(v) - y_less(v))


def dz(v):
    return 0.5 * (z_more(v) - z_less(v))


def x_less(v):
    return pltpu.roll(v, 1, 0)


def x_more(v):
    return pltpu.roll(v, v.shape[0] - 1, 0)


def fields_of(m):
    rho = m[0]
    inverse = 1.0 / rho
    u = [m[1 + i] * inverse for i in range(3)]
    square = u[0] * u[0] + u[1] * u[1] + u[2] * u[2]
    warm = (m[4] * inverse - square) * (1.0 / 3.0)
    force = rho * warm
    second = [[m[5], m[7], m[8]], [m[7], m[6], m[9]], [m[8], m[9], m[4] - m[5] - m[6]]]
    xx = second[0][0] - rho * u[0] * u[0] - force
    yy = second[1][1] - rho * u[1] * u[1] - force
    xy = second[0][1] - rho * u[0] * u[1]
    xz = second[0][2] - rho * u[0] * u[2]
    yz = second[1][2] - rho * u[1] * u[2]
    heat = []
    for i in range(3):
        inner = u[0] * second[i][0] + u[1] * second[i][1] + u[2] * second[i][2]
        heat.append(0.5 * (m[10 + i] - 2.0 * inner - u[i] * m[4] + 2.0 * rho * u[i] * square))
    return rho, inverse, u, warm, (xx, yy, xy, xz, yz), heat


def correction(rho, inverse, u, warm, stress, heat, inside):
    xx, yy, xy, xz, yz = stress
    zz = -(xx + yy)

    def dx(v):
        v = jnp.where(inside, v, 0.0)
        return 0.5 * (x_more(v) - x_less(v))

    source = [
        dx(rho * u[0]) + dy(rho * u[1]) + dz(rho * u[2]),
        dx(xx) + dy(xy) + dz(xz),
        dx(xy) + dy(yy) + dz(yz),
        dx(xz) + dy(yz) + dz(zz),
        dx(heat[0]) + dy(heat[1]) + dz(heat[2]),
    ]
    scale = [-source_gain * inverse] * 4 + [(-source_gain * 2.0 / 3.0) / (rho * warm)]
    source = [jnp.where(inside, s * c, 0.0) for s, c in zip(source, scale)]
    delta = source
    for _ in range(JACOBI):
        fresh = []
        for mu, s, d in zip(diffusion, source, delta):
            beside = x_less(d) + x_more(d) + y_less(d) + y_more(d) + z_less(d) + z_more(d)
            fresh.append(jnp.where(inside, (s + mu * beside) * (1.0 / (1.0 + 6.0 * mu)), 0.0))
        delta = fresh
    return delta


def transport_kernel(first, t_ref, s_ref, drive_ref):
    transport(first, 0, drive_ref.shape[1], t_ref, lambda x, rows: s_ref[x, rows, :], drive_ref)


def first_transport_kernel(first, t_ref, dist_ref, drive_ref, held_ref, sem):
    block = drive_ref.shape[1] // BLOCKS
    copies = [
        pltpu.make_async_copy(
            dist_ref.at[pl.ds(first + k * block, block)], held_ref.at[pl.ds(k * block, block)], sem.at[k]
        )
        for k in range(BLOCKS)
    ]
    for copy in copies:
        copy.start()
    for k, copy in enumerate(copies):
        copy.wait()
        transport(first, k * block, block, t_ref, lambda x, rows: held_ref[rows, x, :], drive_ref)


def transport(first, start, count, t_ref, state_at, drive_ref):
    width = drive_ref.shape[0]
    lane = lax.broadcasted_iota(jnp.int32, (SUB, LANES), 1)
    z = lane % NZ
    y_down, y_up = (lane + LANES - NZ) % LANES, (lane + NZ) % LANES
    z_down, z_up = lane - z + (z + NZ - 1) % NZ, lane - z + (z + 1) % NZ

    def step(g, carry):
        rows = pl.ds(pl.multiple_of(start + g * SUB, SUB), SUB)
        table_rows = pl.ds(pl.multiple_of(first + start + g * SUB, SUB), SUB)
        b, e = t_ref[B, table_rows, :], t_ref[E, table_rows, :]
        hb, he = 0.5 * jnp.abs(b), 0.5 * jnp.abs(e)
        from_y = jnp.where(b > 0.0, y_down, y_up)
        from_z = jnp.where(e > 0.0, z_down, z_up)
        for x in range(width):
            s = state_at(x, rows)
            sy = jnp.take_along_axis(s, from_y, axis=1, mode="promise_in_bounds")
            sz = jnp.take_along_axis(s, from_z, axis=1, mode="promise_in_bounds")
            drive_ref[x, rows, :] = pseudo_rate * s + hb * sy + he * sz
        return carry

    lax.fori_loop(0, count // SUB, step, 0, unroll=fit(count // SUB, 8))


def kinetic_kernel(
    peers, me_ref, before_ref, m_ref, after_ref, f_ref, center_ref, t_ref, rate_ref, wall_ref, drive_ref, rden_ref,
    s_ref, c_ref, macro_ref, field_ref, pad_ref, cell_ref, total_ref,
):
    width, count = s_ref.shape[0], s_ref.shape[1]
    me = me_ref[0]
    tall = width + 2 * SUB
    own = slice(SUB, SUB + width)
    pad_ref[...] = jnp.ones_like(pad_ref)
    for k in range(13):
        pad_ref[k, SUB - HALO : SUB, :] = before_ref[k]
        pad_ref[k, own, :] = m_ref[k]
        pad_ref[k, SUB + width : SUB + width + HALO, :] = after_ref[k]
    row = lax.broadcasted_iota(jnp.int32, (tall, LANES), 0) + (me * width - SUB)
    inside = (row >= 0) & (row < peers * width)
    rho, inverse, u, warm, stress, heat = fields_of([pad_ref[k] for k in range(13)])
    delta = correction(rho, inverse, u, warm, stress, heat, inside)
    for k, value in enumerate(
        (rho * jnp.exp(delta[0]), u[0] + delta[1], u[1] + delta[2], u[2] + delta[3], warm * jnp.exp(delta[4]))
    ):
        pad_ref[k] = value
        macro_ref[k] = pad_ref[k, own, :]
    for k in range(3):
        pad_ref[5 + k] = heat[k]
    R, U, T = macro_ref[0], [macro_ref[1 + k] for k in range(3)], macro_ref[4]
    q = [pad_ref[5 + k, own, :] for k in range(3)]
    cold = 1.0 / T
    beta = (-0.5 * LOG2E) * cold
    V = [U[k] - center_ref[k : k + 1, :] for k in range(3)]
    alpha = [(LOG2E * cold) * V[k] for k in range(3)]
    gamma = beta * (V[0] * V[0] + V[1] * V[1] + V[2] * V[2])
    rows = [side[j] for side in (split(v) for v in (*alpha, beta)) for _, j in PAIRS]
    rows = rows + split(gamma) + [jnp.ones_like(T)] * 3
    rows = rows + [jnp.zeros_like(T)] * (FEATURES - len(rows))
    for i, value in enumerate(rows):
        for x in range(width):
            cell_ref[i : i + 1, x * LANES : (x + 1) * LANES] = value[x : x + 1, :]
    cells = cell_ref[...].astype(jnp.bfloat16)

    def mass(r, acc):
        some = f_ref[pl.ds(pl.multiple_of(r * LANES, LANES), LANES), :]
        power = jnp.dot(some, cells, preferred_element_type=jnp.float32)
        weight = jnp.exp2(power)
        return acc + jnp.sum(weight.reshape(LANES // SUB, SUB, width * LANES), axis=0)

    acc = lax.fori_loop(0, f_ref.shape[0] // LANES, mass, jnp.zeros((SUB, width * LANES), jnp.float32), unroll=fit(f_ref.shape[0] // LANES, 32))
    acc = jnp.sum(acc, axis=0, keepdims=True)
    for x in range(width):
        total_ref[x : x + 1, :] = acc[:, x * LANES : (x + 1) * LANES]
    wall, rate = wall_ref[...], rate_ref[...]
    third = (1.0 - viscous_conduction_ratio) / (5.0 * R * T * T)
    values = [*U, beta, *(v * third for v in q), cold]
    values += [(1.0 - wall) * R * rate / total_ref[...], wall * R * rate]
    for k, value in enumerate(values):
        field_ref[k] = value

    sweep(0, field_ref, t_ref, drive_ref, rden_ref, s_ref, c_ref)
    c_ref[count : count + width, :] = rate


def sweep_kernel(first, t_ref, field_ref, drive_ref, rden_ref, s_ref, c_ref):
    sweep(first, field_ref, t_ref, drive_ref, rden_ref, s_ref, c_ref)


def sweep(first, field_ref, t_ref, drive_ref, rden_ref, s_ref, c_ref):
    width, count = s_ref.shape[0], s_ref.shape[1]

    def both(g):
        return (
            pl.ds(pl.multiple_of(g * SUB, SUB), SUB),
            pl.ds(pl.multiple_of(first + g * SUB, SUB), SUB),
        )

    for x in range(width):
        ux, uy, uz, power, qx, qy, qz, inv, maxwell, rest = (
            jnp.broadcast_to(field_ref[k, x : x + 1, :], (SUB, LANES)) for k in range(10)
        )

        def ahead(g, carry):
            rows, wide = both(g)
            a, b, e = (t_ref[k, wide, :] for k in (A, B, E))
            cx, cy, cz = a - ux, b - uy, e - uz
            square = cx * cx + cy * cy + cz * cz
            expo = jnp.exp2(square * power)
            flux = cx * qx + cy * qy + cz * qz
            target = (expo * maxwell) * (1.0 + flux * (square * inv - 5.0)) + rest * t_ref[REST, wide, :]
            rden = rden_ref[x, wide, :]
            value = (drive_ref[x, rows, :] + target) * rden
            if x:
                value = value + (t_ref[FA, wide, :] * rden) * s_ref[x - 1, rows, :]
            s_ref[x, rows, :] = value
            return carry

        lax.fori_loop(0, count // SUB, ahead, 0, unroll=fit(count // SUB, 32))

    def back(g, carry):
        rows, wide = both(g)
        ba = t_ref[BA, wide, :]
        value = s_ref[width - 1, rows, :]
        last = value
        for x in range(width - 2, -1, -1):
            value = s_ref[x, rows, :] + (ba * rden_ref[x, wide, :]) * value
            s_ref[x, rows, :] = value
        c_ref[rows, :] = jnp.where(t_ref[A, wide, :] >= 0.0, last, value)
        return carry

    lax.fori_loop(0, count // SUB, back, 0, unroll=fit(count // SUB, 4))


def entering(peers, me, first, rows, t_ref, c_ref, g_ref, flow_ref):
    wide = pl.ds(pl.multiple_of(first + rows.start, SUB), SUB)
    up, down = flow_ref[0, wide, :], flow_ref[1, wide, :]
    for d in range(peers - 1):
        up = jnp.where(d < me, g_ref[d, wide, :] * up + c_ref[d ^ me, rows, :], up)
    for d in range(peers - 1, 0, -1):
        down = jnp.where(d > me, g_ref[d, wide, :] * down + c_ref[d ^ me, rows, :], down)
    return jnp.where(t_ref[A, wide, :] >= 0.0, up, down)


def next_kernel(peers, first, me_ref, t_ref, c_ref, g_ref, flow_ref, s_ref, p_ref, *refs):
    partial_ref, (m_ref, state_ref, enter_ref, acc_ref) = refs[:-4], refs[-4:]
    count = s_ref.shape[1]
    me = me_ref[0]

    def enter(g, carry):
        rows = pl.ds(pl.multiple_of(g * SUB, SUB), SUB)
        enter_ref[rows, :] = entering(peers, me, first, rows, t_ref, c_ref, g_ref, flow_ref)
        return carry

    lax.fori_loop(0, count // SUB, enter, 0, unroll=2)
    acc_ref[...] = jnp.zeros_like(acc_ref)

    def state_at(x, rows):
        wide = pl.ds(pl.multiple_of(first + rows.start, SUB), SUB)
        s = s_ref[x, rows, :] + p_ref[x, wide, :] * enter_ref[rows, :]
        state_ref[x, rows, :] = s
        return s

    moments_loop(acc_ref, t_ref, first, count // SUB, state_at)
    write_moments(m_ref, acc_ref)
    if partial_ref:
        m_ref[...] += partial_ref[0][...]


def last_kernel(peers, first, me_ref, t_ref, c_ref, g_ref, flow_ref, s_ref, p_ref, *refs):
    out_ref, held_ref, sem = refs[-3:]
    count, width = held_ref.shape[0], held_ref.shape[1]
    block = count // BLOCKS
    me = me_ref[0]
    copies = [
        pltpu.make_async_copy(
            held_ref.at[pl.ds(k * block, block)], out_ref.at[pl.ds(first + k * block, block)], sem.at[k]
        )
        for k in range(BLOCKS)
    ]
    for k, copy in enumerate(copies):

        def step(g, carry, k=k):
            rows = pl.ds(pl.multiple_of(k * block + g * SUB, SUB), SUB)
            wide = pl.ds(pl.multiple_of(first + k * block + g * SUB, SUB), SUB)
            enter = entering(peers, me, first, rows, t_ref, c_ref, g_ref, flow_ref)
            for x in range(width):
                held_ref[rows, x, :] = s_ref[x, rows, :] + p_ref[x, wide, :] * enter
            return carry

        lax.fori_loop(0, block // SUB, step, 0, unroll=fit(block // SUB, 4))
        copy.start()
    for copy in copies:
        copy.wait()


def stages(size):
    found, stride = [], 1
    while size > 1:
        factor = next(f for f in range(2, size + 1) if size % f == 0)
        if factor == 2 and size % 4 == 0 and (stride > 1 or size % 8):
            factor = 4
        found.append((factor, stride))
        size, stride = size // factor, stride * factor
    return found


def reduce_over(axis, value, rows):
    size = lax.axis_size(axis)
    value, extra = value[:rows], value[None, rows:]
    done = []
    for factor, stride in stages(size):
        sent = jnp.concatenate([value, extra.reshape(-1, LANES)]) if extra.size else value
        got = []
        for turn in range(1, factor):
            pairs = []
            for i in range(size):
                digit = i // stride % factor
                pairs.append((i, i + ((digit + turn) % factor - digit) * stride))
            got.append(lax.ppermute(sent, axis, pairs))
        done.append(factor)
        for piece in got:
            value = value + piece[:rows]
        if extra.size:
            shape = (-1,) + extra.shape[1:]
            extra = jnp.concatenate([extra] + [piece[rows:].reshape(shape) for piece in got])
    return value, extra


def gather_over(axis, value):
    size = lax.axis_size(axis)
    blocks = value[None]
    order = [0]
    bit = size // 2
    while bit:
        got = lax.ppermute(blocks, axis, [(i, i ^ bit) for i in range(size)])
        blocks = jnp.concatenate([blocks, got])
        order = order + [k ^ bit for k in order]
        bit //= 2
    return jnp.concatenate([blocks[order.index(k)][None] for k in range(size)])


def neighbours(axis, value, width):
    size, me = lax.axis_size(axis), lax.axis_index(axis)
    odd = me % 2 == 1
    first, last = value[:, :width], value[:, value.shape[1] - width :]
    near = [(i, i ^ 1) for i in range(size)]
    far = [(i, i + 1) for i in range(1, size - 1, 2)]
    far = lax.ppermute(jnp.where(odd, last, first), axis, far + [(j, i) for i, j in far])
    near = lax.ppermute(jnp.where(odd, first, last), axis, near)
    return jnp.where(odd, near, far), jnp.where(odd, far, near)


def iteration(repeat, m, states, basic, rate, wall, me, inflow, kept):
    width, cells = rate.shape
    count, peers = basic.shape[1] - PAD, lax.axis_size("gx")
    share = count * FIRST // 8
    starts, sizes = (0, share), (share, count - share)
    if repeat == 0:
        kept["gains"] = run(
            functools.partial(gains_kernel, float(width * peers)),
            (f32(TABLE, count + PAD, cells),) + (f32(width, count, cells),) * 2,
            (basic, rate),
            scalar=False,
        )
    table, rden, prefix = kept["gains"]
    drives = []
    for state, start, chunk in zip(states, starts, sizes):
        if repeat:
            kernel = functools.partial(transport_kernel, start)
            drives.append(run(kernel, f32(width, chunk, cells), (basic, state), scalar=False))
            continue
        drives.append(
            pl.pallas_call(
                functools.partial(first_transport_kernel, start),
                out_shape=f32(width, chunk, cells),
                in_specs=[VMEM, HBM],
                out_specs=VMEM,
                scratch_shapes=[
                    pltpu.VMEM((chunk, width, cells), jnp.float32),
                    pltpu.SemaphoreType.DMA((BLOCKS,)),
                ],
                compiler_params=PARAMS,
            )(basic, state)
        )
    m, extra = reduce_over("vel", m, 13 * width)
    m = m.reshape(13, width, cells)
    before, after = neighbours("gx", m, HALO)
    if repeat == 0:
        total = extra.shape[0] * extra.shape[1] // 4
        kept["features"] = run(
            features_kernel,
            (jax.ShapeDtypeStruct((total * LANES, FEATURES), jnp.bfloat16), f32(3, cells)),
            (extra,),
            scratch=(pltpu.VMEM((total, FEATURES, LANES), jnp.float32),),
            scalar=False,
        )
    chunk = sizes[0]
    local, carry, macro, fields = run(
        functools.partial(kinetic_kernel, peers),
        (f32(width, chunk, cells), f32(chunk + width, cells), f32(5, width, cells), f32(10, width, cells)),
        (me, before, m, after, *kept["features"], table, rate, wall, drives[0], rden),
        scratch=(
            pltpu.VMEM((13, width + 2 * SUB, cells), jnp.float32),
            pltpu.VMEM((FEATURES, width * cells), jnp.float32),
            pltpu.VMEM((width, cells), jnp.float32),
        ),
    )
    locals_, carries = [local], [gather_over("gx", carry)]
    for k in range(1, len(states)):
        chunk = sizes[k]
        local, carry = run(
            functools.partial(sweep_kernel, starts[k]),
            (f32(width, chunk, cells), f32(chunk, cells)),
            (table, fields, drives[k], rden),
            scalar=False,
        )
        locals_.append(local)
        carries.append(gather_over("gx", carry))
    if repeat == 0:
        kernel = functools.partial(slabs_kernel, peers, width)
        kept["slabs"] = run(kernel, f32(peers, count, cells), (me, table, carries[0]))
    states, m, state = [], None, None
    for k, chunk in enumerate(sizes):
        args = (me, table, carries[k], kept["slabs"], inflow, locals_[k], prefix)
        if repeat < ITERS - 1:
            m, state = run(
                functools.partial(next_kernel, peers, starts[k]),
                (f32(13 * width, cells), f32(width, chunk, cells)),
                args if m is None else args + (m,),
                (pltpu.VMEM((chunk, cells), jnp.float32), pltpu.VMEM((13, width, SUB, cells), jnp.float32)),
            )
            states.append(state)
        else:
            rest = [] if k == 0 else [states]
            states = pl.pallas_call(
                functools.partial(last_kernel, peers, starts[k]),
                out_shape=f32(count, width, cells),
                in_specs=[SMEM] + [VMEM] * 6 + [HBM] * len(rest),
                out_specs=HBM,
                scratch_shapes=[
                    pltpu.VMEM((chunk, width, cells), jnp.float32),
                    pltpu.SemaphoreType.DMA((BLOCKS,)),
                ],
                input_output_aliases={len(args): 0} if rest else {},
                compiler_params=PARAMS,
            )(*args, *rest)
    return m, states, macro


def per_device(distribution, velocity, weights, collision, solid, inflow):
    count, width, cells = distribution.shape
    me = lax.axis_index("gx").astype(jnp.int32).reshape(1)
    lines = 4 * count // LANES
    far = functools.partial(pltpu.with_memory_space_constraint, memory_space=pltpu.HBM)
    given = tuple(far(x) for x in (velocity, weights.reshape(1, count), collision, solid, distribution))
    m, table, rate, wall = pl.pallas_call(
        first_kernel,
        out_shape=(
            f32(13 * width + lines, cells),
            f32(BASIC, count + PAD, cells),
            f32(width, cells),
            f32(width, cells),
        ),
        in_specs=[HBM] * len(given),
        out_specs=(VMEM,) * 4,
        scratch_shapes=[pltpu.VMEM(x.shape, x.dtype) for x in given]
        + [
            pltpu.VMEM((SUB, count), jnp.float32),
            pltpu.VMEM((13, width, SUB, cells), jnp.float32),
            pltpu.SemaphoreType.DMA((4 + BLOCKS,)),
        ],
        compiler_params=PARAMS,
    )(*given)
    kept, states = {}, given[-1:] * CHUNKS
    for repeat in range(ITERS):
        m, states, macro = iteration(repeat, m, states, table, rate, wall, me, inflow, kept)
    return states, macro


def solution(mesh):
    return jax.shard_map(
        per_device,
        mesh=mesh,
        in_specs=(
            P("vel", "gx", None),
            P(None, "vel"),
            P("vel"),
            P("gx", None),
            P("gx", None),
            P(None, "vel", None),
        ),
        out_specs=(P("vel", "gx", None), P(None, "gx", None)),
        check_vma=False,
    )
```
